8 devices in a mesh: part: 1 (over z), row: 2 (over y), col: 2 (over x), core: 2 (over core).
Axes of the slice: x: 2, y: 2, z: 1, core: 2. Of those that a mesh axis runs over, the one named last changes fastest.
Arguments:
- tokens: bfloat16 [4096, 512], P(('part', 'row', 'col', 'core'))
- route_idx: int32 [4096, 8], P(('part', 'row', 'col', 'core'))
- gate_vals: float32 [4096, 8], P(('part', 'row', 'col', 'core'))
- w_gate: bfloat16 [64, 512, 384], P(('row', 'col', 'core'))
- w_up: bfloat16 [64, 512, 384], P(('row', 'col', 'core'))
- w_down: bfloat16 [64, 384, 512], P(('row', 'col', 'core'))
- grad_out: bfloat16 [4096, 512], P(('part', 'row', 'col', 'core'))
Outputs:
- output 1: bfloat16 [4096, 512], P(('part', 'row', 'col', 'core'))
- output 2: bfloat16 [4096, 512], P(('part', 'row', 'col', 'core'))
- output 3: float32 [4096, 8], P(('part', 'row', 'col', 'core'))
- output 4: float32 [64, 512, 384], P(('part', 'row', 'col', 'core'))
- output 5: float32 [64, 512, 384], P(('part', 'row', 'col', 'core'))
- output 6: float32 [64, 384, 512], P(('part', 'row', 'col', 'core'))
All inputs are finite; a program needn't handle non-finite values.
Results may differ from the reference program's by a relative error of at most 0.0119401.
Values are sent between devices in bfloat16 or wider.
A program may use at most 1 GiB of HBM per device.

```python
import jax
import jax.numpy as jnp
from jax import lax

D = 512
FF = 384
EXPERTS = 64
TOP = 8
TOK = 512
EP_DEVS = 8
TILE = 128


def swiglu(gate_h, up_h):
    return (jax.nn.silu(gate_h.astype(jnp.float32)) * up_h.astype(jnp.float32)).astype(jnp.bfloat16)


def expert_mlp(tok_rows, wt_gate, wt_up, wt_down):
    gate_h = jnp.dot(tok_rows, wt_gate, preferred_element_type=jnp.float32).astype(jnp.bfloat16)
    up_h = jnp.dot(tok_rows, wt_up, preferred_element_type=jnp.float32).astype(jnp.bfloat16)
    hidden = swiglu(gate_h, up_h)
    return jnp.dot(hidden.astype(jnp.float32), wt_down, preferred_element_type=jnp.float32).astype(jnp.bfloat16)


def draw_routes(base_key):
    chip_experts = 2 * EXPERTS // EP_DEVS
    cold_count = EXPERTS - chip_experts
    cold_slots = TOP - 2
    chip_key, perm_key, off_key, slot_key = jax.random.split(base_key, 4)
    hot_chip = jax.random.randint(chip_key, (), 0, EP_DEVS // 2)
    tok_ranks = jax.vmap(lambda sub_key: jax.random.permutation(sub_key, TOK))(jax.random.split(perm_key, EP_DEVS))
    cold_offset = jax.random.randint(off_key, (EP_DEVS, 1, 1), 0, cold_count)
    hot_ids = (tok_ranks[:, :, None] * 2 + jnp.arange(2)) % chip_experts + hot_chip * chip_experts
    cold_pos = (cold_offset + tok_ranks[:, :, None] * cold_slots + jnp.arange(cold_slots)) % cold_count
    cold_ids = jnp.where(cold_pos < hot_chip * chip_experts, cold_pos, cold_pos + chip_experts)
    expert_ids = jnp.concatenate([hot_ids, cold_ids], axis=-1)
    slot_scores = jax.random.randint(slot_key, (EP_DEVS, TOK, TOP), 0, 1 << 20) * TOP + jnp.arange(TOP)
    slot_perm = jnp.argsort(slot_scores, axis=-1)
    picked = jnp.take_along_axis(expert_ids, slot_perm, axis=-1)
    return picked.reshape(EP_DEVS * TOK, TOP).astype(jnp.int32)


def setup_inputs(seed: int = 0, part: int = 0) -> dict:
    part_key = jax.random.fold_in(jax.random.key(seed), part)
    tok_key, route_key, gate_key, grad_key = jax.random.split(part_key, 4)
    wg_key, wu_key, wd_key = jax.random.split(jax.random.key(seed + 1), 3)
    n_tok = EP_DEVS * TOK
    tokens = jax.random.normal(tok_key, (n_tok, D), jnp.float32).astype(jnp.bfloat16)
    gate_raw = jax.random.uniform(gate_key, (n_tok, TOP), jnp.float32, 0.5, 1.5)
    gate_vals = 2.5 * gate_raw / jnp.sum(gate_raw, axis=1, keepdims=True)
    w_gate = (jax.random.normal(wg_key, (EXPERTS, D, FF), jnp.float32) * D ** -0.5).astype(jnp.bfloat16)
    w_up = (jax.random.normal(wu_key, (EXPERTS, D, FF), jnp.float32) * D ** -0.5).astype(jnp.bfloat16)
    w_down = (jax.random.normal(wd_key, (EXPERTS, FF, D), jnp.float32) * FF ** -0.5).astype(jnp.bfloat16)
    grad_out = jax.random.normal(grad_key, (n_tok, D), jnp.float32).astype(jnp.bfloat16)
    return dict(tokens=tokens, route_idx=draw_routes(route_key), gate_vals=gate_vals, w_gate=w_gate, w_up=w_up, w_down=w_down, grad_out=grad_out)


def reference(tokens, route_idx, gate_vals, w_gate, w_up, w_down, grad_out):
    n_tok, top_k = route_idx.shape
    experts, model_dim, ffn_dim = w_gate.shape
    slot_count = n_tok * top_k
    n_tiles = (slot_count + TILE - 1) // TILE + experts
    flat_ids = route_idx.reshape(-1)
    counts = jax.ops.segment_sum(jnp.ones((slot_count,), jnp.int32), flat_ids, num_segments=experts)
    padded = (counts + TILE - 1) // TILE * TILE
    pad_start = jnp.cumsum(padded) - padded
    cnt_start = jnp.cumsum(counts) - counts
    sort_order = jnp.argsort(flat_ids, stable=True).astype(jnp.int32)
    sorted_ids = flat_ids[sort_order]
    row_pos = pad_start[sorted_ids] + jnp.arange(slot_count, dtype=jnp.int32) - cnt_start[sorted_ids]
    row_slot = jnp.full((n_tiles * TILE,), slot_count, jnp.int32).at[row_pos].set(sort_order)
    slot_row = jnp.zeros((slot_count,), jnp.int32).at[sort_order].set(row_pos)
    tile_first = jnp.arange(n_tiles, dtype=jnp.int32) * TILE
    tile_expert = jnp.minimum(jnp.sum((pad_start + padded)[None, :] <= tile_first[:, None], axis=1), experts - 1)
    flat_gate = gate_vals.reshape(-1)

    def tile_step(acc_grads, tile_in):
        acc_gate, acc_up, acc_down = acc_grads
        tile_slots, expert = tile_in
        tok_idx = tile_slots // top_k
        tok_rows = jnp.take(tokens, tok_idx, axis=0, mode='fill', fill_value=0).astype(jnp.float32)
        row_gate = jnp.take(flat_gate, tile_slots, axis=0, mode='fill', fill_value=0)
        row_dy = jnp.take(grad_out, tok_idx, axis=0, mode='fill', fill_value=0).astype(jnp.float32)
        slot_grad = (row_gate[:, None] * row_dy).astype(jnp.bfloat16)
        out_rows, mlp_vjp = jax.vjp(expert_mlp, tok_rows, w_gate[expert].astype(jnp.float32), w_up[expert].astype(jnp.float32), w_down[expert].astype(jnp.float32))
        tile_dx, tile_gw_gate, tile_gw_up, tile_gw_down = mlp_vjp(slot_grad)
        new_acc = (acc_gate.at[expert].add(tile_gw_gate), acc_up.at[expert].add(tile_gw_up), acc_down.at[expert].add(tile_gw_down))
        return new_acc, (out_rows, tile_dx.astype(jnp.bfloat16))

    zero_acc = (jnp.zeros((experts, model_dim, ffn_dim), jnp.float32), jnp.zeros((experts, model_dim, ffn_dim), jnp.float32), jnp.zeros((experts, ffn_dim, model_dim), jnp.float32))
    grad_acc, tiles_out = lax.scan(tile_step, zero_acc, (row_slot.reshape(n_tiles, TILE), tile_expert))
    grad_w_gate, grad_w_up, grad_w_down = grad_acc
    out_tiles, dx_tiles = tiles_out
    slot_out = out_tiles.reshape(-1, model_dim)[slot_row]
    slot_dx = dx_tiles.reshape(-1, model_dim)[slot_row]
    n_blocks = n_tok // TOK

    def combine(comb_in):
        gate_blk, out_blk, dy_blk, dx_blk = comb_in
        out_f32 = out_blk.astype(jnp.float32)
        moe_blk = jnp.einsum('tj,tjd->td', gate_blk, out_f32).astype(jnp.bfloat16)
        gg_blk = jnp.einsum('td,tjd->tj', dy_blk.astype(jnp.float32), out_f32)
        dx_total = jnp.sum(dx_blk.astype(jnp.float32), axis=1).astype(jnp.bfloat16)
        return moe_blk, gg_blk, dx_total

    moe_out, grad_gates, grad_tokens = lax.map(combine, (gate_vals.reshape(n_blocks, TOK, top_k), slot_out.reshape(n_blocks, TOK, top_k, model_dim), grad_out.reshape(n_blocks, TOK, model_dim), slot_dx.reshape(n_blocks, TOK, top_k, model_dim)))
    return (moe_out.reshape(n_tok, model_dim), grad_tokens.reshape(n_tok, model_dim), grad_gates.reshape(n_tok, top_k), grad_w_gate, grad_w_up, grad_w_down)
```

```python
import functools

import jax
import jax.numpy as jnp
from jax import lax
from jax.experimental import pallas as pl
from jax.experimental.pallas import tpu as pltpu
from jax.sharding import PartitionSpec as P

EP_AXES = ('row', 'col', 'core')
ALL_AXES = ('part', 'row', 'col', 'core')
MESH = pl.DeviceIdType.MESH
F32 = jnp.float32
BF16 = jnp.bfloat16
NT = (((1,), (1,)), ((), ()))
TN = (((0,), (0,)), ((), ()))

AG_X, AG_DY, RG, OX, PX, RS_O, RS_P, GG, N_SEM = 0, 10, 20, 27, 31, 35, 41, 47, 54


def dot(a, b):
    return jnp.dot(a, b, preferred_element_type=F32)


def dotg(a, b, dims):
    return lax.dot_general(a, b, dims, preferred_element_type=F32)


def kernel(T, D, FF, NE, CAP,
           x_ref, dy_ref, rg_ref, wg_ref, wu_ref, wd_ref,
           moe_ref, gx_ref, gg_ref, dwg_ref, dwu_ref, dwd_ref,
           xa, dya, xg, us, vs, os_, wg, wu, wd, acc, rd, fr, orv, prv,
           swg, swu, swd, pb, sb, rga, rm, gm, mb, rt, gt, gga, ggs,
           ssem, rsem, lsem):
    H = T // 2
    row, col, core = lax.axis_index('row'), lax.axis_index('col'), lax.axis_index('core')
    me = row * 4 + col * 2 + core
    partner = row * 4 + col * 2 + (1 - core)

    def dev(rel):
        return {
            'row': 1 - row if rel & 4 else row,
            'col': 1 - col if rel & 2 else col,
            'core': 1 - core if rel & 1 else core,
        }

    def rc(i, src, dst, rel):
        return pltpu.make_async_remote_copy(
            src_ref=src, dst_ref=dst, send_sem=ssem.at[i], recv_sem=rsem.at[i],
            device_id=dev(rel), device_id_type=MESH)

    def gather_copies(b, buf):
        lo, hi = pl.ds(0, H), pl.ds(H, H)
        return [
            rc(b + 0, buf.at[0], buf.at[1], 1),
            rc(b + 1, buf.at[0, hi], buf.at[2, hi], 2),
            rc(b + 2, buf.at[0, lo], buf.at[2, lo], 2),
            rc(b + 3, buf.at[0, lo], buf.at[4, lo], 4),
            rc(b + 4, buf.at[0, hi], buf.at[4, hi], 4),
            rc(b + 5, buf.at[2, hi], buf.at[6, hi], 4),
            rc(b + 6, buf.at[4, lo], buf.at[6, lo], 2),
            rc(b + 7, buf.at[2], buf.at[3], 1),
            rc(b + 8, buf.at[4], buf.at[5], 1),
            rc(b + 9, buf.at[6], buf.at[7], 1),
        ]

    lx = pltpu.make_async_copy(x_ref, xa.at[0], lsem.at[0])
    ldy = pltpu.make_async_copy(dy_ref, dya.at[0], lsem.at[1])
    lwg = pltpu.make_async_copy(wg_ref, wg, lsem.at[2])
    lwu = pltpu.make_async_copy(wu_ref, wu, lsem.at[3])
    lwd = pltpu.make_async_copy(wd_ref, wd, lsem.at[4])
    lx.start()
    ldy.start()
    lwg.start()
    lwu.start()
    lwd.start()

    barrier = pltpu.get_barrier_semaphore()
    for rel in range(1, 8):
        pl.semaphore_signal(barrier, inc=1, device_id=dev(rel), device_id_type=MESH)
    pl.semaphore_wait(barrier, 7)

    rgc = [rc(RG + rel - 1, rg_ref, rga.at[rel], rel) for rel in range(1, 8)]
    for c in rgc:
        c.start()
    cx = gather_copies(AG_X, xa)
    cy = gather_copies(AG_DY, dya)
    lx.wait()
    for i in (1, 3, 0, 2, 4):
        cx[i].start()

    rga[0] = rg_ref[...]

    i0 = lax.broadcasted_iota(jnp.int32, (T, T), 0)
    i1 = lax.broadcasted_iota(jnp.int32, (T, T), 1)
    sb[0] = (i0 < i1).astype(F32).astype(BF16)
    sb[1] = (i0 > i1).astype(F32).astype(BF16)
    sb[2] = (i0 == i1).astype(F32).astype(BF16)
    for c in rgc:
        c.wait_recv()
    mb[...] = jnp.zeros_like(mb)
    gm[...] = jnp.zeros_like(gm)
    sub = lax.broadcasted_iota(jnp.int32, (NE, T), 0)
    for idx in range(12):
        src = idx if idx < 8 else 2 * (idx - 8)
        owner = me if idx < 8 else partner
        ids = (sub + owner * NE).astype(F32)
        hits = jnp.zeros((NE, T), F32)
        gates = jnp.zeros((NE, T), F32)
        for j in range(8):
            hit = rga[src, j:j + 1, :] == ids
            hits = hits + jnp.where(hit, 1.0, 0.0)
            gates = gates + jnp.where(hit, rga[src, 8 + j:9 + j, :], 0.0)
        mb[idx] = hits
        gm[idx] = gates
    m_all = mb[...].reshape(16 * NE, T)
    m_bf = m_all.astype(BF16)
    ranks = dot(m_bf, sb[0])
    rm[...] = jnp.where(m_all > 0.5, ranks, -1.0).reshape(16, NE, T)
    m_t = dotg(sb[2], m_bf, NT)
    r_t = dotg(sb[1], m_bf, NT)
    rt[...] = jnp.where(m_t > 0.5, r_t, -1.0).astype(BF16)
    g_all = gm[...].reshape(16 * NE, T)
    g_hi = g_all.astype(BF16)
    rest = g_all - g_hi.astype(F32)
    g_mid = rest.astype(BF16)
    g_lo = (rest - g_mid.astype(F32)).astype(BF16)
    for k, piece in enumerate((g_hi, g_mid, g_lo)):
        gt[k] = dotg(sb[2], piece, NT).astype(BF16)

    lane_r = lax.broadcasted_iota(jnp.int32, (CAP, T), 0).astype(F32)

    def build_p(d):
        r_d = rm[d]
        for l in range(NE):
            pb[l * CAP:(l + 1) * CAP, :] = jnp.where(lane_r == r_d[l:l + 1, :], 1.0, 0.0).astype(BF16)

    def gather_x(d):
        build_p(d)
        xg[d] = dot(pb[...], xa[d]).astype(BF16).reshape(NE, CAP, D)

    def gather_x_loop(first, step, count):
        def one(i, carry):
            gather_x(first + step * i)
            return carry
        lax.fori_loop(0, count, one, 0)

    cx[0].wait_recv()
    gather_x_loop(0, 1, 2)
    cx[1].wait_recv()
    cx[5].start()
    cx[3].wait_recv()
    cx[6].start()
    cx[2].wait_recv()
    cx[7].start()
    cx[4].wait_recv()
    cx[8].start()
    ldy.wait()
    for i in (1, 3, 0, 2, 4):
        cy[i].start()
    gather_x_loop(2, 2, 2)
    cx[7].wait_recv()
    cx[8].wait_recv()
    gather_x_loop(3, 2, 2)
    cx[5].wait_recv()
    cx[6].wait_recv()
    cx[9].start()
    gather_x_loop(6, 1, 1)
    cx[9].wait_recv()
    gather_x_loop(7, 1, 1)

    lwg.wait()
    lwu.wait()
    lwd.wait()

    def forward(l, carry):
        rows = xg[:, pl.ds(l, 1)].reshape(T, D)
        u = dot(rows, wg[l]).astype(BF16)
        v = dot(rows, wu[l]).astype(BF16)
        us[l] = u
        vs[l] = v
        uf = u.astype(F32)
        h = (uf * jax.nn.sigmoid(uf) * v.astype(F32)).astype(BF16)
        o = dot(h, wd[l]).astype(BF16)
        os_[:, pl.ds(l, 1)] = o.reshape(8, 1, CAP, D)
        return carry

    lax.fori_loop(0, NE, forward, 0)

    cy[1].wait_recv()
    cy[5].start()
    cy[3].wait_recv()
    cy[6].start()
    cy[2].wait_recv()
    cy[7].start()
    cy[4].wait_recv()
    cy[8].start()

    order = (3, 1, 2, 0)

    def swap_copies(b, buf):
        return {h: rc(b + h, os_.at[2 * h + 1], buf.at[h], 1) for h in range(4)}

    def reduce_copies(b, k):
        lo, hi = pl.ds(0, H), pl.ds(H, H)
        return [
            rc(b + 0, acc.at[k, 3, lo], rd.at[k, 0], 2),
            rc(b + 1, acc.at[k, 3, hi], rd.at[k, 1], 4),
            rc(b + 2, acc.at[k, 1, lo], fr.at[k, 0, lo], 2),
            rc(b + 3, acc.at[k, 2, hi], fr.at[k, 1, hi], 4),
            rc(b + 4, acc.at[k, 1, hi], fr.at[k, 0, hi], 2),
            rc(b + 5, acc.at[k, 2, lo], fr.at[k, 1, lo], 4),
        ]

    e0 = lax.broadcasted_iota(jnp.int32, (16 * NE, T), 0)
    e1 = lax.broadcasted_iota(jnp.int32, (16 * NE, T), 1) // CAP
    rank_lane = lax.rem(lax.broadcasted_iota(jnp.int32, (T, T), 1), CAP).astype(F32)

    def spread(idx, rows, weighted):
        pick = jnp.where(e0 == e1 + idx * NE, 1.0, 0.0).astype(BF16)
        hit = dot(rt[...], pick) == rank_lane
        if weighted:
            for k in range(3):
                sb[k] = jnp.where(hit, dot(gt[k], pick), 0.0).astype(BF16)
            return dot(sb[0], rows) + dot(sb[1], rows) + dot(sb[2], rows)
        sb[0] = jnp.where(hit, 1.0, 0.0).astype(BF16)
        return dot(sb[0], rows)

    def combine(k, h, recv, weighted):
        a = spread(2 * h, os_[2 * h].reshape(T, D), weighted)
        acc[k, h] = a + spread(8 + h, recv[h].reshape(T, D), weighted)

    ox = swap_copies(OX, orv)
    ro = reduce_copies(RS_O, 0)
    for h in order:
        ox[h].start()
    for h in order:
        ox[h].wait_recv()

    def combine_all(k, recv, copies, weighted):
        def one(i, carry):
            h = 3 - i
            combine(k, h, recv, weighted)

            @pl.when(i == 0)
            def _():
                copies[0].start()
                copies[1].start()

            @pl.when(i == 1)
            def _():
                copies[3].start()

            @pl.when(i == 2)
            def _():
                copies[2].start()
            return carry
        lax.fori_loop(0, 4, one, 0)

    combine_all(0, orv, ro, True)

    cy[5].wait_recv()
    cy[6].wait_recv()
    cy[9].start()
    cy[0].wait_recv()
    cy[7].wait_recv()
    cy[8].wait_recv()
    cy[9].wait_recv()
    for c in cx:
        c.wait_send()

    ggc = [rc(GG + rel - 1, ggs.at[rel], gga.at[rel], rel) for rel in range(1, 8)]

    def gather_dy(d, carry):
        build_p(d)
        rows = dot(pb[...], dya[d])
        outs = os_[d].reshape(T, D).astype(F32)
        gg_rows = jnp.sum(rows * outs, axis=1, keepdims=True)
        r_d = rm[d]
        g_d = gm[d]
        for l in range(NE):
            hit = lane_r == r_d[l:l + 1, :]
            gcol = jnp.sum(jnp.where(hit, g_d[l:l + 1, :], 0.0), axis=1, keepdims=True)
            xa[d, l * CAP:(l + 1) * CAP, :] = (gcol * rows[l * CAP:(l + 1) * CAP, :]).astype(BF16)
            ggs[d, l:l + 1, :] = jnp.sum(
                jnp.where(hit, gg_rows[l * CAP:(l + 1) * CAP, :], 0.0), axis=0, keepdims=True)
        return carry

    lax.fori_loop(0, 8, gather_dy, 0)
    for c in ggc:
        c.start()
    for h in order:
        ox[h].wait_send()

    def finish_grads(l):
        return [
            pltpu.make_async_copy(swg, dwg_ref.at[l], lsem.at[5]),
            pltpu.make_async_copy(swu, dwu_ref.at[l], lsem.at[6]),
            pltpu.make_async_copy(swd, dwd_ref.at[l], lsem.at[7]),
        ]

    def backward(l, carry):
        rows = xg[:, pl.ds(l, 1)].reshape(T, D)
        c = xa[:, pl.ds(pl.multiple_of(l * CAP, CAP), CAP), :].reshape(T, D)
        dh = dotg(c, wd[l], NT).astype(BF16).astype(F32)
        uf = us[l].astype(F32)
        vf = vs[l].astype(F32)
        s = jax.nn.sigmoid(uf)
        sl = uf * s
        h = (sl * vf).astype(BF16)
        dv = (dh * sl).astype(BF16)
        du = (dh * vf * (s + sl * (1.0 - s))).astype(BF16)
        pr = (dotg(du, wg[l], NT) + dotg(dv, wu[l], NT)).astype(BF16)
        os_[:, pl.ds(l, 1)] = pr.reshape(8, 1, CAP, D)

        @pl.when(l > 0)
        def _():
            for cp in finish_grads(l - 1):
                cp.wait()
        swd[...] = dotg(h, c, TN)
        swg[...] = dotg(rows, du, TN)
        swu[...] = dotg(rows, dv, TN)
        for cp in finish_grads(l):
            cp.start()
        return carry

    def pass_on(k, copies):
        copies[0].wait_recv()
        acc[k, 2, :H] = acc[k, 2, :H] + rd[k, 0]
        copies[5].start()
        copies[1].wait_recv()
        acc[k, 1, H:] = acc[k, 1, H:] + rd[k, 1]
        copies[4].start()

    def finish(k, copies, out):
        for i in (2, 3, 4, 5):
            copies[i].wait_recv()
        out[...] = (acc[k, 0] + fr[k, 0] + fr[k, 1]).astype(BF16)

    lax.fori_loop(0, NE // 2, backward, 0)
    pass_on(0, ro)
    lax.fori_loop(NE // 2, NE, backward, 0)

    px = swap_copies(PX, prv)
    rp = reduce_copies(RS_P, 1)
    for h in order:
        px[h].start()
    for h in order:
        px[h].wait_recv()
    combine_all(1, prv, rp, False)

    for c in ggc:
        c.wait_recv()
    gga[0] = ggs[0]
    out = [jnp.zeros((1, T), F32) for _ in range(8)]
    for rel in range(8):
        d = dev(rel)
        base = d['row'] * 4 + d['col'] * 2 + d['core']
        ids = (sub + base * NE).astype(F32)
        part = gga[rel]
        for j in range(8):
            hit = rg_ref[j:j + 1, :] == ids
            out[j] = out[j] + jnp.sum(jnp.where(hit, part, 0.0), axis=0, keepdims=True)
    for j in range(8):
        gg_ref[j:j + 1, :] = out[j]

    finish(0, ro, moe_ref)
    pass_on(1, rp)
    finish(1, rp, gx_ref)

    for cp in finish_grads(NE - 1):
        cp.wait()
    for c in rgc + cy + ggc + ro + rp + [px[h] for h in order]:
        c.wait_send()


def solution(mesh):
    tok_spec = P(ALL_AXES, None)
    w_spec = P(EP_AXES, None, None)
    gw_spec = P(ALL_AXES, None, None)

    def local_step(tokens, route_idx, gate_vals, w_gate, w_up, w_down, grad_out):
        T, K = route_idx.shape
        D = tokens.shape[1]
        NE, _, FF = w_gate.shape
        CAP = T * K // (8 * NE)
        rg = jnp.concatenate([route_idx.astype(F32).T, gate_vals.T], axis=0)
        vm = pl.BlockSpec(memory_space=pltpu.VMEM)
        hbm = pl.BlockSpec(memory_space=pl.ANY)
        sds = jax.ShapeDtypeStruct
        outs = pl.pallas_call(
            functools.partial(kernel, T, D, FF, NE, CAP),
            out_shape=(sds((T, D), BF16), sds((T, D), BF16), sds((K, T), F32),
                       sds((NE, D, FF), F32), sds((NE, D, FF), F32), sds((NE, FF, D), F32)),
            in_specs=[hbm, hbm, vm, hbm, hbm, hbm],
            out_specs=(vm, vm, vm, hbm, hbm, hbm),
            scratch_shapes=[
                pltpu.VMEM((8, T, D), BF16),
                pltpu.VMEM((8, T, D), BF16),
                pltpu.VMEM((8, NE, CAP, D), BF16),
                pltpu.VMEM((NE, T, FF), BF16),
                pltpu.VMEM((NE, T, FF), BF16),
                pltpu.VMEM((8, NE, CAP, D), BF16),
                pltpu.VMEM((NE, D, FF), BF16),
                pltpu.VMEM((NE, D, FF), BF16),
                pltpu.VMEM((NE, FF, D), BF16),
                pltpu.VMEM((2, 4, T, D), F32),
                pltpu.VMEM((2, 2, T // 2, D), F32),
                pltpu.VMEM((2, 2, T, D), F32),
                pltpu.VMEM((4, NE, CAP, D), BF16),
                pltpu.VMEM((4, NE, CAP, D), BF16),
                pltpu.VMEM((D, FF), F32),
                pltpu.VMEM((D, FF), F32),
                pltpu.VMEM((FF, D), F32),
                pltpu.VMEM((T, T), BF16),
                pltpu.VMEM((3, T, T), BF16),
                pltpu.VMEM((8, 2 * K, T), F32),
                pltpu.VMEM((16, NE, T), F32),
                pltpu.VMEM((16, NE, T), F32),
                pltpu.VMEM((16, NE, T), F32),
                pltpu.VMEM((T, 16 * NE), BF16),
                pltpu.VMEM((3, T, 16 * NE), BF16),
                pltpu.VMEM((8, NE, T), F32),
                pltpu.VMEM((8, NE, T), F32),
                pltpu.SemaphoreType.DMA((N_SEM,)),
                pltpu.SemaphoreType.DMA((N_SEM,)),
                pltpu.SemaphoreType.DMA((8,)),
            ],
            compiler_params=pltpu.CompilerParams(
                collective_id=0, has_side_effects=True, vmem_limit_bytes=67043328),
        )(tokens, grad_out, rg, w_gate, w_up, w_down)
        moe, gx, gg, dwg, dwu, dwd = outs
        return moe, gx, gg.T, dwg, dwu, dwd

    return jax.shard_map(
        local_step, mesh=mesh,
        in_specs=(tok_spec, tok_spec, tok_spec, w_spec, w_spec, w_spec, tok_spec),
        out_specs=(tok_spec, tok_spec, tok_spec, gw_spec, gw_spec, gw_spec),
        check_vma=False)
```

```python
import functools

import jax
import jax.numpy as jnp
from jax import lax
from jax.experimental import pallas as pl
from jax.experimental.pallas import tpu as pltpu
from jax.sharding import PartitionSpec as P

EP_AXES = ('row', 'col', 'core')
ALL_AXES = ('part', 'row', 'col', 'core')
MESH = pl.DeviceIdType.MESH
F32 = jnp.float32
BF16 = jnp.bfloat16
NT = (((1,), (1,)), ((), ()))
TN = (((0,), (0,)), ((), ()))

AG_X, AG_DY, RG, OX, PX, RS_O, RS_P, GG, N_SEM = 0, 10, 20, 27, 31, 35, 41, 47, 54


def dot(a, b):
    return jnp.dot(a, b, preferred_element_type=F32)


def dotg(a, b, dims):
    return lax.dot_general(a, b, dims, preferred_element_type=F32)


def kernel(T, D, FF, NE, CAP,
           x_ref, dy_ref, rg_ref, wg_ref, wu_ref, wd_ref,
           moe_ref, gx_ref, gg_ref, dwg_ref, dwu_ref, dwd_ref,
           xa, dya, xg, us, vs, hs, os_, wg, wu, wd, acc, rd, fr, orv, prv,
           swg, swu, swd, pb, sb, rga, rm, gm, mb, rt, gt, gga, ggs,
           ssem, rsem, lsem):
    H = T // 2
    row, col, core = lax.axis_index('row'), lax.axis_index('col'), lax.axis_index('core')
    me = row * 4 + col * 2 + core
    partner = row * 4 + col * 2 + (1 - core)

    def dev(rel):
        return {
            'row': 1 - row if rel & 4 else row,
            'col': 1 - col if rel & 2 else col,
            'core': 1 - core if rel & 1 else core,
        }

    def rc(i, src, dst, rel):
        return pltpu.make_async_remote_copy(
            src_ref=src, dst_ref=dst, send_sem=ssem.at[i], recv_sem=rsem.at[i],
            device_id=dev(rel), device_id_type=MESH)

    def gather_copies(b, buf):
        lo, hi = pl.ds(0, H), pl.ds(H, H)
        return [
            rc(b + 0, buf.at[0], buf.at[1], 1),
            rc(b + 1, buf.at[0, hi], buf.at[2, hi], 2),
            rc(b + 2, buf.at[0, lo], buf.at[2, lo], 2),
            rc(b + 3, buf.at[0, lo], buf.at[4, lo], 4),
            rc(b + 4, buf.at[0, hi], buf.at[4, hi], 4),
            rc(b + 5, buf.at[2, hi], buf.at[6, hi], 4),
            rc(b + 6, buf.at[4, lo], buf.at[6, lo], 2),
            rc(b + 7, buf.at[2], buf.at[3], 1),
            rc(b + 8, buf.at[4], buf.at[5], 1),
            rc(b + 9, buf.at[6], buf.at[7], 1),
        ]

    lx = pltpu.make_async_copy(x_ref, xa.at[0], lsem.at[0])
    ldy = pltpu.make_async_copy(dy_ref, dya.at[0], lsem.at[1])
    lwg = pltpu.make_async_copy(wg_ref, wg, lsem.at[2])
    lwu = pltpu.make_async_copy(wu_ref, wu, lsem.at[3])
    lwd = pltpu.make_async_copy(wd_ref, wd, lsem.at[4])
    lx.start()
    ldy.start()
    lwg.start()
    lwu.start()
    lwd.start()

    barrier = pltpu.get_barrier_semaphore()
    for rel in range(1, 8):
        pl.semaphore_signal(barrier, inc=1, device_id=dev(rel), device_id_type=MESH)
    pl.semaphore_wait(barrier, 7)

    rgc = [rc(RG + rel - 1, rg_ref, rga.at[rel], rel) for rel in range(1, 8)]
    for c in rgc:
        c.start()
    cx = gather_copies(AG_X, xa)
    cy = gather_copies(AG_DY, dya)
    lx.wait()
    for i in (1, 3, 0, 2, 4):
        cx[i].start()

    rga[0] = rg_ref[...]

    i0 = lax.broadcasted_iota(jnp.int32, (T, T), 0)
    i1 = lax.broadcasted_iota(jnp.int32, (T, T), 1)
    sb[0] = (i0 < i1).astype(F32).astype(BF16)
    sb[1] = (i0 > i1).astype(F32).astype(BF16)
    sb[2] = (i0 == i1).astype(F32).astype(BF16)
    for c in rgc:
        c.wait_recv()
    mb[...] = jnp.zeros_like(mb)
    gm[...] = jnp.zeros_like(gm)
    sub = lax.broadcasted_iota(jnp.int32, (NE, T), 0)
    for idx in range(12):
        src = idx if idx < 8 else 2 * (idx - 8)
        owner = me if idx < 8 else partner
        ids = (sub + owner * NE).astype(F32)
        hits = jnp.zeros((NE, T), F32)
        gates = jnp.zeros((NE, T), F32)
        for j in range(8):
            hit = rga[src, j:j + 1, :] == ids
            hits = hits + jnp.where(hit, 1.0, 0.0)
            gates = gates + jnp.where(hit, rga[src, 8 + j:9 + j, :], 0.0)
        mb[idx] = hits
        gm[idx] = gates
    m_all = mb[...].reshape(16 * NE, T)
    m_bf = m_all.astype(BF16)
    ranks = dot(m_bf, sb[0])
    rm[...] = jnp.where(m_all > 0.5, ranks, -1.0).reshape(16, NE, T)
    m_t = dotg(sb[2], m_bf, NT)
    r_t = dotg(sb[1], m_bf, NT)
    rt[...] = jnp.where(m_t > 0.5, r_t, -1.0).astype(BF16)
    g_all = gm[...].reshape(16 * NE, T)
    g_hi = g_all.astype(BF16)
    rest = g_all - g_hi.astype(F32)
    g_mid = rest.astype(BF16)
    g_lo = (rest - g_mid.astype(F32)).astype(BF16)
    for k, piece in enumerate((g_hi, g_mid, g_lo)):
        gt[k] = dotg(sb[2], piece, NT).astype(BF16)

    lane_r = lax.broadcasted_iota(jnp.int32, (CAP, T), 0).astype(F32)

    def build_p(d):
        r_d = rm[d]
        for l in range(NE):
            pb[l * CAP:(l + 1) * CAP, :] = jnp.where(lane_r == r_d[l:l + 1, :], 1.0, 0.0).astype(BF16)

    def gather_x(d):
        build_p(d)
        xg[d] = dot(pb[...], xa[d]).astype(BF16).reshape(NE, CAP, D)

    def gather_x_loop(first, step, count):
        def one(i, carry):
            gather_x(first + step * i)
            return carry
        lax.fori_loop(0, count, one, 0)

    cx[0].wait_recv()
    gather_x_loop(0, 1, 2)
    cx[1].wait_recv()
    cx[5].start()
    cx[3].wait_recv()
    cx[6].start()
    cx[2].wait_recv()
    cx[7].start()
    cx[4].wait_recv()
    cx[8].start()
    ldy.wait()
    for i in (1, 3, 0, 2, 4):
        cy[i].start()
    gather_x_loop(2, 2, 2)
    cx[7].wait_recv()
    cx[8].wait_recv()
    gather_x_loop(3, 2, 2)
    cx[5].wait_recv()
    cx[6].wait_recv()
    cx[9].start()
    gather_x_loop(6, 1, 1)
    cx[9].wait_recv()
    gather_x_loop(7, 1, 1)

    lwg.wait()
    lwu.wait()
    lwd.wait()

    def forward(l, carry):
        rows = xg[:, pl.ds(l, 1)].reshape(T, D)
        u = dot(rows, wg[l]).astype(BF16)
        v = dot(rows, wu[l]).astype(BF16)
        us[l] = u
        vs[l] = v
        uf = u.astype(F32)
        h = (uf * jax.nn.sigmoid(uf) * v.astype(F32)).astype(BF16)
        o = dot(h, wd[l]).astype(BF16)
        os_[:, pl.ds(l, 1)] = o.reshape(8, 1, CAP, D)
        return carry

    lax.fori_loop(0, NE // 2, forward, 0)
    cy[1].wait_recv()
    cy[5].start()
    cy[3].wait_recv()
    cy[6].start()
    lax.fori_loop(NE // 2, NE, forward, 0)

    order = (3, 1, 2, 0)

    def swap_copy(b, buf, h):
        return rc(b + h, os_.at[2 * h + 1], buf.at[h], 1)

    def reduce_copies(b, k):
        lo, hi = pl.ds(0, H), pl.ds(H, H)
        return [
            rc(b + 0, acc.at[k, 3, lo], rd.at[k, 0], 2),
            rc(b + 1, acc.at[k, 3, hi], rd.at[k, 1], 4),
            rc(b + 2, acc.at[k, 1, lo], fr.at[k, 0, lo], 2),
            rc(b + 3, acc.at[k, 2, hi], fr.at[k, 1, hi], 4),
            rc(b + 4, acc.at[k, 1, hi], fr.at[k, 0, hi], 2),
            rc(b + 5, acc.at[k, 2, lo], fr.at[k, 1, lo], 4),
        ]

    e0 = lax.broadcasted_iota(jnp.int32, (16 * NE, T), 0)
    e1 = lax.broadcasted_iota(jnp.int32, (16 * NE, T), 1) // CAP
    rank_lane = lax.rem(lax.broadcasted_iota(jnp.int32, (T, T), 1), CAP).astype(F32)

    def spread(idx, rows, weighted):
        pick = jnp.where(e0 == e1 + idx * NE, 1.0, 0.0).astype(BF16)
        hit = dot(rt[...], pick) == rank_lane
        if weighted:
            for k in range(3):
                sb[k] = jnp.where(hit, dot(gt[k], pick), 0.0).astype(BF16)
            return dot(sb[0], rows) + dot(sb[1], rows) + dot(sb[2], rows)
        sb[0] = jnp.where(hit, 1.0, 0.0).astype(BF16)
        return dot(sb[0], rows)

    def combine_all(k, b, recv, copies, weighted):
        def one(i, carry):
            h = 3 - i
            acc[k, h] = spread(2 * h, os_[2 * h].reshape(T, D), weighted)
            swap_copy(b, recv, h).wait_recv()
            acc[k, h] = acc[k, h] + spread(8 + h, recv[h].reshape(T, D), weighted)

            @pl.when(i == 0)
            def _():
                copies[0].start()
                copies[1].start()

            @pl.when(i == 1)
            def _():
                copies[3].start()

            @pl.when(i == 2)
            def _():
                copies[2].start()
            return carry
        lax.fori_loop(0, 4, one, 0)

    ro = reduce_copies(RS_O, 0)
    for h in order:
        swap_copy(OX, orv, h).start()
    cy[2].wait_recv()
    cy[7].start()
    cy[4].wait_recv()
    cy[8].start()
    combine_all(0, OX, orv, ro, True)

    cy[5].wait_recv()
    cy[6].wait_recv()
    cy[9].start()
    cy[0].wait_recv()
    cy[7].wait_recv()
    cy[8].wait_recv()
    cy[9].wait_recv()
    for c in cx:
        c.wait_send()

    ggc = [rc(GG + rel - 1, ggs.at[rel], gga.at[rel], rel) for rel in range(1, 8)]

    def gather_dy(d, carry):
        build_p(d)
        rows = dot(pb[...], dya[d])
        outs = os_[d].reshape(T, D).astype(F32)
        gg_rows = jnp.sum(rows * outs, axis=1, keepdims=True)
        r_d = rm[d]
        g_d = gm[d]
        for l in range(NE):
            hit = lane_r == r_d[l:l + 1, :]
            gcol = jnp.sum(jnp.where(hit, g_d[l:l + 1, :], 0.0), axis=1, keepdims=True)
            xa[d, l * CAP:(l + 1) * CAP, :] = (gcol * rows[l * CAP:(l + 1) * CAP, :]).astype(BF16)
            ggs[d, l:l + 1, :] = jnp.sum(
                jnp.where(hit, gg_rows[l * CAP:(l + 1) * CAP, :], 0.0), axis=0, keepdims=True)
        return carry

    lax.fori_loop(0, 8, gather_dy, 0)
    for c in ggc:
        c.start()
    for h in order:
        swap_copy(OX, orv, h).wait_send()

    def pass_on(k, copies):
        copies[0].wait_recv()
        acc[k, 2, :H] = acc[k, 2, :H] + rd[k, 0]
        copies[5].start()
        copies[1].wait_recv()
        acc[k, 1, H:] = acc[k, 1, H:] + rd[k, 1]
        copies[4].start()

    def finish(k, copies, out):
        for i in (2, 3, 4, 5):
            copies[i].wait_recv()
        out[...] = (acc[k, 0] + fr[k, 0] + fr[k, 1]).astype(BF16)

    pass_on(0, ro)

    def expert_rows(buf, l):
        return buf[:, pl.ds(pl.multiple_of(l * CAP, CAP), CAP), :].reshape(T, D)

    def backward(l, carry):
        dh = dotg(expert_rows(xa, l), wd[l], NT).astype(BF16).astype(F32)
        uf = us[l].astype(F32)
        vf = vs[l].astype(F32)
        s = jax.nn.sigmoid(uf)
        sl = uf * s
        hs[l] = (sl * vf).astype(BF16)
        dv = (dh * sl).astype(BF16)
        du = (dh * vf * (s + sl * (1.0 - s))).astype(BF16)
        us[l] = du
        vs[l] = dv
        pr = (dotg(du, wg[l], NT) + dotg(dv, wu[l], NT)).astype(BF16)
        os_[:, pl.ds(l, 1)] = pr.reshape(8, 1, CAP, D)
        return carry

    lax.fori_loop(0, NE, backward, 0)

    rp = reduce_copies(RS_P, 1)
    for h in order:
        swap_copy(PX, prv, h).start()
    combine_all(1, PX, prv, rp, False)

    def finish_grads(l):
        return [
            pltpu.make_async_copy(swg, dwg_ref.at[l], lsem.at[5]),
            pltpu.make_async_copy(swu, dwu_ref.at[l], lsem.at[6]),
            pltpu.make_async_copy(swd, dwd_ref.at[l], lsem.at[7]),
        ]

    def weight_grads(l, carry):
        rows = xg[:, pl.ds(l, 1)].reshape(T, D)

        @pl.when(l > 0)
        def _():
            for cp in finish_grads(l - 1):
                cp.wait()
        swg[...] = dotg(rows, us[l], TN)
        swu[...] = dotg(rows, vs[l], TN)
        swd[...] = dotg(hs[l], expert_rows(xa, l), TN)
        for cp in finish_grads(l):
            cp.start()
        return carry

    for c in ggc:
        c.wait_recv()
    gga[0] = ggs[0]
    out = [jnp.zeros((1, T), F32) for _ in range(8)]
    for rel in range(8):
        d = dev(rel)
        base = d['row'] * 4 + d['col'] * 2 + d['core']
        ids = (sub + base * NE).astype(F32)
        part = gga[rel]
        for j in range(8):
            hit = rg_ref[j:j + 1, :] == ids
            out[j] = out[j] + jnp.sum(jnp.where(hit, part, 0.0), axis=0, keepdims=True)
    for j in range(8):
        gg_ref[j:j + 1, :] = out[j]

    finish(0, ro, moe_ref)
    lax.fori_loop(0, NE // 2, weight_grads, 0)
    pass_on(1, rp)
    lax.fori_loop(NE // 2, NE, weight_grads, 0)
    for cp in finish_grads(NE - 1):
        cp.wait()
    for c in rgc + cy + ggc + ro:
        c.wait_send()
    for h in order:
        swap_copy(PX, prv, h).wait_send()
    finish(1, rp, gx_ref)
    for c in rp:
        c.wait_send()


def solution(mesh):
    tok_spec = P(ALL_AXES, None)
    w_spec = P(EP_AXES, None, None)
    gw_spec = P(ALL_AXES, None, None)

    def local_step(tokens, route_idx, gate_vals, w_gate, w_up, w_down, grad_out):
        T, K = route_idx.shape
        D = tokens.shape[1]
        NE, _, FF = w_gate.shape
        CAP = T * K // (8 * NE)
        rg = jnp.concatenate([route_idx.astype(F32).T, gate_vals.T], axis=0)
        vm = pl.BlockSpec(memory_space=pltpu.VMEM)
        hbm = pl.BlockSpec(memory_space=pl.ANY)
        sds = jax.ShapeDtypeStruct
        outs = pl.pallas_call(
            functools.partial(kernel, T, D, FF, NE, CAP),
            out_shape=(sds((T, D), BF16), sds((T, D), BF16), sds((K, T), F32),
                       sds((NE, D, FF), F32), sds((NE, D, FF), F32), sds((NE, FF, D), F32)),
            in_specs=[hbm, hbm, vm, hbm, hbm, hbm],
            out_specs=(vm, vm, vm, hbm, hbm, hbm),
            scratch_shapes=[
                pltpu.VMEM((8, T, D), BF16),
                pltpu.VMEM((8, T, D), BF16),
                pltpu.VMEM((8, NE, CAP, D), BF16),
                pltpu.VMEM((NE, T, FF), BF16),
                pltpu.VMEM((NE, T, FF), BF16),
                pltpu.VMEM((NE, T, FF), BF16),
                pltpu.VMEM((8, NE, CAP, D), BF16),
                pltpu.VMEM((NE, D, FF), BF16),
                pltpu.VMEM((NE, D, FF), BF16),
                pltpu.VMEM((NE, FF, D), BF16),
                pltpu.VMEM((2, 4, T, D), F32),
                pltpu.VMEM((2, 2, T // 2, D), F32),
                pltpu.VMEM((2, 2, T, D), F32),
                pltpu.VMEM((4, NE, CAP, D), BF16),
                pltpu.VMEM((4, NE, CAP, D), BF16),
                pltpu.VMEM((D, FF), F32),
                pltpu.VMEM((D, FF), F32),
                pltpu.VMEM((FF, D), F32),
                pltpu.VMEM((T, T), BF16),
                pltpu.VMEM((3, T, T), BF16),
                pltpu.VMEM((8, 2 * K, T), F32),
                pltpu.VMEM((16, NE, T), F32),
                pltpu.VMEM((16, NE, T), F32),
                pltpu.VMEM((16, NE, T), F32),
                pltpu.VMEM((T, 16 * NE), BF16),
                pltpu.VMEM((3, T, 16 * NE), BF16),
                pltpu.VMEM((8, NE, T), F32),
                pltpu.VMEM((8, NE, T), F32),
                pltpu.SemaphoreType.DMA((N_SEM,)),
                pltpu.SemaphoreType.DMA((N_SEM,)),
                pltpu.SemaphoreType.DMA((8,)),
            ],
            compiler_params=pltpu.CompilerParams(
                collective_id=0, has_side_effects=True, vmem_limit_bytes=67043328),
        )(tokens, grad_out, rg, w_gate, w_up, w_down)
        moe, gx, gg, dwg, dwu, dwd = outs
        return moe, gx, gg.T, dwg, dwu, dwd

    return jax.shard_map(
        local_step, mesh=mesh,
        in_specs=(tok_spec, tok_spec, tok_spec, w_spec, w_spec, w_spec, tok_spec),
        out_specs=(tok_spec, tok_spec, tok_spec, gw_spec, gw_spec, gw_spec),
        check_vma=False)
```

```python
import functools

import jax
import jax.numpy as jnp
from jax import lax
from jax.experimental import pallas as pl
from jax.experimental.pallas import tpu as pltpu
from jax.sharding import PartitionSpec as P


EP_AXES = ('row', 'col', 'core')
ALL_AXES = ('part', 'row', 'col', 'core')
MESH = pl.DeviceIdType.MESH
F32 = jnp.float32
BF16 = jnp.bfloat16
NT = (((1,), (1,)), ((), ()))
TN = (((0,), (0,)), ((), ()))

AG_X, AG_DY, RG, OX, PX, RS_O, RS_P, GG, N_SEM = 0, 10, 20, 34, 38, 42, 48, 52, 59


def dot(a, b):
    return jnp.dot(a, b, preferred_element_type=F32)


def dotg(a, b, dims):
    return lax.dot_general(a, b, dims, preferred_element_type=F32)


def kernel(T, D, FF, NE, CAP,
           x_ref, dy_ref, route_ref, gate_ref, wg_ref, wu_ref, wd_ref,
           moe_ref, gg_ref, base_ref, mx_ref, my_ref, dwg_ref, dwu_ref, dwd_ref,
           xa, dya, xg, us, vs, hs, os_, wg, wu, wd, acc, rd, fr, orv, prv,
           swg, swu, swd, pb, sb, ra, ga, rm, gm, mb, rt, gt, gga, ggs,
           ssem, rsem, lsem):
    H = T // 2
    row, col, core = lax.axis_index('row'), lax.axis_index('col'), lax.axis_index('core')
    me = row * 4 + col * 2 + core
    partner = row * 4 + col * 2 + (1 - core)

    def dev(rel):
        return {
            'row': 1 - row if rel & 4 else row,
            'col': 1 - col if rel & 2 else col,
            'core': 1 - core if rel & 1 else core,
        }

    def rc(i, src, dst, rel):
        return pltpu.make_async_remote_copy(
            src_ref=src, dst_ref=dst, send_sem=ssem.at[i], recv_sem=rsem.at[i],
            device_id=dev(rel), device_id_type=MESH)

    def gather_copies(b, buf):
        lo, hi = pl.ds(0, H), pl.ds(H, H)
        return [
            rc(b + 0, buf.at[0], buf.at[1], 1),
            rc(b + 1, buf.at[0, hi], buf.at[2, hi], 2),
            rc(b + 2, buf.at[0, lo], buf.at[2, lo], 2),
            rc(b + 3, buf.at[0, lo], buf.at[4, lo], 4),
            rc(b + 4, buf.at[0, hi], buf.at[4, hi], 4),
            rc(b + 5, buf.at[2, hi], buf.at[6, hi], 4),
            rc(b + 6, buf.at[4, lo], buf.at[6, lo], 2),
            rc(b + 7, buf.at[2], buf.at[3], 1),
            rc(b + 8, buf.at[4], buf.at[5], 1),
            rc(b + 9, buf.at[6], buf.at[7], 1),
        ]

    lx = pltpu.make_async_copy(x_ref, xa.at[0], lsem.at[0])
    ldy = pltpu.make_async_copy(dy_ref, dya.at[0], lsem.at[1])
    lwg = pltpu.make_async_copy(wg_ref, wg, lsem.at[2])
    lwu = pltpu.make_async_copy(wu_ref, wu, lsem.at[3])
    lwd = pltpu.make_async_copy(wd_ref, wd, lsem.at[4])
    lx.start()
    ldy.start()
    lwg.start()
    lwu.start()
    lwd.start()

    barrier = pltpu.get_barrier_semaphore()
    for rel in range(1, 8):
        pl.semaphore_signal(barrier, inc=1, device_id=dev(rel), device_id_type=MESH)
    pl.semaphore_wait(barrier, 7)

    rgc = [rc(RG + rel - 1, route_ref, ra.at[rel], rel) for rel in range(1, 8)]
    rgc += [rc(RG + 6 + rel, gate_ref, ga.at[rel], rel) for rel in range(1, 8)]
    for c in rgc:
        c.start()
    cx = gather_copies(AG_X, xa)
    cy = gather_copies(AG_DY, dya)
    lx.wait()
    for i in (1, 3, 0, 2, 4):
        cx[i].start()

    ra[0] = route_ref[...]
    ga[0] = gate_ref[...]

    i0 = lax.broadcasted_iota(jnp.int32, (T, T), 0)
    i1 = lax.broadcasted_iota(jnp.int32, (T, T), 1)
    sb[0] = (i0 < i1).astype(F32).astype(BF16)
    sb[1] = (i0 > i1).astype(F32).astype(BF16)
    sb[2] = (i0 == i1).astype(F32).astype(BF16)
    for c in rgc:
        c.wait_recv()
    mb[...] = jnp.zeros_like(mb)
    gm[...] = jnp.zeros_like(gm)
    sub = lax.broadcasted_iota(jnp.int32, (NE, T), 0)
    for idx in range(12):
        src = idx if idx < 8 else 2 * (idx - 8)
        owner = me if idx < 8 else partner
        ids = sub + owner * NE
        hits = jnp.zeros((NE, T), F32)
        gates = jnp.zeros((NE, T), F32)
        for j in range(8):
            hit = ra[src, j:j + 1, :] == ids
            hits = hits + jnp.where(hit, 1.0, 0.0)
            gates = gates + jnp.where(hit, ga[src, j:j + 1, :], 0.0)
        mb[idx] = hits
        gm[idx] = gates
    m_all = mb[...].reshape(16 * NE, T)
    m_bf = m_all.astype(BF16)
    ranks = dot(m_bf, sb[0])
    rm[...] = jnp.where(m_all > 0.5, ranks, -1.0).reshape(16, NE, T)
    m_t = dotg(sb[2], m_bf, NT)
    r_t = dotg(sb[1], m_bf, NT)
    rt[...] = jnp.where(m_t > 0.5, r_t, -1.0).astype(BF16)
    g_all = gm[...].reshape(16 * NE, T)
    g_hi = g_all.astype(BF16)
    rest = g_all - g_hi.astype(F32)
    g_mid = rest.astype(BF16)
    g_lo = (rest - g_mid.astype(F32)).astype(BF16)
    for k, piece in enumerate((g_hi, g_mid, g_lo)):
        gt[k] = dotg(sb[2], piece, NT).astype(BF16)

    lane_r = lax.broadcasted_iota(jnp.int32, (CAP, T), 0).astype(F32)

    def build_p(d):
        r_d = rm[d]
        for l in range(NE):
            pb[l * CAP:(l + 1) * CAP, :] = jnp.where(lane_r == r_d[l:l + 1, :], 1.0, 0.0).astype(BF16)

    def gather_x(d):
        build_p(d)
        xg[d] = dot(pb[...], xa[d]).astype(BF16).reshape(NE, CAP, D)

    def gather_x_loop(first, step, count):
        def one(i, carry):
            gather_x(first + step * i)
            return carry
        lax.fori_loop(0, count, one, 0)

    cx[0].wait_recv()
    gather_x_loop(0, 1, 2)
    cx[1].wait_recv()
    cx[5].start()
    cx[3].wait_recv()
    cx[6].start()
    cx[2].wait_recv()
    cx[7].start()
    cx[4].wait_recv()
    cx[8].start()
    ldy.wait()
    for i in (1, 3, 0, 2, 4):
        cy[i].start()
    gather_x_loop(2, 2, 2)
    cx[7].wait_recv()
    cx[8].wait_recv()
    gather_x_loop(3, 2, 2)
    cx[5].wait_recv()
    cx[6].wait_recv()
    cx[9].start()
    gather_x_loop(6, 1, 1)
    cx[9].wait_recv()
    gather_x_loop(7, 1, 1)

    lwg.wait()
    lwu.wait()
    lwd.wait()

    def forward(l, carry):
        rows = xg[:, pl.ds(l, 1)].reshape(T, D)
        u = dot(rows, wg[l]).astype(BF16)
        v = dot(rows, wu[l]).astype(BF16)
        us[l] = u
        vs[l] = v
        uf = u.astype(F32)
        h = (uf * jax.nn.sigmoid(uf) * v.astype(F32)).astype(BF16)
        o = dot(h, wd[l]).astype(BF16)
        os_[:, pl.ds(l, 1)] = o.reshape(8, 1, CAP, D)
        return carry

    lax.fori_loop(0, NE // 2, forward, 0)
    cy[1].wait_recv()
    cy[5].start()
    cy[3].wait_recv()
    cy[6].start()
    lax.fori_loop(NE // 2, NE, forward, 0)

    order = (3, 1, 2, 0)

    def swap_copy(b, buf, h):
        return rc(b + h, os_.at[2 * h + 1], buf.at[h], 1)

    def reduce_copies(b, k):
        lo, hi = pl.ds(0, H), pl.ds(H, H)
        return [
            rc(b + 0, acc.at[k, 3, lo], rd.at[k, 0], 2),
            rc(b + 1, acc.at[k, 3, hi], rd.at[k, 1], 4),
            rc(b + 2, acc.at[k, 1, lo], fr.at[k, 0, lo], 2),
            rc(b + 3, acc.at[k, 2, hi], fr.at[k, 1, hi], 4),
        ] + ([
            rc(b + 4, acc.at[k, 1, hi], fr.at[k, 0, hi], 2),
            rc(b + 5, acc.at[k, 2, lo], fr.at[k, 1, lo], 4),
        ] if k == 0 else [])

    e0 = lax.broadcasted_iota(jnp.int32, (16 * NE, T), 0)
    e1 = lax.broadcasted_iota(jnp.int32, (16 * NE, T), 1) // CAP
    rank_lane = lax.rem(lax.broadcasted_iota(jnp.int32, (T, T), 1), CAP).astype(F32)

    def spread(idx, rows, weighted):
        pick = jnp.where(e0 == e1 + idx * NE, 1.0, 0.0).astype(BF16)
        hit = dot(rt[...], pick) == rank_lane
        if weighted:
            for k in range(3):
                sb[k] = jnp.where(hit, dot(gt[k], pick), 0.0).astype(BF16)
            return dot(sb[0], rows) + dot(sb[1], rows) + dot(sb[2], rows)
        sb[0] = jnp.where(hit, 1.0, 0.0).astype(BF16)
        return dot(sb[0], rows)

    def combine_all(k, b, recv, copies, weighted):
        def one(i, carry):
            h = 3 - i
            acc[k, h] = spread(2 * h, os_[2 * h].reshape(T, D), weighted)
            swap_copy(b, recv, h).wait_recv()
            acc[k, h] = acc[k, h] + spread(8 + h, recv[h].reshape(T, D), weighted)

            @pl.when(i == 0)
            def _():
                copies[0].start()
                copies[1].start()

            @pl.when(i == 1)
            def _():
                copies[3].start()

            @pl.when(i == 2)
            def _():
                copies[2].start()
            return carry
        lax.fori_loop(0, 4, one, 0)

    ro = reduce_copies(RS_O, 0)
    for h in order:
        swap_copy(OX, orv, h).start()
    cy[2].wait_recv()
    cy[7].start()
    cy[4].wait_recv()
    cy[8].start()
    combine_all(0, OX, orv, ro, True)

    cy[5].wait_recv()
    cy[6].wait_recv()
    cy[9].start()
    cy[0].wait_recv()
    cy[7].wait_recv()
    cy[8].wait_recv()
    cy[9].wait_recv()
    for c in cx:
        c.wait_send()

    ggc = [rc(GG + rel - 1, ggs.at[rel], gga.at[rel], rel) for rel in range(1, 8)]

    def gather_dy(d, carry):
        build_p(d)
        rows = dot(pb[...], dya[d])
        outs = os_[d].reshape(T, D).astype(F32)
        gg_rows = jnp.sum(rows * outs, axis=1, keepdims=True)
        r_d = rm[d]
        g_d = gm[d]
        for l in range(NE):
            hit = lane_r == r_d[l:l + 1, :]
            gcol = jnp.sum(jnp.where(hit, g_d[l:l + 1, :], 0.0), axis=1, keepdims=True)
            xa[d, l * CAP:(l + 1) * CAP, :] = (gcol * rows[l * CAP:(l + 1) * CAP, :]).astype(BF16)
            ggs[d, l:l + 1, :] = jnp.sum(
                jnp.where(hit, gg_rows[l * CAP:(l + 1) * CAP, :], 0.0), axis=0, keepdims=True)
        return carry

    lax.fori_loop(0, 8, gather_dy, 0)
    for c in ggc:
        c.start()
    for h in order:
        swap_copy(OX, orv, h).wait_send()

    ro[0].wait_recv()
    acc[0, 2, :H] = acc[0, 2, :H] + rd[0, 0]
    ro[5].start()
    ro[1].wait_recv()
    acc[0, 1, H:] = acc[0, 1, H:] + rd[0, 1]
    ro[4].start()

    def expert_rows(buf, l):
        return buf[:, pl.ds(pl.multiple_of(l * CAP, CAP), CAP), :].reshape(T, D)

    def backward(l, carry):
        dh = dotg(expert_rows(xa, l), wd[l], NT).astype(BF16).astype(F32)
        uf = us[l].astype(F32)
        vf = vs[l].astype(F32)
        s = jax.nn.sigmoid(uf)
        sl = uf * s
        hs[l] = (sl * vf).astype(BF16)
        dv = (dh * sl).astype(BF16)
        du = (dh * vf * (s + sl * (1.0 - s))).astype(BF16)
        us[l] = du
        vs[l] = dv
        pr = (dotg(du, wg[l], NT) + dotg(dv, wu[l], NT)).astype(BF16)
        os_[:, pl.ds(l, 1)] = pr.reshape(8, 1, CAP, D)
        return carry

    lax.fori_loop(0, NE, backward, 0)

    rp = reduce_copies(RS_P, 1)
    for h in order:
        swap_copy(PX, prv, h).start()
    combine_all(1, PX, prv, rp, False)

    def finish_grads(l):
        return [
            pltpu.make_async_copy(swg, dwg_ref.at[l], lsem.at[5]),
            pltpu.make_async_copy(swu, dwu_ref.at[l], lsem.at[6]),
            pltpu.make_async_copy(swd, dwd_ref.at[l], lsem.at[7]),
        ]

    def weight_grads(l, carry):
        rows = xg[:, pl.ds(l, 1)].reshape(T, D)

        @pl.when(l > 0)
        def _():
            for cp in finish_grads(l - 1):
                cp.wait()
        swg[...] = dotg(rows, us[l], TN)
        swu[...] = dotg(rows, vs[l], TN)
        swd[...] = dotg(hs[l], expert_rows(xa, l), TN)
        for cp in finish_grads(l):
            cp.start()
        return carry

    for c in ggc:
        c.wait_recv()
    gga[0] = ggs[0]
    out = [jnp.zeros((1, T), F32) for _ in range(8)]
    for rel in range(8):
        d = dev(rel)
        base = d['row'] * 4 + d['col'] * 2 + d['core']
        ids = sub + base * NE
        part = gga[rel]
        for j in range(8):
            hit = route_ref[j:j + 1, :] == ids
            out[j] = out[j] + jnp.sum(jnp.where(hit, part, 0.0), axis=0, keepdims=True)
    for j in range(8):
        gg_ref[j:j + 1, :] = out[j]

    for i in (2, 3, 4, 5):
        ro[i].wait_recv()
    moe_ref[...] = (acc[0, 0] + fr[0, 0] + fr[0, 1]).astype(BF16)
    lax.fori_loop(0, NE, weight_grads, 0)
    rp[0].wait_recv()
    my_ref[...] = acc[1, 2, :H] + rd[1, 0]
    rp[1].wait_recv()
    mx_ref[...] = acc[1, 1, H:] + rd[1, 1]
    for cp in finish_grads(NE - 1):
        cp.wait()
    for c in rgc + cy + ggc + ro:
        c.wait_send()
    for h in order:
        swap_copy(PX, prv, h).wait_send()
    rp[2].wait_recv()
    base_ref[:H] = acc[1, 0, :H] + fr[1, 0, :H]
    rp[3].wait_recv()
    base_ref[H:] = acc[1, 0, H:] + fr[1, 1, H:]
    for c in rp:
        c.wait_send()


def publish(*refs):
    n = (len(refs) - 2) // 3
    ins, outs, bufs, (sin, sout) = refs[:n], refs[n:2 * n], refs[2 * n:3 * n], refs[3 * n:]
    pieces = []
    for a, o, b in zip(ins, outs, bufs):
        if len(a.shape) == 3:
            pieces += [(a.at[l], o.at[l], b.at[l]) for l in range(a.shape[0])]
        else:
            pieces.append((a, o, b))
    loads = [pltpu.make_async_copy(a, b, sin.at[i]) for i, (a, o, b) in enumerate(pieces)]
    stores = [pltpu.make_async_copy(b, o, sout.at[i]) for i, (a, o, b) in enumerate(pieces)]
    for c in loads:
        c.start()
    for c, w in zip(loads, stores):
        c.wait()
        w.start()
    for w in stores:
        w.wait()


def solution(mesh):
    tok_spec = P(ALL_AXES, None)
    w_spec = P(EP_AXES, None, None)
    gw_spec = P(ALL_AXES, None, None)

    def local_step(tokens, route_idx, gate_vals, w_gate, w_up, w_down, grad_out):
        T, K = route_idx.shape
        D = tokens.shape[1]
        NE, _, FF = w_gate.shape
        CAP = T * K // (8 * NE)
        vm = pl.BlockSpec(memory_space=pltpu.VMEM)
        hbm = pl.BlockSpec(memory_space=pl.ANY)
        sds = jax.ShapeDtypeStruct
        outs = pl.pallas_call(
            functools.partial(kernel, T, D, FF, NE, CAP),
            out_shape=(sds((T, D), BF16), sds((K, T), F32),
                       sds((T, D), F32), sds((T // 2, D), F32), sds((T // 2, D), F32),
                       sds((NE, D, FF), F32), sds((NE, D, FF), F32), sds((NE, FF, D), F32)),
            in_specs=[hbm, hbm, vm, vm, hbm, hbm, hbm],
            out_specs=(vm, vm, vm, vm, vm, hbm, hbm, hbm),
            scratch_shapes=[
                pltpu.VMEM((8, T, D), BF16),
                pltpu.VMEM((8, T, D), BF16),
                pltpu.VMEM((8, NE, CAP, D), BF16),
                pltpu.VMEM((NE, T, FF), BF16),
                pltpu.VMEM((NE, T, FF), BF16),
                pltpu.VMEM((NE, T, FF), BF16),
                pltpu.VMEM((8, NE, CAP, D), BF16),
                pltpu.VMEM((NE, D, FF), BF16),
                pltpu.VMEM((NE, D, FF), BF16),
                pltpu.VMEM((NE, FF, D), BF16),
                pltpu.VMEM((2, 4, T, D), F32),
                pltpu.VMEM((2, 2, T // 2, D), F32),
                pltpu.VMEM((2, 2, T, D), F32),
                pltpu.VMEM((4, NE, CAP, D), BF16),
                pltpu.VMEM((4, NE, CAP, D), BF16),
                pltpu.VMEM((D, FF), F32),
                pltpu.VMEM((D, FF), F32),
                pltpu.VMEM((FF, D), F32),
                pltpu.VMEM((T, T), BF16),
                pltpu.VMEM((3, T, T), BF16),
                pltpu.VMEM((8, K, T), jnp.int32),
                pltpu.VMEM((8, K, T), F32),
                pltpu.VMEM((16, NE, T), F32),
                pltpu.VMEM((16, NE, T), F32),
                pltpu.VMEM((16, NE, T), F32),
                pltpu.VMEM((T, 16 * NE), BF16),
                pltpu.VMEM((3, T, 16 * NE), BF16),
                pltpu.VMEM((8, NE, T), F32),
                pltpu.VMEM((8, NE, T), F32),
                pltpu.SemaphoreType.DMA((N_SEM,)),
                pltpu.SemaphoreType.DMA((N_SEM,)),
                pltpu.SemaphoreType.DMA((8,)),
            ],
            compiler_params=pltpu.CompilerParams(
                collective_id=0, has_side_effects=True, vmem_limit_bytes=67043328),
        )(tokens, grad_out, route_idx.T, gate_vals.T, w_gate, w_up, w_down)
        base, mx, my = outs[2:5]
        rx = lax.ppermute(mx, 'col', [(0, 1), (1, 0)])
        ry = lax.ppermute(my, 'row', [(0, 1), (1, 0)])
        res = outs[:2] + outs[5:]
        n_pieces = 2 + 3 * NE
        moe, gg, dwg, dwu, dwd = pl.pallas_call(
            publish,
            out_shape=tuple(sds(a.shape, a.dtype) for a in res),
            in_specs=[hbm] * 5,
            out_specs=(hbm,) * 5,
            scratch_shapes=[pltpu.VMEM(a.shape, a.dtype) for a in res] + [
                pltpu.SemaphoreType.DMA((n_pieces,)),
                pltpu.SemaphoreType.DMA((n_pieces,)),
            ],
            cost_estimate=pl.CostEstimate(
                flops=2_000_000_000, bytes_accessed=2 * 3 * NE * D * FF * 4, transcendentals=0),
            compiler_params=pltpu.CompilerParams(vmem_limit_bytes=67043328),
        )(*res)
        gx = (base + jnp.concatenate([ry, rx], axis=0)).astype(BF16)
        return moe, gx, gg.T, dwg, dwu, dwd

    return jax.shard_map(
        local_step, mesh=mesh,
        in_specs=(tok_spec, tok_spec, tok_spec, w_spec, w_spec, w_spec, tok_spec),
        out_specs=(tok_spec, tok_spec, tok_spec, gw_spec, gw_spec, gw_spec),
        check_vma=False)
```

```python
import functools

import jax
import jax.numpy as jnp
from jax import lax
from jax.experimental import pallas as pl
from jax.experimental.pallas import tpu as pltpu
from jax.sharding import PartitionSpec as P


EP_AXES = ('row', 'col', 'core')
ALL_AXES = ('part', 'row', 'col', 'core')
MESH = pl.DeviceIdType.MESH
F32 = jnp.float32
BF16 = jnp.bfloat16
NT = (((1,), (1,)), ((), ()))
TN = (((0,), (0,)), ((), ()))

AG_X, AG_DY, RG, OX, PX, RS_O, RS_P, GG, N_SEM = 0, 10, 20, 34, 38, 42, 48, 52, 56


def dot(a, b):
    return jnp.dot(a, b, preferred_element_type=F32)


def dotg(a, b, dims):
    return lax.dot_general(a, b, dims, preferred_element_type=F32)


def kernel(T, D, FF, NE, CAP,
           x_ref, dy_ref, route_ref, gate_ref, wg_ref, wu_ref, wd_ref,
           moe_ref, gg_ref, base_ref, mx_ref, my_ref, dwg_ref, dwu_ref, dwd_ref,
           xa, dya, xg, us, vs, hs, os_, wg, wu, wd, acc, rd, fr, orv, prv,
           swg, swu, swd, pb, sb, ra, ga, rm, gm, mb, rt, gt, gj, gr, gacc, gd, gf,
           ssem, rsem, lsem):
    H = T // 2
    row, col, core = lax.axis_index('row'), lax.axis_index('col'), lax.axis_index('core')
    me = row * 4 + col * 2 + core
    partner = row * 4 + col * 2 + (1 - core)

    def dev(rel):
        return {
            'row': 1 - row if rel & 4 else row,
            'col': 1 - col if rel & 2 else col,
            'core': 1 - core if rel & 1 else core,
        }

    def rc(i, src, dst, rel):
        return pltpu.make_async_remote_copy(
            src_ref=src, dst_ref=dst, send_sem=ssem.at[i], recv_sem=rsem.at[i],
            device_id=dev(rel), device_id_type=MESH)

    def gather_copies(b, buf):
        lo, hi = pl.ds(0, H), pl.ds(H, H)
        return [
            rc(b + 0, buf.at[0], buf.at[1], 1),
            rc(b + 1, buf.at[0, hi], buf.at[2, hi], 2),
            rc(b + 2, buf.at[0, lo], buf.at[2, lo], 2),
            rc(b + 3, buf.at[0, lo], buf.at[4, lo], 4),
            rc(b + 4, buf.at[0, hi], buf.at[4, hi], 4),
            rc(b + 5, buf.at[2, hi], buf.at[6, hi], 4),
            rc(b + 6, buf.at[4, lo], buf.at[6, lo], 2),
            rc(b + 7, buf.at[2], buf.at[3], 1),
            rc(b + 8, buf.at[4], buf.at[5], 1),
            rc(b + 9, buf.at[6], buf.at[7], 1),
        ]

    lx = pltpu.make_async_copy(x_ref, xa.at[0], lsem.at[0])
    ldy = pltpu.make_async_copy(dy_ref, dya.at[0], lsem.at[1])
    lwg = pltpu.make_async_copy(wg_ref, wg, lsem.at[2])
    lwu = pltpu.make_async_copy(wu_ref, wu, lsem.at[3])
    lwd = pltpu.make_async_copy(wd_ref, wd, lsem.at[4])
    lx.start()
    ldy.start()
    lwg.start()
    lwu.start()
    lwd.start()

    barrier = pltpu.get_barrier_semaphore()
    for rel in (1, 2, 4):
        pl.semaphore_signal(barrier, inc=1, device_id=dev(rel), device_id_type=MESH)
    pl.semaphore_wait(barrier, 3)

    def small_copies(b, src, buf, diag):
        return [
            rc(b + 0, src, buf.at[1], 1),
            rc(b + 1, src, buf.at[2], 2),
            rc(b + 2, src, buf.at[4], 4),
            rc(b + 3, buf.at[6 - diag], buf.at[6], diag),
            rc(b + 4, buf.at[2], buf.at[3], 1),
            rc(b + 5, buf.at[4], buf.at[5], 1),
            rc(b + 6, buf.at[6], buf.at[7], 1),
        ]

    cr = small_copies(RG, route_ref, ra, 2)
    cg = small_copies(RG + 7, gate_ref, ga, 4)
    cx = gather_copies(AG_X, xa)
    cy = gather_copies(AG_DY, dya)
    for i in (1, 2, 0):
        cr[i].start()
        cg[i].start()
    lx.wait()
    for i in (1, 3, 0):
        cx[i].start()
    cr[2].wait_recv()
    cr[3].start()
    cg[1].wait_recv()
    cg[3].start()
    cx[2].start()
    cx[4].start()
    cr[5].start()
    cg[4].start()
    cr[1].wait_recv()
    cr[4].start()
    cg[2].wait_recv()
    cg[5].start()
    ra[0] = route_ref[...]
    ga[0] = gate_ref[...]

    i0 = lax.broadcasted_iota(jnp.int32, (T, T), 0)
    i1 = lax.broadcasted_iota(jnp.int32, (T, T), 1)
    sb[0] = (i0 < i1).astype(F32).astype(BF16)
    sb[1] = (i0 > i1).astype(F32).astype(BF16)
    sb[2] = (i0 == i1).astype(F32).astype(BF16)
    cx[1].wait_recv()
    cx[5].start()
    cx[3].wait_recv()
    cx[6].start()
    cr[3].wait_recv()
    cr[6].start()
    cg[3].wait_recv()
    cg[6].start()
    for i in (0, 4, 5, 6):
        cr[i].wait_recv()
        cg[i].wait_recv()
    mb[...] = jnp.zeros_like(mb)
    gm[...] = jnp.zeros_like(gm)
    sub = lax.broadcasted_iota(jnp.int32, (NE, T), 0)
    for idx in range(12):
        src = idx if idx < 8 else 2 * (idx - 8)
        owner = me if idx < 8 else partner
        ids = sub + owner * NE
        hits = jnp.zeros((NE, T), F32)
        gates = jnp.zeros((NE, T), F32)
        for j in range(8):
            hit = ra[src, j:j + 1, :] == ids
            hits = hits + jnp.where(hit, 1.0, 0.0)
            gates = gates + jnp.where(hit, ga[src, j:j + 1, :], 0.0)
        mb[idx] = hits
        gm[idx] = gates
    m_all = mb[...].reshape(16 * NE, T)
    m_bf = m_all.astype(BF16)
    ranks = dot(m_bf, sb[0])
    rm[...] = jnp.where(m_all > 0.5, ranks, -1.0).reshape(16, NE, T)
    m_t = dotg(sb[2], m_bf, NT)
    r_t = dotg(sb[1], m_bf, NT)
    rt[...] = jnp.where(m_t > 0.5, r_t, -1.0).astype(BF16)
    g_all = gm[...].reshape(16 * NE, T)
    g_hi = g_all.astype(BF16)
    rest = g_all - g_hi.astype(F32)
    g_mid = rest.astype(BF16)
    g_lo = (rest - g_mid.astype(F32)).astype(BF16)
    for k, piece in enumerate((g_hi, g_mid, g_lo)):
        gt[k] = dotg(sb[2], piece, NT).astype(BF16)

    lane_r = lax.broadcasted_iota(jnp.int32, (CAP, T), 0).astype(F32)

    def build_p(d):
        r_d = rm[d]
        for l in range(NE):
            pb[l * CAP:(l + 1) * CAP, :] = jnp.where(lane_r == r_d[l:l + 1, :], 1.0, 0.0).astype(BF16)

    def gather_x(d):
        build_p(d)
        xg[d] = dot(pb[...], xa[d]).astype(BF16).reshape(NE, CAP, D)

    def gather_x_loop(first, step, count):
        def one(i, carry):
            gather_x(first + step * i)
            return carry
        lax.fori_loop(0, count, one, 0)

    cx[0].wait_recv()
    gather_x_loop(0, 1, 2)
    cx[2].wait_recv()
    cx[7].start()
    cx[4].wait_recv()
    cx[8].start()
    ldy.wait()
    for i in (1, 3, 0, 2, 4):
        cy[i].start()
    gather_x_loop(2, 2, 2)
    cx[7].wait_recv()
    cx[8].wait_recv()
    gather_x_loop(3, 2, 2)
    cx[5].wait_recv()
    cx[6].wait_recv()
    cx[9].start()
    gather_x_loop(6, 1, 1)
    cx[9].wait_recv()
    gather_x_loop(7, 1, 1)

    lwg.wait()
    lwu.wait()
    lwd.wait()

    def forward(l, carry):
        rows = xg[:, pl.ds(l, 1)].reshape(T, D)
        u = dot(rows, wg[l]).astype(BF16)
        v = dot(rows, wu[l]).astype(BF16)
        us[l] = u
        vs[l] = v
        uf = u.astype(F32)
        h = (uf * jax.nn.sigmoid(uf) * v.astype(F32)).astype(BF16)
        o = dot(h, wd[l]).astype(BF16)
        os_[:, pl.ds(l, 1)] = o.reshape(8, 1, CAP, D)
        return carry

    lax.fori_loop(0, NE // 2, forward, 0)
    cy[1].wait_recv()
    cy[5].start()
    cy[3].wait_recv()
    cy[6].start()
    lax.fori_loop(NE // 2, NE, forward, 0)

    order = (3, 1, 2, 0)

    def swap_copy(b, buf, h):
        return rc(b + h, os_.at[2 * h + 1], buf.at[h], 1)

    def reduce_copies(b, k):
        lo, hi = pl.ds(0, H), pl.ds(H, H)
        return [
            rc(b + 0, acc.at[k, 3, lo], rd.at[k, 0], 2),
            rc(b + 1, acc.at[k, 3, hi], rd.at[k, 1], 4),
            rc(b + 2, acc.at[k, 1, lo], fr.at[k, 0, lo], 2),
            rc(b + 3, acc.at[k, 2, hi], fr.at[k, 1, hi], 4),
        ] + ([
            rc(b + 4, acc.at[k, 1, hi], fr.at[k, 0, hi], 2),
            rc(b + 5, acc.at[k, 2, lo], fr.at[k, 1, lo], 4),
        ] if k == 0 else [])

    e0 = lax.broadcasted_iota(jnp.int32, (16 * NE, T), 0)
    e1 = lax.broadcasted_iota(jnp.int32, (16 * NE, T), 1) // CAP
    rank_lane = lax.rem(lax.broadcasted_iota(jnp.int32, (T, T), 1), CAP).astype(F32)

    def spread(idx, rows, weighted):
        pick = jnp.where(e0 == e1 + idx * NE, 1.0, 0.0).astype(BF16)
        hit = dot(rt[...], pick) == rank_lane
        if weighted:
            for k in range(3):
                sb[k] = jnp.where(hit, dot(gt[k], pick), 0.0).astype(BF16)
            return dot(sb[0], rows) + dot(sb[1], rows) + dot(sb[2], rows)
        sb[0] = jnp.where(hit, 1.0, 0.0).astype(BF16)
        return dot(sb[0], rows)

    def combine_all(k, b, recv, copies, weighted):
        def one(i, carry):
            h = 3 - i
            acc[k, h] = spread(2 * h, os_[2 * h].reshape(T, D), weighted)
            swap_copy(b, recv, h).wait_recv()
            acc[k, h] = acc[k, h] + spread(8 + h, recv[h].reshape(T, D), weighted)

            @pl.when(i == 0)
            def _():
                copies[0].start()
                copies[1].start()

            @pl.when(i == 1)
            def _():
                copies[3].start()

            @pl.when(i == 2)
            def _():
                copies[2].start()
            return carry
        lax.fori_loop(0, 4, one, 0)

    ro = reduce_copies(RS_O, 0)
    for h in order:
        swap_copy(OX, orv, h).start()
    cy[2].wait_recv()
    cy[7].start()
    cy[4].wait_recv()
    cy[8].start()
    combine_all(0, OX, orv, ro, True)

    cy[5].wait_recv()
    cy[6].wait_recv()
    cy[9].start()
    cy[0].wait_recv()
    cy[7].wait_recv()
    cy[8].wait_recv()
    cy[9].wait_recv()
    for c in cx:
        c.wait_send()

    swap_gg = rc(GG, gj.at[1], gr, 1)
    gg_diag = rc(GG + 1, gacc.at[3], gd, 4)
    gg_y = rc(GG + 2, gacc.at[2], gf.at[1], 4)
    gg_x = rc(GG + 3, gacc.at[1], gf.at[0], 2)

    def gather_dy(d, carry):
        build_p(d)
        rows = dot(pb[...], dya[d])
        outs = os_[d].reshape(T, D).astype(F32)
        gg_rows = jnp.sum(rows * outs, axis=1, keepdims=True)
        r_d = rm[d]
        g_d = gm[d]
        r_ids = ra[d]
        gg_d = jnp.zeros((8, T), F32)
        for l in range(NE):
            hit = lane_r == r_d[l:l + 1, :]
            gcol = jnp.sum(jnp.where(hit, g_d[l:l + 1, :], 0.0), axis=1, keepdims=True)
            xa[d, l * CAP:(l + 1) * CAP, :] = (gcol * rows[l * CAP:(l + 1) * CAP, :]).astype(BF16)
            gg_l = jnp.sum(
                jnp.where(hit, gg_rows[l * CAP:(l + 1) * CAP, :], 0.0), axis=0, keepdims=True)
            gg_d = gg_d + jnp.where(r_ids == me * NE + l, gg_l, 0.0)
        gj[lax.rem(d, 2), d // 2] = gg_d
        return carry

    lax.fori_loop(0, 8, gather_dy, 0)
    swap_gg.start()
    for h in order:
        swap_copy(OX, orv, h).wait_send()

    ro[0].wait_recv()
    acc[0, 2, :H] = acc[0, 2, :H] + rd[0, 0]
    ro[5].start()
    ro[1].wait_recv()
    acc[0, 1, H:] = acc[0, 1, H:] + rd[0, 1]
    ro[4].start()
    swap_gg.wait_recv()
    gacc[...] = gj[0] + gr[...]

    def expert_rows(buf, l):
        return buf[:, pl.ds(pl.multiple_of(l * CAP, CAP), CAP), :].reshape(T, D)

    def backward(l, carry):
        dh = dotg(expert_rows(xa, l), wd[l], NT).astype(BF16).astype(F32)
        uf = us[l].astype(F32)
        vf = vs[l].astype(F32)
        s = jax.nn.sigmoid(uf)
        sl = uf * s
        hs[l] = (sl * vf).astype(BF16)
        dv = (dh * sl).astype(BF16)
        du = (dh * vf * (s + sl * (1.0 - s))).astype(BF16)
        us[l] = du
        vs[l] = dv
        pr = (dotg(du, wg[l], NT) + dotg(dv, wu[l], NT)).astype(BF16)
        os_[:, pl.ds(l, 1)] = pr.reshape(8, 1, CAP, D)
        return carry

    gg_diag.start()
    gg_y.start()
    lax.fori_loop(0, NE, backward, 0)
    gg_diag.wait_recv()
    gacc[1] = gacc[1] + gd[...]

    rp = reduce_copies(RS_P, 1)
    for h in order:
        swap_copy(PX, prv, h).start()
    combine_all(1, PX, prv, rp, False)

    def finish_grads(l):
        return [
            pltpu.make_async_copy(swg, dwg_ref.at[l], lsem.at[5]),
            pltpu.make_async_copy(swu, dwu_ref.at[l], lsem.at[6]),
            pltpu.make_async_copy(swd, dwd_ref.at[l], lsem.at[7]),
        ]

    def weight_grads(l, carry):
        rows = xg[:, pl.ds(l, 1)].reshape(T, D)

        @pl.when(l > 0)
        def _():
            for cp in finish_grads(l - 1):
                cp.wait()
        swg[...] = dotg(rows, us[l], TN)
        swu[...] = dotg(rows, vs[l], TN)
        swd[...] = dotg(hs[l], expert_rows(xa, l), TN)
        for cp in finish_grads(l):
            cp.start()
        return carry

    gg_x.start()
    for i in (2, 3, 4, 5):
        ro[i].wait_recv()
    moe_ref[...] = (acc[0, 0] + fr[0, 0] + fr[0, 1]).astype(BF16)
    lax.fori_loop(0, NE, weight_grads, 0)
    rp[0].wait_recv()
    my_ref[...] = acc[1, 2, :H] + rd[1, 0]
    rp[1].wait_recv()
    mx_ref[...] = acc[1, 1, H:] + rd[1, 1]
    for cp in finish_grads(NE - 1):
        cp.wait()
    gg_x.wait_recv()
    gg_y.wait_recv()
    gg_ref[...] = gacc[0] + gf[0] + gf[1]
    for c in cr + cg + cy + ro + [swap_gg, gg_diag, gg_y, gg_x]:
        c.wait_send()
    for h in order:
        swap_copy(PX, prv, h).wait_send()
    rp[2].wait_recv()
    base_ref[:H] = acc[1, 0, :H] + fr[1, 0, :H]
    rp[3].wait_recv()
    base_ref[H:] = acc[1, 0, H:] + fr[1, 1, H:]
    for c in rp:
        c.wait_send()


def publish(*refs):
    n = (len(refs) - 2) // 3
    ins, outs, bufs, (sin, sout) = refs[:n], refs[n:2 * n], refs[2 * n:3 * n], refs[3 * n:]
    pieces = []
    for a, o, b in zip(ins, outs, bufs):
        if len(a.shape) == 3:
            pieces += [(a.at[l], o.at[l], b.at[l]) for l in range(a.shape[0])]
        else:
            pieces.append((a, o, b))
    loads = [pltpu.make_async_copy(a, b, sin.at[i]) for i, (a, o, b) in enumerate(pieces)]
    stores = [pltpu.make_async_copy(b, o, sout.at[i]) for i, (a, o, b) in enumerate(pieces)]
    for c in loads:
        c.start()
    for c, w in zip(loads, stores):
        c.wait()
        w.start()
    for w in stores:
        w.wait()


def solution(mesh):
    tok_spec = P(ALL_AXES, None)
    w_spec = P(EP_AXES, None, None)
    gw_spec = P(ALL_AXES, None, None)

    def local_step(tokens, route_idx, gate_vals, w_gate, w_up, w_down, grad_out):
        T, K = route_idx.shape
        D = tokens.shape[1]
        NE, _, FF = w_gate.shape
        CAP = T * K // (8 * NE)
        vm = pl.BlockSpec(memory_space=pltpu.VMEM)
        hbm = pl.BlockSpec(memory_space=pl.ANY)
        sds = jax.ShapeDtypeStruct
        outs = pl.pallas_call(
            functools.partial(kernel, T, D, FF, NE, CAP),
            out_shape=(sds((T, D), BF16), sds((K, T), F32),
                       sds((T, D), F32), sds((T // 2, D), F32), sds((T // 2, D), F32),
                       sds((NE, D, FF), F32), sds((NE, D, FF), F32), sds((NE, FF, D), F32)),
            in_specs=[hbm, hbm, vm, vm, hbm, hbm, hbm],
            out_specs=(vm, vm, vm, vm, vm, hbm, hbm, hbm),
            scratch_shapes=[
                pltpu.VMEM((8, T, D), BF16),
                pltpu.VMEM((8, T, D), BF16),
                pltpu.VMEM((8, NE, CAP, D), BF16),
                pltpu.VMEM((NE, T, FF), BF16),
                pltpu.VMEM((NE, T, FF), BF16),
                pltpu.VMEM((NE, T, FF), BF16),
                pltpu.VMEM((8, NE, CAP, D), BF16),
                pltpu.VMEM((NE, D, FF), BF16),
                pltpu.VMEM((NE, D, FF), BF16),
                pltpu.VMEM((NE, FF, D), BF16),
                pltpu.VMEM((2, 4, T, D), F32),
                pltpu.VMEM((2, 2, T // 2, D), F32),
                pltpu.VMEM((2, 2, T, D), F32),
                pltpu.VMEM((4, NE, CAP, D), BF16),
                pltpu.VMEM((4, NE, CAP, D), BF16),
                pltpu.VMEM((D, FF), F32),
                pltpu.VMEM((D, FF), F32),
                pltpu.VMEM((FF, D), F32),
                pltpu.VMEM((T, T), BF16),
                pltpu.VMEM((3, T, T), BF16),
                pltpu.VMEM((8, K, T), jnp.int32),
                pltpu.VMEM((8, K, T), F32),
                pltpu.VMEM((16, NE, T), F32),
                pltpu.VMEM((16, NE, T), F32),
                pltpu.VMEM((16, NE, T), F32),
                pltpu.VMEM((T, 16 * NE), BF16),
                pltpu.VMEM((3, T, 16 * NE), BF16),
                pltpu.VMEM((2, 4, K, T), F32),
                pltpu.VMEM((4, K, T), F32),
                pltpu.VMEM((4, K, T), F32),
                pltpu.VMEM((K, T), F32),
                pltpu.VMEM((2, K, T), F32),
                pltpu.SemaphoreType.DMA((N_SEM,)),
                pltpu.SemaphoreType.DMA((N_SEM,)),
                pltpu.SemaphoreType.DMA((8,)),
            ],
            compiler_params=pltpu.CompilerParams(
                collective_id=0, has_side_effects=True, vmem_limit_bytes=67043328),
        )(tokens, grad_out, route_idx.T, gate_vals.T, w_gate, w_up, w_down)
        base, mx, my = outs[2:5]
        rx = lax.ppermute(mx, 'col', [(0, 1), (1, 0)])
        ry = lax.ppermute(my, 'row', [(0, 1), (1, 0)])
        res = outs[:2] + outs[5:]
        n_pieces = 2 + 3 * NE
        moe, gg, dwg, dwu, dwd = pl.pallas_call(
            publish,
            out_shape=tuple(sds(a.shape, a.dtype) for a in res),
            in_specs=[hbm] * 5,
            out_specs=(hbm,) * 5,
            scratch_shapes=[pltpu.VMEM(a.shape, a.dtype) for a in res] + [
                pltpu.SemaphoreType.DMA((n_pieces,)),
                pltpu.SemaphoreType.DMA((n_pieces,)),
            ],
            cost_estimate=pl.CostEstimate(
                flops=2_000_000_000, bytes_accessed=2 * 3 * NE * D * FF * 4, transcendentals=0),
            compiler_params=pltpu.CompilerParams(vmem_limit_bytes=60 * 1024 * 1024),
        )(*res)
        gx = (base + jnp.concatenate([ry, rx], axis=0)).astype(BF16)
        return moe, gx, gg.T, dwg, dwu, dwd

    return jax.shard_map(
        local_step, mesh=mesh,
        in_specs=(tok_spec, tok_spec, tok_spec, w_spec, w_spec, w_spec, tok_spec),
        out_specs=(tok_spec, tok_spec, tok_spec, gw_spec, gw_spec, gw_spec),
        check_vma=False)
```

```python
import functools

import jax
import jax.numpy as jnp
from jax import lax
from jax.experimental import pallas as pl
from jax.experimental.pallas import tpu as pltpu
from jax.sharding import PartitionSpec as P


EP_AXES = ('row', 'col', 'core')
ALL_AXES = ('part', 'row', 'col', 'core')
MESH = pl.DeviceIdType.MESH
F32 = jnp.float32
BF16 = jnp.bfloat16
NT = (((1,), (1,)), ((), ()))
TN = (((0,), (0,)), ((), ()))

AG_X, AG_DY, RG, OX, PX, RS_O, RS_P, GG, N_SEM = 0, 10, 20, 34, 38, 42, 48, 50, 54


def dot(a, b):
    return jnp.dot(a, b, preferred_element_type=F32)


def dotg(a, b, dims):
    return lax.dot_general(a, b, dims, preferred_element_type=F32)


def kernel(T, D, FF, NE, CAP,
           x_ref, dy_ref, route_ref, gate_ref, wg_ref, wu_ref, wd_ref,
           moe_ref, gg_ref, base_ref, mx_ref, my_ref, dwg_ref, dwu_ref, dwd_ref,
           xa, dya, xg, us, vs, hs, os_, wg, wu, wd, acc, rd, fr, orv, prv,
           swg, swu, swd, pb, sb, ra, ga, rm, gm, mb, rt, gt, gj, gr, gacc, gd, gf, moe_sc,
           ssem, rsem, lsem):
    H = T // 2
    row, col, core = lax.axis_index('row'), lax.axis_index('col'), lax.axis_index('core')
    me = row * 4 + col * 2 + core
    partner = row * 4 + col * 2 + (1 - core)

    def dev(rel):
        return {
            'row': 1 - row if rel & 4 else row,
            'col': 1 - col if rel & 2 else col,
            'core': 1 - core if rel & 1 else core,
        }

    def rc(i, src, dst, rel):
        return pltpu.make_async_remote_copy(
            src_ref=src, dst_ref=dst, send_sem=ssem.at[i], recv_sem=rsem.at[i],
            device_id=dev(rel), device_id_type=MESH)

    def gather_copies(b, buf):
        lo, hi = pl.ds(0, H), pl.ds(H, H)
        return [
            rc(b + 0, buf.at[0], buf.at[1], 1),
            rc(b + 1, buf.at[0, hi], buf.at[2, hi], 2),
            rc(b + 2, buf.at[0, lo], buf.at[2, lo], 2),
            rc(b + 3, buf.at[0, lo], buf.at[4, lo], 4),
            rc(b + 4, buf.at[0, hi], buf.at[4, hi], 4),
            rc(b + 5, buf.at[2, hi], buf.at[6, hi], 4),
            rc(b + 6, buf.at[4, lo], buf.at[6, lo], 2),
            rc(b + 7, buf.at[2], buf.at[3], 1),
            rc(b + 8, buf.at[4], buf.at[5], 1),
            rc(b + 9, buf.at[6], buf.at[7], 1),
        ]

    lx = pltpu.make_async_copy(x_ref, xa.at[0], lsem.at[0])
    ldy = pltpu.make_async_copy(dy_ref, dya.at[0], lsem.at[1])
    lwg = pltpu.make_async_copy(wg_ref, wg, lsem.at[2])
    lwu = pltpu.make_async_copy(wu_ref, wu, lsem.at[3])
    lwd = pltpu.make_async_copy(wd_ref, wd, lsem.at[4])
    lx.start()
    ldy.start()
    lwg.start()
    lwu.start()
    lwd.start()

    barrier = pltpu.get_barrier_semaphore()
    for rel in (1, 2, 4):
        pl.semaphore_signal(barrier, inc=1, device_id=dev(rel), device_id_type=MESH)
    pl.semaphore_wait(barrier, 3)

    def small_copies(b, src, buf, diag):
        return [
            rc(b + 0, src, buf.at[1], 1),
            rc(b + 1, src, buf.at[2], 2),
            rc(b + 2, src, buf.at[4], 4),
            rc(b + 3, buf.at[6 - diag], buf.at[6], diag),
            rc(b + 4, buf.at[2], buf.at[3], 1),
            rc(b + 5, buf.at[4], buf.at[5], 1),
            rc(b + 6, buf.at[6], buf.at[7], 1),
        ]

    cr = small_copies(RG, route_ref, ra, 2)
    cg = small_copies(RG + 7, gate_ref, ga, 4)
    cx = gather_copies(AG_X, xa)
    cy = gather_copies(AG_DY, dya)
    for i in (1, 2, 0):
        cr[i].start()
        cg[i].start()
    lx.wait()
    for i in (1, 3, 0):
        cx[i].start()
    cr[2].wait_recv()
    cr[3].start()
    cg[1].wait_recv()
    cg[3].start()
    cx[2].start()
    cx[4].start()
    cr[5].start()
    cg[4].start()
    cr[1].wait_recv()
    cr[4].start()
    cg[2].wait_recv()
    cg[5].start()
    ra[0] = route_ref[...]
    ga[0] = gate_ref[...]

    i0 = lax.broadcasted_iota(jnp.int32, (T, T), 0)
    i1 = lax.broadcasted_iota(jnp.int32, (T, T), 1)
    sb[0] = (i0 < i1).astype(F32).astype(BF16)
    sb[1] = (i0 > i1).astype(F32).astype(BF16)
    sb[2] = (i0 == i1).astype(F32).astype(BF16)
    cx[1].wait_recv()
    cx[5].start()
    cx[3].wait_recv()
    cx[6].start()
    cr[3].wait_recv()
    cr[6].start()
    cg[3].wait_recv()
    cg[6].start()
    for i in (0, 4, 5, 6):
        cr[i].wait_recv()
        cg[i].wait_recv()
    mb[...] = jnp.zeros_like(mb)
    gm[...] = jnp.zeros_like(gm)
    sub = lax.broadcasted_iota(jnp.int32, (NE, T), 0)
    for idx in range(12):
        src = idx if idx < 8 else 2 * (idx - 8)
        owner = me if idx < 8 else partner
        ids = sub + owner * NE
        hits = jnp.zeros((NE, T), F32)
        gates = jnp.zeros((NE, T), F32)
        for j in range(8):
            hit = ra[src, j:j + 1, :] == ids
            hits = hits + jnp.where(hit, 1.0, 0.0)
            gates = gates + jnp.where(hit, ga[src, j:j + 1, :], 0.0)
        mb[idx] = hits
        gm[idx] = gates
    m_all = mb[...].reshape(16 * NE, T)
    m_bf = m_all.astype(BF16)
    ranks = dot(m_bf, sb[0])
    rm[...] = jnp.where(m_all > 0.5, ranks, -1.0).reshape(16, NE, T)
    m_t = dotg(sb[2], m_bf, NT)
    r_t = dotg(sb[1], m_bf, NT)
    rt[...] = jnp.where(m_t > 0.5, r_t, -1.0).astype(BF16)
    g_all = gm[...].reshape(16 * NE, T)
    g_hi = g_all.astype(BF16)
    rest = g_all - g_hi.astype(F32)
    g_mid = rest.astype(BF16)
    g_lo = (rest - g_mid.astype(F32)).astype(BF16)
    for k, piece in enumerate((g_hi, g_mid, g_lo)):
        gt[k] = dotg(sb[2], piece, NT).astype(BF16)

    lane_r = lax.broadcasted_iota(jnp.int32, (CAP, T), 0).astype(F32)

    def build_p(d):
        r_d = rm[d]
        for l in range(NE):
            pb[l * CAP:(l + 1) * CAP, :] = jnp.where(lane_r == r_d[l:l + 1, :], 1.0, 0.0).astype(BF16)

    def gather_x(d):
        build_p(d)
        xg[d] = dot(pb[...], xa[d]).astype(BF16).reshape(NE, CAP, D)

    def gather_x_loop(first, step, count):
        def one(i, carry):
            gather_x(first + step * i)
            return carry
        lax.fori_loop(0, count, one, 0)

    cx[0].wait_recv()
    gather_x_loop(0, 1, 2)
    cx[2].wait_recv()
    cx[7].start()
    cx[4].wait_recv()
    cx[8].start()
    ldy.wait()
    for i in (1, 3, 0, 2, 4):
        cy[i].start()
    gather_x_loop(2, 2, 2)
    cx[7].wait_recv()
    cx[8].wait_recv()
    gather_x_loop(3, 2, 2)
    cx[5].wait_recv()
    cx[6].wait_recv()
    cx[9].start()
    gather_x_loop(6, 1, 1)
    cx[9].wait_recv()
    gather_x_loop(7, 1, 1)

    lwg.wait()
    lwu.wait()
    lwd.wait()

    def forward(l, carry):
        rows = xg[:, pl.ds(l, 1)].reshape(T, D)
        u = dot(rows, wg[l]).astype(BF16)
        v = dot(rows, wu[l]).astype(BF16)
        us[l] = u
        vs[l] = v
        uf = u.astype(F32)
        h = (uf * jax.nn.sigmoid(uf) * v.astype(F32)).astype(BF16)
        o = dot(h, wd[l]).astype(BF16)
        os_[:, pl.ds(l, 1)] = o.reshape(8, 1, CAP, D)
        return carry

    lax.fori_loop(0, NE // 2, forward, 0)
    cy[1].wait_recv()
    cy[5].start()
    cy[3].wait_recv()
    cy[6].start()
    lax.fori_loop(NE // 2, NE, forward, 0)

    order = (3, 1, 2, 0)

    def swap_copy(b, buf, h):
        return rc(b + h, os_.at[2 * h + 1], buf.at[h], 1)

    def reduce_copies(b, k):
        lo, hi = pl.ds(0, H), pl.ds(H, H)
        return [
            rc(b + 0, acc.at[k, 3, lo], rd.at[k, 0], 2),
            rc(b + 1, acc.at[k, 3, hi], rd.at[k, 1], 4),
            rc(b + 2, acc.at[k, 1, lo], fr.at[0, lo], 2),
            rc(b + 3, acc.at[k, 2, hi], fr.at[1, hi], 4),
            rc(b + 4, acc.at[k, 1, hi], fr.at[0, hi], 2),
            rc(b + 5, acc.at[k, 2, lo], fr.at[1, lo], 4),
        ][:6 if k == 0 else 2]

    e0 = lax.broadcasted_iota(jnp.int32, (16 * NE, T), 0)
    e1 = lax.broadcasted_iota(jnp.int32, (16 * NE, T), 1) // CAP
    rank_lane = lax.rem(lax.broadcasted_iota(jnp.int32, (T, T), 1), CAP).astype(F32)

    def spread(idx, rows, weighted):
        pick = jnp.where(e0 == e1 + idx * NE, 1.0, 0.0).astype(BF16)
        hit = dot(rt[...], pick) == rank_lane
        if weighted:
            for k in range(3):
                sb[k] = jnp.where(hit, dot(gt[k], pick), 0.0).astype(BF16)
            return dot(sb[0], rows) + dot(sb[1], rows) + dot(sb[2], rows)
        sb[0] = jnp.where(hit, 1.0, 0.0).astype(BF16)
        return dot(sb[0], rows)

    def combine_all(k, b, recv, copies, weighted):
        def one(i, carry):
            h = 3 - i
            acc[k, h] = spread(2 * h, os_[2 * h].reshape(T, D), weighted)
            swap_copy(b, recv, h).wait_recv()
            acc[k, h] = acc[k, h] + spread(8 + h, recv[h].reshape(T, D), weighted)

            @pl.when(i == 0)
            def _():
                copies[0].start()
                copies[1].start()

            if k == 0:
                @pl.when(i == 1)
                def _():
                    copies[3].start()

                @pl.when(i == 2)
                def _():
                    copies[2].start()
            return carry
        lax.fori_loop(0, 4, one, 0)

    ro = reduce_copies(RS_O, 0)
    for h in order:
        swap_copy(OX, orv, h).start()
    cy[2].wait_recv()
    cy[7].start()
    cy[4].wait_recv()
    cy[8].start()
    combine_all(0, OX, orv, ro, True)

    cy[5].wait_recv()
    cy[6].wait_recv()
    cy[9].start()
    cy[0].wait_recv()
    cy[7].wait_recv()
    cy[8].wait_recv()
    cy[9].wait_recv()
    for c in cx:
        c.wait_send()

    swap_gg = rc(GG, gj.at[1], gr, 1)
    gg_diag = rc(GG + 1, gacc.at[3], gd, 4)
    gg_y = rc(GG + 2, gacc.at[2], gf.at[1], 4)
    gg_x = rc(GG + 3, gacc.at[1], gf.at[0], 2)

    def gather_dy(d, carry):
        build_p(d)
        rows = dot(pb[...], dya[d])
        outs = os_[d].reshape(T, D).astype(F32)
        gg_rows = jnp.sum(rows * outs, axis=1, keepdims=True)
        r_d = rm[d]
        g_d = gm[d]
        r_ids = ra[d]
        gg_d = jnp.zeros((8, T), F32)
        for l in range(NE):
            hit = lane_r == r_d[l:l + 1, :]
            gcol = jnp.sum(jnp.where(hit, g_d[l:l + 1, :], 0.0), axis=1, keepdims=True)
            xa[d, l * CAP:(l + 1) * CAP, :] = (gcol * rows[l * CAP:(l + 1) * CAP, :]).astype(BF16)
            gg_l = jnp.sum(
                jnp.where(hit, gg_rows[l * CAP:(l + 1) * CAP, :], 0.0), axis=0, keepdims=True)
            gg_d = gg_d + jnp.where(r_ids == me * NE + l, gg_l, 0.0)
        gj[lax.rem(d, 2), d // 2] = gg_d
        return carry

    lax.fori_loop(0, 8, gather_dy, 0)
    swap_gg.start()
    for h in order:
        swap_copy(OX, orv, h).wait_send()

    ro[0].wait_recv()
    acc[0, 2, :H] = acc[0, 2, :H] + rd[0, 0]
    ro[5].start()
    ro[1].wait_recv()
    acc[0, 1, H:] = acc[0, 1, H:] + rd[0, 1]
    ro[4].start()
    swap_gg.wait_recv()
    gacc[...] = gj[0] + gr[...]

    def expert_rows(buf, l):
        return buf[:, pl.ds(pl.multiple_of(l * CAP, CAP), CAP), :].reshape(T, D)

    def backward(l, carry):
        dh = dotg(expert_rows(xa, l), wd[l], NT).astype(BF16).astype(F32)
        uf = us[l].astype(F32)
        vf = vs[l].astype(F32)
        s = jax.nn.sigmoid(uf)
        sl = uf * s
        hs[l] = (sl * vf).astype(BF16)
        dv = (dh * sl).astype(BF16)
        du = (dh * vf * (s + sl * (1.0 - s))).astype(BF16)
        us[l] = du
        vs[l] = dv
        pr = (dotg(du, wg[l], NT) + dotg(dv, wu[l], NT)).astype(BF16)
        os_[:, pl.ds(l, 1)] = pr.reshape(8, 1, CAP, D)
        return carry

    gg_diag.start()
    gg_y.start()
    lax.fori_loop(0, NE, backward, 0)
    gg_diag.wait_recv()
    gacc[1] = gacc[1] + gd[...]

    rp = reduce_copies(RS_P, 1)
    for h in order:
        swap_copy(PX, prv, h).start()
    combine_all(1, PX, prv, rp, False)

    def finish_grads(l):
        slot = lax.rem(l, 2)
        return [
            pltpu.make_async_copy(swg.at[slot], dwg_ref.at[l], lsem.at[5 + 9 * slot]),
            pltpu.make_async_copy(swu.at[slot], dwu_ref.at[l], lsem.at[6 + 9 * slot]),
            pltpu.make_async_copy(swd.at[slot], dwd_ref.at[l], lsem.at[7 + 9 * slot]),
        ]

    def weight_grads(l, carry):
        rows = xg[:, pl.ds(l, 1)].reshape(T, D)
        slot = lax.rem(l, 2)

        @pl.when(l > 1)
        def _():
            for cp in finish_grads(l - 2):
                cp.wait()
        swg[slot] = dotg(rows, us[l], TN)
        swu[slot] = dotg(rows, vs[l], TN)
        swd[slot] = dotg(hs[l], expert_rows(xa, l), TN)
        for cp in finish_grads(l):
            cp.start()
        return carry

    gg_x.start()
    lo, hi = pl.ds(0, H), pl.ds(H, H)
    early = [
        pltpu.make_async_copy(acc.at[1, 0], base_ref, lsem.at[8]),
        pltpu.make_async_copy(acc.at[1, 1, lo], mx_ref.at[lo], lsem.at[9]),
        pltpu.make_async_copy(acc.at[1, 2, hi], my_ref.at[hi], lsem.at[10]),
    ]
    for c in early:
        c.start()
    lax.fori_loop(0, NE, weight_grads, 0)
    gg_x.wait_recv()
    gg_y.wait_recv()
    gg_ref[...] = gacc[0] + gf[0] + gf[1]
    for i in (2, 3, 4, 5):
        ro[i].wait_recv()
    moe_sc[...] = (acc[0, 0] + fr[0] + fr[1]).astype(BF16)
    out_moe = pltpu.make_async_copy(moe_sc, moe_ref, lsem.at[11])
    out_moe.start()
    for l in (NE - 2, NE - 1):
        for cp in finish_grads(l):
            cp.wait()
    for c in cr + cg + cy + ro + [swap_gg, gg_diag, gg_y, gg_x]:
        c.wait_send()
    for h in order:
        swap_copy(PX, prv, h).wait_send()
    late_y = pltpu.make_async_copy(acc.at[1, 2, lo], my_ref.at[lo], lsem.at[12])
    late_x = pltpu.make_async_copy(acc.at[1, 1, hi], mx_ref.at[hi], lsem.at[13])
    rp[0].wait_recv()
    acc[1, 2, :H] = acc[1, 2, :H] + rd[1, 0]
    late_y.start()
    rp[1].wait_recv()
    acc[1, 1, H:] = acc[1, 1, H:] + rd[1, 1]
    late_x.start()
    for c in rp:
        c.wait_send()
    for c in early + [out_moe, late_y, late_x]:
        c.wait()


def publish(*refs):
    n = (len(refs) - 2) // 3
    ins, outs, bufs, (sin, sout) = refs[:n], refs[n:2 * n], refs[2 * n:3 * n], refs[3 * n:]
    pieces = []
    for a, o, b in zip(ins, outs, bufs):
        if len(a.shape) == 3:
            pieces += [(a.at[l], o.at[l], b.at[l]) for l in range(a.shape[0])]
        else:
            pieces.append((a, o, b))
    loads = [pltpu.make_async_copy(a, b, sin.at[i]) for i, (a, o, b) in enumerate(pieces)]
    stores = [pltpu.make_async_copy(b, o, sout.at[i]) for i, (a, o, b) in enumerate(pieces)]
    for c in loads:
        c.start()
    for c, w in zip(loads, stores):
        c.wait()
        w.start()
    for w in stores:
        w.wait()


def solution(mesh):
    tok_spec = P(ALL_AXES, None)
    w_spec = P(EP_AXES, None, None)
    gw_spec = P(ALL_AXES, None, None)

    def local_step(tokens, route_idx, gate_vals, w_gate, w_up, w_down, grad_out):
        T, K = route_idx.shape
        D = tokens.shape[1]
        NE, _, FF = w_gate.shape
        CAP = T * K // (8 * NE)
        vm = pl.BlockSpec(memory_space=pltpu.VMEM)
        hbm = pl.BlockSpec(memory_space=pl.ANY)
        sds = jax.ShapeDtypeStruct
        outs = pl.pallas_call(
            functools.partial(kernel, T, D, FF, NE, CAP),
            out_shape=(sds((T, D), BF16), sds((K, T), F32),
                       sds((T, D), F32), sds((T, D), F32), sds((T, D), F32),
                       sds((NE, D, FF), F32), sds((NE, D, FF), F32), sds((NE, FF, D), F32)),
            in_specs=[hbm, hbm, vm, vm, hbm, hbm, hbm],
            out_specs=(hbm, vm, hbm, hbm, hbm, hbm, hbm, hbm),
            scratch_shapes=[
                pltpu.VMEM((8, T, D), BF16),
                pltpu.VMEM((8, T, D), BF16),
                pltpu.VMEM((8, NE, CAP, D), BF16),
                pltpu.VMEM((NE, T, FF), BF16),
                pltpu.VMEM((NE, T, FF), BF16),
                pltpu.VMEM((NE, T, FF), BF16),
                pltpu.VMEM((8, NE, CAP, D), BF16),
                pltpu.VMEM((NE, D, FF), BF16),
                pltpu.VMEM((NE, D, FF), BF16),
                pltpu.VMEM((NE, FF, D), BF16),
                pltpu.VMEM((2, 4, T, D), F32),
                pltpu.VMEM((2, 2, T // 2, D), F32),
                pltpu.VMEM((2, T, D), F32),
                pltpu.VMEM((4, NE, CAP, D), BF16),
                pltpu.VMEM((4, NE, CAP, D), BF16),
                pltpu.VMEM((2, D, FF), F32),
                pltpu.VMEM((2, D, FF), F32),
                pltpu.VMEM((2, FF, D), F32),
                pltpu.VMEM((T, T), BF16),
                pltpu.VMEM((3, T, T), BF16),
                pltpu.VMEM((8, K, T), jnp.int32),
                pltpu.VMEM((8, K, T), F32),
                pltpu.VMEM((16, NE, T), F32),
                pltpu.VMEM((16, NE, T), F32),
                pltpu.VMEM((16, NE, T), F32),
                pltpu.VMEM((T, 16 * NE), BF16),
                pltpu.VMEM((3, T, 16 * NE), BF16),
                pltpu.VMEM((2, 4, K, T), F32),
                pltpu.VMEM((4, K, T), F32),
                pltpu.VMEM((4, K, T), F32),
                pltpu.VMEM((K, T), F32),
                pltpu.VMEM((2, K, T), F32),
                pltpu.VMEM((T, D), BF16),
                pltpu.SemaphoreType.DMA((N_SEM,)),
                pltpu.SemaphoreType.DMA((N_SEM,)),
                pltpu.SemaphoreType.DMA((17,)),
            ],
            compiler_params=pltpu.CompilerParams(
                collective_id=0, has_side_effects=True, vmem_limit_bytes=67043328),
        )(tokens, grad_out, route_idx.T, gate_vals.T, w_gate, w_up, w_down)
        base, mx, my = outs[2:5]
        rx = lax.ppermute(mx, 'col', [(0, 1), (1, 0)])
        ry = lax.ppermute(my, 'row', [(0, 1), (1, 0)])
        res = outs[:2] + outs[5:]
        n_pieces = 2 + 3 * NE
        moe, gg, dwg, dwu, dwd = pl.pallas_call(
            publish,
            out_shape=tuple(sds(a.shape, a.dtype) for a in res),
            in_specs=[hbm] * 5,
            out_specs=(hbm,) * 5,
            scratch_shapes=[pltpu.VMEM(a.shape, a.dtype) for a in res] + [
                pltpu.SemaphoreType.DMA((n_pieces,)),
                pltpu.SemaphoreType.DMA((n_pieces,)),
            ],
            cost_estimate=pl.CostEstimate(
                flops=2_000_000_000, bytes_accessed=2 * 3 * NE * D * FF * 4, transcendentals=0),
            compiler_params=pltpu.CompilerParams(vmem_limit_bytes=60 * 1024 * 1024),
        )(*res)
        gx = (base + rx + ry).astype(BF16)
        return moe, gx, gg.T, dwg, dwu, dwd

    return jax.shard_map(
        local_step, mesh=mesh,
        in_specs=(tok_spec, tok_spec, tok_spec, w_spec, w_spec, w_spec, tok_spec),
        out_specs=(tok_spec, tok_spec, tok_spec, gw_spec, gw_spec, gw_spec),
        check_vma=False)
```

```python
import functools

import jax
import jax.numpy as jnp
from jax import lax
from jax.experimental import pallas as pl
from jax.experimental.pallas import tpu as pltpu
from jax.sharding import PartitionSpec as P


EP_AXES = ('row', 'col', 'core')
ALL_AXES = ('part', 'row', 'col', 'core')
MESH = pl.DeviceIdType.MESH
F32 = jnp.float32
BF16 = jnp.bfloat16
NT = (((1,), (1,)), ((), ()))
TN = (((0,), (0,)), ((), ()))

AG_X, AG_DY, RG, OX, PX, RS_O, RS_P, GG, N_SEM = 0, 10, 20, 34, 38, 42, 48, 50, 54


def dot(a, b):
    return jnp.dot(a, b, preferred_element_type=F32)


def dotg(a, b, dims):
    return lax.dot_general(a, b, dims, preferred_element_type=F32)


def kernel(T, D, FF, NE, CAP,
           x_ref, dy_ref, route_ref, gate_ref, wg_ref, wu_ref, wd_ref,
           moe_ref, gg_ref, base_ref, mx_ref, my_ref, xg_ref, c_ref, du_ref, dv_ref, h_ref,
           xa, dya, xg, us, vs, hs, os_, wg, wu, wd, acc, rd, fr, orv, prv,
           pb, sb, ra, ga, rm, gm, mb, rt, gt, gj, gr, gacc, gd, gf, moe_sc,
           ssem, rsem, lsem):
    H = T // 2
    row, col, core = lax.axis_index('row'), lax.axis_index('col'), lax.axis_index('core')
    me = row * 4 + col * 2 + core
    partner = row * 4 + col * 2 + (1 - core)

    def dev(rel):
        return {
            'row': 1 - row if rel & 4 else row,
            'col': 1 - col if rel & 2 else col,
            'core': 1 - core if rel & 1 else core,
        }

    def rc(i, src, dst, rel):
        return pltpu.make_async_remote_copy(
            src_ref=src, dst_ref=dst, send_sem=ssem.at[i], recv_sem=rsem.at[i],
            device_id=dev(rel), device_id_type=MESH)

    def gather_copies(b, buf):
        lo, hi = pl.ds(0, H), pl.ds(H, H)
        return [
            rc(b + 0, buf.at[0], buf.at[1], 1),
            rc(b + 1, buf.at[0, hi], buf.at[2, hi], 2),
            rc(b + 2, buf.at[0, lo], buf.at[2, lo], 2),
            rc(b + 3, buf.at[0, lo], buf.at[4, lo], 4),
            rc(b + 4, buf.at[0, hi], buf.at[4, hi], 4),
            rc(b + 5, buf.at[2, hi], buf.at[6, hi], 4),
            rc(b + 6, buf.at[4, lo], buf.at[6, lo], 2),
            rc(b + 7, buf.at[2], buf.at[3], 1),
            rc(b + 8, buf.at[4], buf.at[5], 1),
            rc(b + 9, buf.at[6], buf.at[7], 1),
        ]

    lx = pltpu.make_async_copy(x_ref, xa.at[0], lsem.at[0])
    ldy = pltpu.make_async_copy(dy_ref, dya.at[0], lsem.at[1])
    lwg = pltpu.make_async_copy(wg_ref, wg, lsem.at[2])
    lwu = pltpu.make_async_copy(wu_ref, wu, lsem.at[3])
    lwd = pltpu.make_async_copy(wd_ref, wd, lsem.at[4])
    lx.start()
    ldy.start()
    lwg.start()
    lwu.start()
    lwd.start()

    barrier = pltpu.get_barrier_semaphore()
    for rel in (1, 2, 4):
        pl.semaphore_signal(barrier, inc=1, device_id=dev(rel), device_id_type=MESH)
    pl.semaphore_wait(barrier, 3)

    def small_copies(b, src, buf, diag):
        return [
            rc(b + 0, src, buf.at[1], 1),
            rc(b + 1, src, buf.at[2], 2),
            rc(b + 2, src, buf.at[4], 4),
            rc(b + 3, buf.at[6 - diag], buf.at[6], diag),
            rc(b + 4, buf.at[2], buf.at[3], 1),
            rc(b + 5, buf.at[4], buf.at[5], 1),
            rc(b + 6, buf.at[6], buf.at[7], 1),
        ]

    cr = small_copies(RG, route_ref, ra, 2)
    cg = small_copies(RG + 7, gate_ref, ga, 4)
    cx = gather_copies(AG_X, xa)
    cy = gather_copies(AG_DY, dya)
    for i in (1, 2, 0):
        cr[i].start()
        cg[i].start()
    lx.wait()
    for i in (1, 3, 0):
        cx[i].start()
    cr[2].wait_recv()
    cr[3].start()
    cg[1].wait_recv()
    cg[3].start()
    cx[2].start()
    cx[4].start()
    cr[5].start()
    cg[4].start()
    cr[1].wait_recv()
    cr[4].start()
    cg[2].wait_recv()
    cg[5].start()
    ra[0] = route_ref[...]
    ga[0] = gate_ref[...]

    i0 = lax.broadcasted_iota(jnp.int32, (T, T), 0)
    i1 = lax.broadcasted_iota(jnp.int32, (T, T), 1)
    sb[0] = (i0 < i1).astype(F32).astype(BF16)
    sb[1] = (i0 > i1).astype(F32).astype(BF16)
    sb[2] = (i0 == i1).astype(F32).astype(BF16)
    cx[1].wait_recv()
    cx[5].start()
    cx[3].wait_recv()
    cx[6].start()
    cr[3].wait_recv()
    cr[6].start()
    cg[3].wait_recv()
    cg[6].start()
    for i in (0, 4, 5, 6):
        cr[i].wait_recv()
        cg[i].wait_recv()
    mb[...] = jnp.zeros_like(mb)
    gm[...] = jnp.zeros_like(gm)
    sub = lax.broadcasted_iota(jnp.int32, (NE, T), 0)
    for idx in range(12):
        src = idx if idx < 8 else 2 * (idx - 8)
        owner = me if idx < 8 else partner
        ids = sub + owner * NE
        hits = jnp.zeros((NE, T), F32)
        gates = jnp.zeros((NE, T), F32)
        for j in range(8):
            hit = ra[src, j:j + 1, :] == ids
            hits = hits + jnp.where(hit, 1.0, 0.0)
            gates = gates + jnp.where(hit, ga[src, j:j + 1, :], 0.0)
        mb[idx] = hits
        gm[idx] = gates
    m_all = mb[...].reshape(16 * NE, T)
    m_bf = m_all.astype(BF16)
    ranks = dot(m_bf, sb[0])
    rm[...] = jnp.where(m_all > 0.5, ranks, -1.0).reshape(16, NE, T)
    m_t = dotg(sb[2], m_bf, NT)
    r_t = dotg(sb[1], m_bf, NT)
    rt[...] = jnp.where(m_t > 0.5, r_t, -1.0).astype(BF16)
    g_all = gm[...].reshape(16 * NE, T)
    g_hi = g_all.astype(BF16)
    rest = g_all - g_hi.astype(F32)
    g_mid = rest.astype(BF16)
    g_lo = (rest - g_mid.astype(F32)).astype(BF16)
    for k, piece in enumerate((g_hi, g_mid, g_lo)):
        gt[k] = dotg(sb[2], piece, NT).astype(BF16)

    lane_r = lax.broadcasted_iota(jnp.int32, (CAP, T), 0).astype(F32)

    def build_p(d):
        r_d = rm[d]
        for l in range(NE):
            pb[l * CAP:(l + 1) * CAP, :] = jnp.where(lane_r == r_d[l:l + 1, :], 1.0, 0.0).astype(BF16)

    def gather_x(d):
        build_p(d)
        xg[d] = dot(pb[...], xa[d]).astype(BF16).reshape(NE, CAP, D)

    def gather_x_loop(first, step, count):
        def one(i, carry):
            gather_x(first + step * i)
            return carry
        lax.fori_loop(0, count, one, 0)

    cx[0].wait_recv()
    gather_x_loop(0, 1, 2)
    cx[2].wait_recv()
    cx[7].start()
    cx[4].wait_recv()
    cx[8].start()
    ldy.wait()
    for i in (1, 3, 0, 2, 4):
        cy[i].start()
    gather_x_loop(2, 2, 2)
    cx[7].wait_recv()
    cx[8].wait_recv()
    gather_x_loop(3, 2, 2)
    cx[5].wait_recv()
    cx[6].wait_recv()
    cx[9].start()
    gather_x_loop(6, 1, 1)
    cx[9].wait_recv()
    gather_x_loop(7, 1, 1)

    lwg.wait()
    lwu.wait()
    lwd.wait()

    def forward(l, carry):
        rows = xg[:, pl.ds(l, 1)].reshape(T, D)
        u = dot(rows, wg[l]).astype(BF16)
        v = dot(rows, wu[l]).astype(BF16)
        us[l] = u
        vs[l] = v
        uf = u.astype(F32)
        h = (uf * jax.nn.sigmoid(uf) * v.astype(F32)).astype(BF16)
        o = dot(h, wd[l]).astype(BF16)
        os_[:, pl.ds(l, 1)] = o.reshape(8, 1, CAP, D)
        return carry

    lax.fori_loop(0, NE // 2, forward, 0)
    cy[1].wait_recv()
    cy[5].start()
    cy[3].wait_recv()
    cy[6].start()
    lax.fori_loop(NE // 2, NE, forward, 0)

    order = (3, 1, 2, 0)

    def swap_copy(b, buf, h):
        return rc(b + h, os_.at[2 * h + 1], buf.at[h], 1)

    def reduce_copies(b, k):
        lo, hi = pl.ds(0, H), pl.ds(H, H)
        return [
            rc(b + 0, acc.at[k, 3, lo], rd.at[k, 0], 2),
            rc(b + 1, acc.at[k, 3, hi], rd.at[k, 1], 4),
            rc(b + 2, acc.at[k, 1, lo], fr.at[0, lo], 2),
            rc(b + 3, acc.at[k, 2, hi], fr.at[1, hi], 4),
            rc(b + 4, acc.at[k, 1, hi], fr.at[0, hi], 2),
            rc(b + 5, acc.at[k, 2, lo], fr.at[1, lo], 4),
        ][:6 if k == 0 else 2]

    e0 = lax.broadcasted_iota(jnp.int32, (16 * NE, T), 0)
    e1 = lax.broadcasted_iota(jnp.int32, (16 * NE, T), 1) // CAP
    rank_lane = lax.rem(lax.broadcasted_iota(jnp.int32, (T, T), 1), CAP).astype(F32)

    def spread(idx, rows, weighted):
        pick = jnp.where(e0 == e1 + idx * NE, 1.0, 0.0).astype(BF16)
        hit = dot(rt[...], pick) == rank_lane
        if weighted:
            for k in range(3):
                sb[k] = jnp.where(hit, dot(gt[k], pick), 0.0).astype(BF16)
            return dot(sb[0], rows) + dot(sb[1], rows) + dot(sb[2], rows)
        sb[0] = jnp.where(hit, 1.0, 0.0).astype(BF16)
        return dot(sb[0], rows)

    def combine_all(k, b, recv, copies, weighted):
        def one(i, carry):
            h = 3 - i
            acc[k, h] = spread(2 * h, os_[2 * h].reshape(T, D), weighted)
            swap_copy(b, recv, h).wait_recv()
            acc[k, h] = acc[k, h] + spread(8 + h, recv[h].reshape(T, D), weighted)

            @pl.when(i == 0)
            def _():
                copies[0].start()
                copies[1].start()

            if k == 0:
                @pl.when(i == 1)
                def _():
                    copies[3].start()

                @pl.when(i == 2)
                def _():
                    copies[2].start()
            return carry
        lax.fori_loop(0, 4, one, 0)

    ro = reduce_copies(RS_O, 0)
    for h in order:
        swap_copy(OX, orv, h).start()
    cy[2].wait_recv()
    cy[7].start()
    cy[4].wait_recv()
    cy[8].start()
    combine_all(0, OX, orv, ro, True)

    cy[5].wait_recv()
    cy[6].wait_recv()
    cy[9].start()
    cy[0].wait_recv()
    cy[7].wait_recv()
    cy[8].wait_recv()
    cy[9].wait_recv()
    for c in cx:
        c.wait_send()

    swap_gg = rc(GG, gj.at[1], gr, 1)
    gg_diag = rc(GG + 1, gacc.at[3], gd, 4)
    gg_y = rc(GG + 2, gacc.at[2], gf.at[1], 4)
    gg_x = rc(GG + 3, gacc.at[1], gf.at[0], 2)

    def gather_dy(d, carry):
        build_p(d)
        rows = dot(pb[...], dya[d])
        outs = os_[d].reshape(T, D).astype(F32)
        gg_rows = jnp.sum(rows * outs, axis=1, keepdims=True)
        r_d = rm[d]
        g_d = gm[d]
        r_ids = ra[d]
        gg_d = jnp.zeros((8, T), F32)
        for l in range(NE):
            hit = lane_r == r_d[l:l + 1, :]
            gcol = jnp.sum(jnp.where(hit, g_d[l:l + 1, :], 0.0), axis=1, keepdims=True)
            xa[d, l * CAP:(l + 1) * CAP, :] = (gcol * rows[l * CAP:(l + 1) * CAP, :]).astype(BF16)
            gg_l = jnp.sum(
                jnp.where(hit, gg_rows[l * CAP:(l + 1) * CAP, :], 0.0), axis=0, keepdims=True)
            gg_d = gg_d + jnp.where(r_ids == me * NE + l, gg_l, 0.0)
        gj[lax.rem(d, 2), d // 2] = gg_d
        return carry

    lax.fori_loop(0, 8, gather_dy, 0)
    swap_gg.start()
    for h in order:
        swap_copy(OX, orv, h).wait_send()

    ro[0].wait_recv()
    acc[0, 2, :H] = acc[0, 2, :H] + rd[0, 0]
    ro[5].start()
    ro[1].wait_recv()
    acc[0, 1, H:] = acc[0, 1, H:] + rd[0, 1]
    ro[4].start()
    swap_gg.wait_recv()
    gacc[...] = gj[0] + gr[...]

    def expert_rows(buf, l):
        return buf[:, pl.ds(pl.multiple_of(l * CAP, CAP), CAP), :].reshape(T, D)

    def backward(l, carry):
        dh = dotg(expert_rows(xa, l), wd[l], NT).astype(BF16).astype(F32)
        uf = us[l].astype(F32)
        vf = vs[l].astype(F32)
        s = jax.nn.sigmoid(uf)
        sl = uf * s
        hs[l] = (sl * vf).astype(BF16)
        dv = (dh * sl).astype(BF16)
        du = (dh * vf * (s + sl * (1.0 - s))).astype(BF16)
        us[l] = du
        vs[l] = dv
        pr = (dotg(du, wg[l], NT) + dotg(dv, wu[l], NT)).astype(BF16)
        os_[:, pl.ds(l, 1)] = pr.reshape(8, 1, CAP, D)
        return carry

    gg_diag.start()
    gg_y.start()
    out_xg = pltpu.make_async_copy(xg, xg_ref, lsem.at[5])
    out_c = pltpu.make_async_copy(xa, c_ref, lsem.at[6])
    out_xg.start()
    out_c.start()
    lax.fori_loop(0, NE, backward, 0)
    gg_diag.wait_recv()
    gacc[1] = gacc[1] + gd[...]

    rp = reduce_copies(RS_P, 1)
    for h in order:
        swap_copy(PX, prv, h).start()
    combine_all(1, PX, prv, rp, False)

    gg_x.start()
    lo, hi = pl.ds(0, H), pl.ds(H, H)
    early = [
        pltpu.make_async_copy(acc.at[1, 0], base_ref, lsem.at[8]),
        pltpu.make_async_copy(acc.at[1, 1, lo], mx_ref.at[lo], lsem.at[9]),
        pltpu.make_async_copy(acc.at[1, 2, hi], my_ref.at[hi], lsem.at[10]),
        pltpu.make_async_copy(us, du_ref, lsem.at[14]),
        pltpu.make_async_copy(vs, dv_ref, lsem.at[15]),
        pltpu.make_async_copy(hs, h_ref, lsem.at[16]),
    ]
    for c in early:
        c.start()
    gg_x.wait_recv()
    gg_y.wait_recv()
    gg_ref[...] = gacc[0] + gf[0] + gf[1]
    for i in (2, 3, 4, 5):
        ro[i].wait_recv()
    moe_sc[...] = (acc[0, 0] + fr[0] + fr[1]).astype(BF16)
    out_moe = pltpu.make_async_copy(moe_sc, moe_ref, lsem.at[11])
    out_moe.start()
    for c in cr + cg + cy + ro + [swap_gg, gg_diag, gg_y, gg_x]:
        c.wait_send()
    for h in order:
        swap_copy(PX, prv, h).wait_send()
    late_y = pltpu.make_async_copy(acc.at[1, 2, lo], my_ref.at[lo], lsem.at[12])
    late_x = pltpu.make_async_copy(acc.at[1, 1, hi], mx_ref.at[hi], lsem.at[13])
    rp[0].wait_recv()
    acc[1, 2, :H] = acc[1, 2, :H] + rd[1, 0]
    late_y.start()
    rp[1].wait_recv()
    acc[1, 1, H:] = acc[1, 1, H:] + rd[1, 1]
    late_x.start()
    for c in rp:
        c.wait_send()
    for c in early + [out_xg, out_c, out_moe, late_y, late_x]:
        c.wait()


def publish(T, D, xg_ref, c_ref, du_ref, dv_ref, h_ref, moe_in, gg_in,
            dwg_ref, dwu_ref, dwd_ref, moe_ref, gg_ref):
    rows = xg_ref[...].reshape(T, D)
    dwg_ref[0] = dotg(rows, du_ref[0], TN)
    dwu_ref[0] = dotg(rows, dv_ref[0], TN)
    dwd_ref[0] = dotg(h_ref[0], c_ref[...].reshape(T, D), TN)

    @pl.when(pl.program_id(0) == 0)
    def _():
        moe_ref[...] = moe_in[...]
        gg_ref[...] = gg_in[...]


def solution(mesh):
    tok_spec = P(ALL_AXES, None)
    w_spec = P(EP_AXES, None, None)
    gw_spec = P(ALL_AXES, None, None)

    def local_step(tokens, route_idx, gate_vals, w_gate, w_up, w_down, grad_out):
        T, K = route_idx.shape
        D = tokens.shape[1]
        NE, _, FF = w_gate.shape
        CAP = T * K // (8 * NE)
        vm = pl.BlockSpec(memory_space=pltpu.VMEM)
        hbm = pl.BlockSpec(memory_space=pl.ANY)
        sds = jax.ShapeDtypeStruct
        outs = pl.pallas_call(
            functools.partial(kernel, T, D, FF, NE, CAP),
            out_shape=(sds((T, D), BF16), sds((K, T), F32),
                       sds((T, D), F32), sds((T, D), F32), sds((T, D), F32),
                       sds((8, NE, CAP, D), BF16), sds((8, T, D), BF16),
                       sds((NE, T, FF), BF16), sds((NE, T, FF), BF16), sds((NE, T, FF), BF16)),
            in_specs=[hbm, hbm, vm, vm, hbm, hbm, hbm],
            out_specs=(hbm, vm) + (hbm,) * 8,
            scratch_shapes=[
                pltpu.VMEM((8, T, D), BF16),
                pltpu.VMEM((8, T, D), BF16),
                pltpu.VMEM((8, NE, CAP, D), BF16),
                pltpu.VMEM((NE, T, FF), BF16),
                pltpu.VMEM((NE, T, FF), BF16),
                pltpu.VMEM((NE, T, FF), BF16),
                pltpu.VMEM((8, NE, CAP, D), BF16),
                pltpu.VMEM((NE, D, FF), BF16),
                pltpu.VMEM((NE, D, FF), BF16),
                pltpu.VMEM((NE, FF, D), BF16),
                pltpu.VMEM((2, 4, T, D), F32),
                pltpu.VMEM((2, 2, T // 2, D), F32),
                pltpu.VMEM((2, T, D), F32),
                pltpu.VMEM((4, NE, CAP, D), BF16),
                pltpu.VMEM((4, NE, CAP, D), BF16),
                pltpu.VMEM((T, T), BF16),
                pltpu.VMEM((3, T, T), BF16),
                pltpu.VMEM((8, K, T), jnp.int32),
                pltpu.VMEM((8, K, T), F32),
                pltpu.VMEM((16, NE, T), F32),
                pltpu.VMEM((16, NE, T), F32),
                pltpu.VMEM((16, NE, T), F32),
                pltpu.VMEM((T, 16 * NE), BF16),
                pltpu.VMEM((3, T, 16 * NE), BF16),
                pltpu.VMEM((2, 4, K, T), F32),
                pltpu.VMEM((4, K, T), F32),
                pltpu.VMEM((4, K, T), F32),
                pltpu.VMEM((K, T), F32),
                pltpu.VMEM((2, K, T), F32),
                pltpu.VMEM((T, D), BF16),
                pltpu.SemaphoreType.DMA((N_SEM,)),
                pltpu.SemaphoreType.DMA((N_SEM,)),
                pltpu.SemaphoreType.DMA((17,)),
            ],
            compiler_params=pltpu.CompilerParams(
                collective_id=0, has_side_effects=True, vmem_limit_bytes=67043328),
        )(tokens, grad_out, route_idx.T, gate_vals.T, w_gate, w_up, w_down)
        moe, gg, base, mx, my, xg, c, du, dv, h = outs
        rx = lax.ppermute(mx, 'col', [(0, 1), (1, 0)])
        ry = lax.ppermute(my, 'row', [(0, 1), (1, 0)])

        def per_expert(*shape):
            return pl.BlockSpec((1,) + shape, lambda l: (l, 0, 0))

        def whole(a):
            return pl.BlockSpec(a.shape, lambda l: (0, 0))

        dwg, dwu, dwd, moe, gg = pl.pallas_call(
            functools.partial(publish, T, D),
            grid=(NE,),
            out_shape=(sds((NE, D, FF), F32), sds((NE, D, FF), F32), sds((NE, FF, D), F32),
                       sds(moe.shape, BF16), sds(gg.shape, F32)),
            in_specs=[pl.BlockSpec((8, 1, CAP, D), lambda l: (0, l, 0, 0)),
                      pl.BlockSpec((8, CAP, D), lambda l: (0, l, 0)),
                      per_expert(T, FF), per_expert(T, FF), per_expert(T, FF), whole(moe), whole(gg)],
            out_specs=(per_expert(D, FF), per_expert(D, FF), per_expert(FF, D), whole(moe), whole(gg)),
            cost_estimate=pl.CostEstimate(
                flops=6 * NE * T * D * FF, bytes_accessed=36 * 1024 * 1024, transcendentals=0),
            compiler_params=pltpu.CompilerParams(vmem_limit_bytes=60 * 1024 * 1024),
        )(xg, c, du, dv, h, moe, gg)
        gx = (base + rx + ry).astype(BF16)
        return moe, gx, gg.T, dwg, dwu, dwd

    return jax.shard_map(
        local_step, mesh=mesh,
        in_specs=(tok_spec, tok_spec, tok_spec, w_spec, w_spec, w_spec, tok_spec),
        out_specs=(tok_spec, tok_spec, tok_spec, gw_spec, gw_spec, gw_spec),
        check_vma=False)
```

```python
import functools

import jax
import jax.numpy as jnp
from jax import lax
from jax.experimental import pallas as pl
from jax.experimental.pallas import tpu as pltpu
from jax.sharding import PartitionSpec as P


EP_AXES = ('row', 'col', 'core')
ALL_AXES = ('part', 'row', 'col', 'core')
MESH = pl.DeviceIdType.MESH
F32 = jnp.float32
BF16 = jnp.bfloat16
NT = (((1,), (1,)), ((), ()))
TN = (((0,), (0,)), ((), ()))

AG_X, AG_DY, RG, OX, PX, RS_O, RS_P, GG, N_SEM = 0, 10, 20, 34, 38, 42, 48, 50, 54


def dot(a, b):
    return jnp.dot(a, b, preferred_element_type=F32)


def dotg(a, b, dims):
    return lax.dot_general(a, b, dims, preferred_element_type=F32)


def kernel(T, D, FF, NE, CAP,
           x_ref, dy_ref, route_ref, gate_ref, wg_ref, wu_ref, wd_ref,
           moe_ref, gg_ref, base_ref, mx_ref, my_ref, xg_ref, c_ref, du_ref, dv_ref, h_ref,
           xa, dya, xg, us, vs, hs, os_, wg, wu, wd, acc, rd, fr, orv, prv,
           pb, sb, ra, ga, rm, gm, mb, rt, gt, gj, gr, gacc, gd, gf, moe_sc,
           ssem, rsem, lsem):
    H = T // 2
    row, col, core = lax.axis_index('row'), lax.axis_index('col'), lax.axis_index('core')
    me = row * 4 + col * 2 + core
    partner = row * 4 + col * 2 + (1 - core)

    def dev(rel):
        return {
            'row': 1 - row if rel & 4 else row,
            'col': 1 - col if rel & 2 else col,
            'core': 1 - core if rel & 1 else core,
        }

    def rc(i, src, dst, rel):
        return pltpu.make_async_remote_copy(
            src_ref=src, dst_ref=dst, send_sem=ssem.at[i], recv_sem=rsem.at[i],
            device_id=dev(rel), device_id_type=MESH)

    def gather_copies(b, buf):
        lo, hi = pl.ds(0, H), pl.ds(H, H)
        return [
            rc(b + 0, buf.at[0], buf.at[1], 1),
            rc(b + 1, buf.at[0, hi], buf.at[2, hi], 2),
            rc(b + 2, buf.at[0, lo], buf.at[2, lo], 2),
            rc(b + 3, buf.at[0, lo], buf.at[4, lo], 4),
            rc(b + 4, buf.at[0, hi], buf.at[4, hi], 4),
            rc(b + 5, buf.at[2, hi], buf.at[6, hi], 4),
            rc(b + 6, buf.at[4, lo], buf.at[6, lo], 2),
            rc(b + 7, buf.at[2], buf.at[3], 1),
            rc(b + 8, buf.at[4], buf.at[5], 1),
            rc(b + 9, buf.at[6], buf.at[7], 1),
        ]

    lx = pltpu.make_async_copy(x_ref, xa.at[0], lsem.at[0])
    ldy = pltpu.make_async_copy(dy_ref, dya.at[0], lsem.at[1])
    lwg = pltpu.make_async_copy(wg_ref, wg, lsem.at[2])
    lwu = pltpu.make_async_copy(wu_ref, wu, lsem.at[3])
    lwd = pltpu.make_async_copy(wd_ref, wd, lsem.at[4])
    lr = pltpu.make_async_copy(route_ref, ra.at[0], lsem.at[14])
    lg = pltpu.make_async_copy(gate_ref, ga.at[0], lsem.at[15])
    lx.start()
    lr.start()
    lg.start()
    ldy.start()
    lwg.start()
    lwu.start()
    lwd.start()

    barrier = pltpu.get_barrier_semaphore()
    for rel in (1, 2, 4):
        pl.semaphore_signal(barrier, inc=1, device_id=dev(rel), device_id_type=MESH)
    pl.semaphore_wait(barrier, 3)

    def small_copies(b, src, buf, diag):
        return [
            rc(b + 0, src, buf.at[1], 1),
            rc(b + 1, src, buf.at[2], 2),
            rc(b + 2, src, buf.at[4], 4),
            rc(b + 3, buf.at[6 - diag], buf.at[6], diag),
            rc(b + 4, buf.at[2], buf.at[3], 1),
            rc(b + 5, buf.at[4], buf.at[5], 1),
            rc(b + 6, buf.at[6], buf.at[7], 1),
        ]

    cr = small_copies(RG, ra.at[0], ra, 2)
    cg = small_copies(RG + 7, ga.at[0], ga, 4)
    cx = gather_copies(AG_X, xa)
    cy = gather_copies(AG_DY, dya)
    lr.wait()
    lg.wait()
    for i in (1, 2, 0):
        cr[i].start()
        cg[i].start()
    lx.wait()
    for i in (1, 3, 0):
        cx[i].start()
    cr[2].wait_recv()
    cr[3].start()
    cg[1].wait_recv()
    cg[3].start()
    cx[2].start()
    cx[4].start()
    cr[5].start()
    cg[4].start()
    cr[1].wait_recv()
    cr[4].start()
    cg[2].wait_recv()
    cg[5].start()

    i0 = lax.broadcasted_iota(jnp.int32, (T, T), 0)
    i1 = lax.broadcasted_iota(jnp.int32, (T, T), 1)
    sb[0] = (i0 < i1).astype(F32).astype(BF16)
    sb[1] = (i0 > i1).astype(F32).astype(BF16)
    sb[2] = (i0 == i1).astype(F32).astype(BF16)
    cx[1].wait_recv()
    cx[5].start()
    cx[3].wait_recv()
    cx[6].start()
    cr[3].wait_recv()
    cr[6].start()
    cg[3].wait_recv()
    cg[6].start()
    for i in (0, 4, 5, 6):
        cr[i].wait_recv()
        cg[i].wait_recv()
    mb[...] = jnp.zeros_like(mb)
    gm[...] = jnp.zeros_like(gm)
    sub = lax.broadcasted_iota(jnp.int32, (NE, T), 0)
    for idx in range(12):
        src = idx if idx < 8 else 2 * (idx - 8)
        owner = me if idx < 8 else partner
        ids = sub + owner * NE
        hits = jnp.zeros((NE, T), F32)
        gates = jnp.zeros((NE, T), F32)
        for j in range(8):
            hit = ra[src, j:j + 1, :] == ids
            hits = hits + jnp.where(hit, 1.0, 0.0)
            gates = gates + jnp.where(hit, ga[src, j:j + 1, :], 0.0)
        mb[idx] = hits
        gm[idx] = gates
    m_all = mb[...].reshape(16 * NE, T)
    m_bf = m_all.astype(BF16)
    ranks = dot(m_bf, sb[0])
    rm[...] = jnp.where(m_all > 0.5, ranks, -1.0).reshape(16, NE, T)
    m_t = dotg(sb[2], m_bf, NT)
    r_t = dotg(sb[1], m_bf, NT)
    rt[...] = jnp.where(m_t > 0.5, r_t, -1.0).astype(BF16)
    g_all = gm[...].reshape(16 * NE, T)
    g_hi = g_all.astype(BF16)
    rest = g_all - g_hi.astype(F32)
    g_mid = rest.astype(BF16)
    g_lo = (rest - g_mid.astype(F32)).astype(BF16)
    for k, piece in enumerate((g_hi, g_mid, g_lo)):
        gt[k] = dotg(sb[2], piece, NT).astype(BF16)

    lane_r = lax.broadcasted_iota(jnp.int32, (CAP, T), 0).astype(F32)

    def build_p(d):
        r_d = rm[d]
        for l in range(NE):
            pb[l * CAP:(l + 1) * CAP, :] = jnp.where(lane_r == r_d[l:l + 1, :], 1.0, 0.0).astype(BF16)

    def gather_x(d):
        build_p(d)
        xg[d] = dot(pb[...], xa[d]).astype(BF16).reshape(NE, CAP, D)

    def gather_x_loop(first, step, count):
        def one(i, carry):
            gather_x(first + step * i)
            return carry
        lax.fori_loop(0, count, one, 0)

    cx[0].wait_recv()
    gather_x_loop(0, 1, 2)
    cx[2].wait_recv()
    cx[7].start()
    cx[4].wait_recv()
    cx[8].start()
    ldy.wait()
    for i in (1, 3, 0, 2, 4):
        cy[i].start()
    gather_x_loop(2, 2, 2)
    cx[7].wait_recv()
    cx[8].wait_recv()
    gather_x_loop(3, 2, 2)
    cx[5].wait_recv()
    cx[6].wait_recv()
    cx[9].start()
    gather_x_loop(6, 1, 1)
    cx[9].wait_recv()
    gather_x_loop(7, 1, 1)

    lwg.wait()
    lwu.wait()
    lwd.wait()

    def forward(l, carry):
        rows = xg[:, pl.ds(l, 1)].reshape(T, D)
        u = dot(rows, wg[l]).astype(BF16)
        v = dot(rows, wu[l]).astype(BF16)
        us[l] = u
        vs[l] = v
        uf = u.astype(F32)
        h = (uf * jax.nn.sigmoid(uf) * v.astype(F32)).astype(BF16)
        o = dot(h, wd[l]).astype(BF16)
        os_[:, pl.ds(l, 1)] = o.reshape(8, 1, CAP, D)
        return carry

    lax.fori_loop(0, NE // 2, forward, 0)
    cy[1].wait_recv()
    cy[5].start()
    cy[3].wait_recv()
    cy[6].start()
    lax.fori_loop(NE // 2, NE, forward, 0)

    order = (3, 1, 2, 0)

    def swap_copy(b, buf, h):
        return rc(b + h, os_.at[2 * h + 1], buf.at[h], 1)

    def reduce_copies(b, k):
        lo, hi = pl.ds(0, H), pl.ds(H, H)
        return [
            rc(b + 0, acc.at[k, 3, lo], rd.at[k, 0], 2),
            rc(b + 1, acc.at[k, 3, hi], rd.at[k, 1], 4),
            rc(b + 2, acc.at[k, 1, lo], fr.at[0, lo], 2),
            rc(b + 3, acc.at[k, 2, hi], fr.at[1, hi], 4),
            rc(b + 4, acc.at[k, 1, hi], fr.at[0, hi], 2),
            rc(b + 5, acc.at[k, 2, lo], fr.at[1, lo], 4),
        ][:6 if k == 0 else 2]

    e0 = lax.broadcasted_iota(jnp.int32, (16 * NE, T), 0)
    e1 = lax.broadcasted_iota(jnp.int32, (16 * NE, T), 1) // CAP
    rank_lane = lax.rem(lax.broadcasted_iota(jnp.int32, (T, T), 1), CAP).astype(F32)

    def spread(idx, rows, weighted):
        pick = jnp.where(e0 == e1 + idx * NE, 1.0, 0.0).astype(BF16)
        hit = dot(rt[...], pick) == rank_lane
        if weighted:
            for k in range(3):
                sb[k] = jnp.where(hit, dot(gt[k], pick), 0.0).astype(BF16)
            return dot(sb[0], rows) + dot(sb[1], rows) + dot(sb[2], rows)
        sb[0] = jnp.where(hit, 1.0, 0.0).astype(BF16)
        return dot(sb[0], rows)

    def combine_all(k, b, recv, copies, weighted):
        def one(i, carry):
            h = 3 - i
            acc[k, h] = spread(2 * h, os_[2 * h].reshape(T, D), weighted)
            swap_copy(b, recv, h).wait_recv()
            acc[k, h] = acc[k, h] + spread(8 + h, recv[h].reshape(T, D), weighted)

            @pl.when(i == 0)
            def _():
                copies[0].start()
                copies[1].start()

            if k == 0:
                @pl.when(i == 1)
                def _():
                    copies[3].start()

                @pl.when(i == 2)
                def _():
                    copies[2].start()
            return carry
        lax.fori_loop(0, 4, one, 0)

    ro = reduce_copies(RS_O, 0)
    for h in order:
        swap_copy(OX, orv, h).start()
    cy[2].wait_recv()
    cy[7].start()
    cy[4].wait_recv()
    cy[8].start()
    combine_all(0, OX, orv, ro, True)

    cy[5].wait_recv()
    cy[6].wait_recv()
    cy[9].start()
    cy[0].wait_recv()
    cy[7].wait_recv()
    cy[8].wait_recv()
    cy[9].wait_recv()
    for c in cx:
        c.wait_send()

    swap_gg = rc(GG, gj.at[1], gr, 1)
    gg_diag = rc(GG + 1, gacc.at[3], gd, 4)
    gg_y = rc(GG + 2, gacc.at[2], gf.at[1], 4)
    gg_x = rc(GG + 3, gacc.at[1], gf.at[0], 2)

    def gather_dy(d, carry):
        build_p(d)
        rows = dot(pb[...], dya[d])
        outs = os_[d].reshape(T, D).astype(F32)
        gg_rows = jnp.sum(rows * outs, axis=1, keepdims=True)
        r_d = rm[d]
        g_d = gm[d]
        r_ids = ra[d]
        gg_d = jnp.zeros((8, T), F32)
        for l in range(NE):
            hit = lane_r == r_d[l:l + 1, :]
            gcol = jnp.sum(jnp.where(hit, g_d[l:l + 1, :], 0.0), axis=1, keepdims=True)
            xa[d, l * CAP:(l + 1) * CAP, :] = (gcol * rows[l * CAP:(l + 1) * CAP, :]).astype(BF16)
            gg_l = jnp.sum(
                jnp.where(hit, gg_rows[l * CAP:(l + 1) * CAP, :], 0.0), axis=0, keepdims=True)
            gg_d = gg_d + jnp.where(r_ids == me * NE + l, gg_l, 0.0)
        gj[lax.rem(d, 2), d // 2] = gg_d
        return carry

    lax.fori_loop(0, 8, gather_dy, 0)
    swap_gg.start()
    for h in order:
        swap_copy(OX, orv, h).wait_send()

    ro[0].wait_recv()
    acc[0, 2, :H] = acc[0, 2, :H] + rd[0, 0]
    ro[5].start()
    ro[1].wait_recv()
    acc[0, 1, H:] = acc[0, 1, H:] + rd[0, 1]
    ro[4].start()
    swap_gg.wait_recv()
    gacc[...] = gj[0] + gr[...]

    def expert_rows(buf, l):
        return buf[:, pl.ds(pl.multiple_of(l * CAP, CAP), CAP), :].reshape(T, D)

    def backward(l, carry):
        dh = dotg(expert_rows(xa, l), wd[l], NT).astype(BF16).astype(F32)
        uf = us[l].astype(F32)
        vf = vs[l].astype(F32)
        s = jax.nn.sigmoid(uf)
        sl = uf * s
        hs[l] = (sl * vf).astype(BF16)
        dv = (dh * sl).astype(BF16)
        du = (dh * vf * (s + sl * (1.0 - s))).astype(BF16)
        us[l] = du
        vs[l] = dv
        pr = (dotg(du, wg[l], NT) + dotg(dv, wu[l], NT)).astype(BF16)
        os_[:, pl.ds(l, 1)] = pr.reshape(8, 1, CAP, D)
        return carry

    gg_diag.start()
    gg_y.start()
    out_xg = pltpu.make_async_copy(xg, xg_ref, lsem.at[5])
    out_c = pltpu.make_async_copy(xa, c_ref, lsem.at[6])
    out_xg.start()
    out_c.start()
    lax.fori_loop(0, NE, backward, 0)

    rp = reduce_copies(RS_P, 1)
    for h in order:
        swap_copy(PX, prv, h).start()
    combine_all(1, PX, prv, rp, False)

    lo, hi = pl.ds(0, H), pl.ds(H, H)
    early = [
        pltpu.make_async_copy(acc.at[1, 0], base_ref, lsem.at[8]),
        pltpu.make_async_copy(acc.at[1, 1, lo], mx_ref.at[lo], lsem.at[9]),
        pltpu.make_async_copy(acc.at[1, 2, hi], my_ref.at[hi], lsem.at[10]),
        pltpu.make_async_copy(us, du_ref, lsem.at[14]),
        pltpu.make_async_copy(vs, dv_ref, lsem.at[15]),
        pltpu.make_async_copy(hs, h_ref, lsem.at[16]),
    ]
    for c in early:
        c.start()
    gg_diag.wait_recv()
    gacc[1] = gacc[1] + gd[...]
    gg_x.start()
    gg_x.wait_recv()
    gg_y.wait_recv()
    gd[...] = gacc[0] + gf[0] + gf[1]
    out_gg = pltpu.make_async_copy(gd, gg_ref, lsem.at[7])
    out_gg.start()
    for i in (2, 3, 4, 5):
        ro[i].wait_recv()
    moe_sc[...] = (acc[0, 0] + fr[0] + fr[1]).astype(BF16)
    out_moe = pltpu.make_async_copy(moe_sc, moe_ref, lsem.at[11])
    out_moe.start()
    for c in cr + cg + cy + ro + [swap_gg, gg_diag, gg_y, gg_x]:
        c.wait_send()
    for h in order:
        swap_copy(PX, prv, h).wait_send()
    late_y = pltpu.make_async_copy(acc.at[1, 2, lo], my_ref.at[lo], lsem.at[12])
    late_x = pltpu.make_async_copy(acc.at[1, 1, hi], mx_ref.at[hi], lsem.at[13])
    rp[0].wait_recv()
    acc[1, 2, :H] = acc[1, 2, :H] + rd[1, 0]
    late_y.start()
    rp[1].wait_recv()
    acc[1, 1, H:] = acc[1, 1, H:] + rd[1, 1]
    late_x.start()
    for c in rp:
        c.wait_send()
    for c in early + [out_xg, out_c, out_moe, out_gg, late_y, late_x]:
        c.wait()


def publish(T, D, xg_ref, c_ref, du_ref, dv_ref, h_ref, moe_in, gg_in,
            dwg_ref, dwu_ref, dwd_ref, moe_ref, gg_ref):
    rows = xg_ref[...].reshape(T, D)
    dwg_ref[0] = dotg(rows, du_ref[0], TN)
    dwu_ref[0] = dotg(rows, dv_ref[0], TN)
    dwd_ref[0] = dotg(h_ref[0], c_ref[...].reshape(T, D), TN)

    @pl.when(pl.program_id(0) == 0)
    def _():
        moe_ref[...] = moe_in[...]
        gg_ref[...] = gg_in[...]


def solution(mesh):
    tok_spec = P(ALL_AXES, None)
    w_spec = P(EP_AXES, None, None)
    gw_spec = P(ALL_AXES, None, None)

    def local_step(tokens, route_idx, gate_vals, w_gate, w_up, w_down, grad_out):
        T, K = route_idx.shape
        D = tokens.shape[1]
        NE, _, FF = w_gate.shape
        CAP = T * K // (8 * NE)
        hbm = pl.BlockSpec(memory_space=pl.ANY)
        sds = jax.ShapeDtypeStruct
        outs = pl.pallas_call(
            functools.partial(kernel, T, D, FF, NE, CAP),
            out_shape=(sds((T, D), BF16), sds((K, T), F32),
                       sds((T, D), F32), sds((T, D), F32), sds((T, D), F32),
                       sds((8, NE, CAP, D), BF16), sds((8, T, D), BF16),
                       sds((NE, T, FF), BF16), sds((NE, T, FF), BF16), sds((NE, T, FF), BF16)),
            in_specs=[hbm] * 7,
            out_specs=(hbm,) * 10,
            scratch_shapes=[
                pltpu.VMEM((8, T, D), BF16),
                pltpu.VMEM((8, T, D), BF16),
                pltpu.VMEM((8, NE, CAP, D), BF16),
                pltpu.VMEM((NE, T, FF), BF16),
                pltpu.VMEM((NE, T, FF), BF16),
                pltpu.VMEM((NE, T, FF), BF16),
                pltpu.VMEM((8, NE, CAP, D), BF16),
                pltpu.VMEM((NE, D, FF), BF16),
                pltpu.VMEM((NE, D, FF), BF16),
                pltpu.VMEM((NE, FF, D), BF16),
                pltpu.VMEM((2, 4, T, D), F32),
                pltpu.VMEM((2, 2, T // 2, D), F32),
                pltpu.VMEM((2, T, D), F32),
                pltpu.VMEM((4, NE, CAP, D), BF16),
                pltpu.VMEM((4, NE, CAP, D), BF16),
                pltpu.VMEM((T, T), BF16),
                pltpu.VMEM((3, T, T), BF16),
                pltpu.VMEM((8, K, T), jnp.int32),
                pltpu.VMEM((8, K, T), F32),
                pltpu.VMEM((16, NE, T), F32),
                pltpu.VMEM((16, NE, T), F32),
                pltpu.VMEM((16, NE, T), F32),
                pltpu.VMEM((T, 16 * NE), BF16),
                pltpu.VMEM((3, T, 16 * NE), BF16),
                pltpu.VMEM((2, 4, K, T), F32),
                pltpu.VMEM((4, K, T), F32),
                pltpu.VMEM((4, K, T), F32),
                pltpu.VMEM((K, T), F32),
                pltpu.VMEM((2, K, T), F32),
                pltpu.VMEM((T, D), BF16),
                pltpu.SemaphoreType.DMA((N_SEM,)),
                pltpu.SemaphoreType.DMA((N_SEM,)),
                pltpu.SemaphoreType.DMA((17,)),
            ],
            compiler_params=pltpu.CompilerParams(
                collective_id=0, has_side_effects=True, vmem_limit_bytes=67043328),
        )(tokens, grad_out, route_idx.T, gate_vals.T, w_gate, w_up, w_down)
        moe, gg, base, mx, my, xg, c, du, dv, h = outs
        rx = lax.ppermute(mx, 'col', [(0, 1), (1, 0)])
        ry = lax.ppermute(my, 'row', [(0, 1), (1, 0)])

        def per_expert(*shape):
            return pl.BlockSpec((1,) + shape, lambda l: (l, 0, 0))

        def whole(a):
            return pl.BlockSpec(a.shape, lambda l: (0, 0))

        dwg, dwu, dwd, moe, gg = pl.pallas_call(
            functools.partial(publish, T, D),
            grid=(NE,),
            out_shape=(sds((NE, D, FF), F32), sds((NE, D, FF), F32), sds((NE, FF, D), F32),
                       sds(moe.shape, BF16), sds(gg.shape, F32)),
            in_specs=[pl.BlockSpec((8, 1, CAP, D), lambda l: (0, l, 0, 0)),
                      pl.BlockSpec((8, CAP, D), lambda l: (0, l, 0)),
                      per_expert(T, FF), per_expert(T, FF), per_expert(T, FF), whole(moe), whole(gg)],
            out_specs=(per_expert(D, FF), per_expert(D, FF), per_expert(FF, D), whole(moe), whole(gg)),
            cost_estimate=pl.CostEstimate(
                flops=6 * NE * T * D * FF, bytes_accessed=36 * 1024 * 1024, transcendentals=0),
            compiler_params=pltpu.CompilerParams(vmem_limit_bytes=60 * 1024 * 1024),
        )(xg, c, du, dv, h, moe, gg)
        gx = (base + rx + ry).astype(BF16)
        return moe, gx, gg.T, dwg, dwu, dwd

    return jax.shard_map(
        local_step, mesh=mesh,
        in_specs=(tok_spec, tok_spec, tok_spec, w_spec, w_spec, w_spec, tok_spec),
        out_specs=(tok_spec, tok_spec, tok_spec, gw_spec, gw_spec, gw_spec),
        check_vma=False)
```

```python
import functools

import jax
import jax.numpy as jnp
from jax import lax
from jax.experimental import pallas as pl
from jax.experimental.pallas import tpu as pltpu
from jax.sharding import PartitionSpec as P


EP_AXES = ('row', 'col', 'core')
ALL_AXES = ('part', 'row', 'col', 'core')
MESH = pl.DeviceIdType.MESH
F32 = jnp.float32
BF16 = jnp.bfloat16
NT = (((1,), (1,)), ((), ()))
TN = (((0,), (0,)), ((), ()))

AG_X, AG_DY, RG, OX, PX, RS_O, RS_P, GG, N_SEM = 0, 10, 20, 34, 38, 42, 48, 52, 56


FILL_X, FILL_Y = 96, 120


def dot(a, b):
    return jnp.dot(a, b, preferred_element_type=F32)


def dotg(a, b, dims):
    return lax.dot_general(a, b, dims, preferred_element_type=F32)


def kernel(T, D, FF, NE, CAP,
           x_ref, dy_ref, route_ref, gate_ref, wg_ref, wu_ref, wd_ref,
           moe_ref, gg_ref, base_ref, mx_ref, my_ref, fx_ref, fy_ref, xg_ref, c_ref, du_ref, dv_ref, h_ref,
           xa, dya, xg, us, vs, hs, os_, wg, wu, wd, acc, rd, fr, orv, prv,
           pb, sb, ra, ga, rm, gm, mb, rt, gt, gj, gr, gacc, gd, gf, moe_sc,
           ssem, rsem, lsem):
    H = T // 2
    row, col, core = lax.axis_index('row'), lax.axis_index('col'), lax.axis_index('core')
    me = row * 4 + col * 2 + core
    partner = row * 4 + col * 2 + (1 - core)

    def dev(rel):
        return {
            'row': 1 - row if rel & 4 else row,
            'col': 1 - col if rel & 2 else col,
            'core': 1 - core if rel & 1 else core,
        }

    def rc(i, src, dst, rel):
        return pltpu.make_async_remote_copy(
            src_ref=src, dst_ref=dst, send_sem=ssem.at[i], recv_sem=rsem.at[i],
            device_id=dev(rel), device_id_type=MESH)

    def gather_copies(b, buf):
        lo, hi = pl.ds(0, H), pl.ds(H, H)
        return [
            rc(b + 0, buf.at[0], buf.at[1], 1),
            rc(b + 1, buf.at[0, hi], buf.at[2, hi], 2),
            rc(b + 2, buf.at[0, lo], buf.at[2, lo], 2),
            rc(b + 3, buf.at[0, lo], buf.at[4, lo], 4),
            rc(b + 4, buf.at[0, hi], buf.at[4, hi], 4),
            rc(b + 5, buf.at[2, hi], buf.at[6, hi], 4),
            rc(b + 6, buf.at[4, lo], buf.at[6, lo], 2),
            rc(b + 7, buf.at[2], buf.at[3], 1),
            rc(b + 8, buf.at[4], buf.at[5], 1),
            rc(b + 9, buf.at[6], buf.at[7], 1),
        ]

    lx = pltpu.make_async_copy(x_ref, xa.at[0], lsem.at[0])
    ldy = pltpu.make_async_copy(dy_ref, dya.at[0], lsem.at[1])
    lwg = pltpu.make_async_copy(wg_ref, wg, lsem.at[2])
    lwu = pltpu.make_async_copy(wu_ref, wu, lsem.at[3])
    lwd = pltpu.make_async_copy(wd_ref, wd, lsem.at[4])
    lr = pltpu.make_async_copy(route_ref, ra.at[0], lsem.at[14])
    lg = pltpu.make_async_copy(gate_ref, ga.at[0], lsem.at[15])
    lx.start()
    lr.start()
    lg.start()
    ldy.start()
    lwg.start()
    lwu.start()
    lwd.start()

    barrier = pltpu.get_barrier_semaphore()
    for rel in (1, 2, 4):
        pl.semaphore_signal(barrier, inc=1, device_id=dev(rel), device_id_type=MESH)
    pl.semaphore_wait(barrier, 3)

    def small_copies(b, src, buf, diag):
        return [
            rc(b + 0, src, buf.at[1], 1),
            rc(b + 1, src, buf.at[2], 2),
            rc(b + 2, src, buf.at[4], 4),
            rc(b + 3, buf.at[6 - diag], buf.at[6], diag),
            rc(b + 4, buf.at[2], buf.at[3], 1),
            rc(b + 5, buf.at[4], buf.at[5], 1),
            rc(b + 6, buf.at[6], buf.at[7], 1),
        ]

    cr = small_copies(RG, ra.at[0], ra, 2)
    cg = small_copies(RG + 7, ga.at[0], ga, 4)
    cx = gather_copies(AG_X, xa)
    cy = gather_copies(AG_DY, dya)
    lr.wait()
    lg.wait()
    for i in (1, 2, 0):
        cr[i].start()
        cg[i].start()
    lx.wait()
    for i in (1, 3, 0):
        cx[i].start()
    cr[2].wait_recv()
    cr[3].start()
    cg[1].wait_recv()
    cg[3].start()
    cx[2].start()
    cx[4].start()
    cr[5].start()
    cg[4].start()
    cr[1].wait_recv()
    cr[4].start()
    cg[2].wait_recv()
    cg[5].start()

    i0 = lax.broadcasted_iota(jnp.int32, (T, T), 0)
    i1 = lax.broadcasted_iota(jnp.int32, (T, T), 1)
    sb[0] = (i0 < i1).astype(F32).astype(BF16)
    sb[1] = (i0 > i1).astype(F32).astype(BF16)
    sb[2] = (i0 == i1).astype(F32).astype(BF16)
    cx[1].wait_recv()
    cx[5].start()
    cx[3].wait_recv()
    cx[6].start()
    cr[3].wait_recv()
    cr[6].start()
    cg[3].wait_recv()
    cg[6].start()
    for i in (0, 4, 5, 6):
        cr[i].wait_recv()
        cg[i].wait_recv()
    mb[...] = jnp.zeros_like(mb)
    gm[...] = jnp.zeros_like(gm)
    sub = lax.broadcasted_iota(jnp.int32, (NE, T), 0)
    for idx in range(12):
        src = idx if idx < 8 else 2 * (idx - 8)
        owner = me if idx < 8 else partner
        ids = sub + owner * NE
        hits = jnp.zeros((NE, T), F32)
        gates = jnp.zeros((NE, T), F32)
        for j in range(8):
            hit = ra[src, j:j + 1, :] == ids
            hits = hits + jnp.where(hit, 1.0, 0.0)
            gates = gates + jnp.where(hit, ga[src, j:j + 1, :], 0.0)
        mb[idx] = hits
        gm[idx] = gates
    m_all = mb[...].reshape(16 * NE, T)
    m_bf = m_all.astype(BF16)
    ranks = dot(m_bf, sb[0])
    rm[...] = jnp.where(m_all > 0.5, ranks, -1.0).reshape(16, NE, T)
    m_t = dotg(sb[2], m_bf, NT)
    r_t = dotg(sb[1], m_bf, NT)
    rt[...] = jnp.where(m_t > 0.5, r_t, -1.0).astype(BF16)
    g_all = gm[...].reshape(16 * NE, T)
    g_hi = g_all.astype(BF16)
    rest = g_all - g_hi.astype(F32)
    g_mid = rest.astype(BF16)
    g_lo = (rest - g_mid.astype(F32)).astype(BF16)
    for k, piece in enumerate((g_hi, g_mid, g_lo)):
        gt[k] = dotg(sb[2], piece, NT).astype(BF16)

    lane_r = lax.broadcasted_iota(jnp.int32, (CAP, T), 0).astype(F32)

    def build_p(d):
        r_d = rm[d]
        for l in range(NE):
            pb[l * CAP:(l + 1) * CAP, :] = jnp.where(lane_r == r_d[l:l + 1, :], 1.0, 0.0).astype(BF16)

    def gather_x(d):
        build_p(d)
        xg[d] = dot(pb[...], xa[d]).astype(BF16).reshape(NE, CAP, D)

    def gather_x_loop(first, step, count):
        def one(i, carry):
            gather_x(first + step * i)
            return carry
        lax.fori_loop(0, count, one, 0)

    cx[0].wait_recv()
    gather_x_loop(0, 1, 2)
    cx[2].wait_recv()
    cx[7].start()
    cx[4].wait_recv()
    cx[8].start()
    ldy.wait()
    for i in (1, 3, 0, 2, 4):
        cy[i].start()
    gather_x_loop(2, 2, 2)
    cx[7].wait_recv()
    cx[8].wait_recv()
    gather_x_loop(3, 2, 2)
    cx[5].wait_recv()
    cx[6].wait_recv()
    cx[9].start()
    gather_x_loop(6, 1, 1)
    cx[9].wait_recv()
    gather_x_loop(7, 1, 1)

    lwg.wait()
    lwu.wait()
    lwd.wait()

    def forward(l, carry):
        rows = xg[:, pl.ds(l, 1)].reshape(T, D)
        u = dot(rows, wg[l]).astype(BF16)
        v = dot(rows, wu[l]).astype(BF16)
        us[l] = u
        vs[l] = v
        uf = u.astype(F32)
        h = (uf * jax.nn.sigmoid(uf) * v.astype(F32)).astype(BF16)
        o = dot(h, wd[l]).astype(BF16)
        os_[:, pl.ds(l, 1)] = o.reshape(8, 1, CAP, D)
        return carry

    lax.fori_loop(0, NE // 2, forward, 0)
    cy[1].wait_recv()
    cy[5].start()
    cy[3].wait_recv()
    cy[6].start()
    lax.fori_loop(NE // 2, NE, forward, 0)

    order = (3, 1, 2, 0)

    def swap_copy(b, buf, h):
        return rc(b + h, os_.at[2 * h + 1], buf.at[h], 1)

    def reduce_copies(b, k):
        lo, hi = pl.ds(0, H), pl.ds(H, H)
        diag = [
            rc(b + 0, acc.at[k, 3, lo], rd.at[k, 0], 2),
            rc(b + 1, acc.at[k, 3, hi], rd.at[k, 1], 4),
        ]
        if k == 1:
            return diag + [
                rc(b + 2, acc.at[k, 1, pl.ds(0, FILL_X)], fx_ref, 2),
                rc(b + 3, acc.at[k, 2, pl.ds(T - FILL_Y, FILL_Y)], fy_ref, 4),
            ]
        return diag + [
            rc(b + 2, acc.at[k, 1, lo], fr.at[0, lo], 2),
            rc(b + 3, acc.at[k, 2, hi], fr.at[1, hi], 4),
            rc(b + 4, acc.at[k, 1, hi], fr.at[0, hi], 2),
            rc(b + 5, acc.at[k, 2, lo], fr.at[1, lo], 4),
        ]

    e0 = lax.broadcasted_iota(jnp.int32, (16 * NE, T), 0)
    e1 = lax.broadcasted_iota(jnp.int32, (16 * NE, T), 1) // CAP
    rank_lane = lax.rem(lax.broadcasted_iota(jnp.int32, (T, T), 1), CAP).astype(F32)

    def spread(idx, rows, weighted):
        pick = jnp.where(e0 == e1 + idx * NE, 1.0, 0.0).astype(BF16)
        hit = dot(rt[...], pick) == rank_lane
        if weighted:
            for k in range(3):
                sb[k] = jnp.where(hit, dot(gt[k], pick), 0.0).astype(BF16)
            return dot(sb[0], rows) + dot(sb[1], rows) + dot(sb[2], rows)
        sb[0] = jnp.where(hit, 1.0, 0.0).astype(BF16)
        return dot(sb[0], rows)

    def combine_all(k, b, recv, copies, weighted):
        def one(i, carry):
            h = 3 - i
            acc[k, h] = spread(2 * h, os_[2 * h].reshape(T, D), weighted)
            swap_copy(b, recv, h).wait_recv()
            acc[k, h] = acc[k, h] + spread(8 + h, recv[h].reshape(T, D), weighted)

            @pl.when(i == 0)
            def _():
                copies[0].start()
                copies[1].start()

            @pl.when(i == 1)
            def _():
                copies[3].start()

            @pl.when(i == 2)
            def _():
                copies[2].start()
            return carry
        lax.fori_loop(0, 4, one, 0)

    ro = reduce_copies(RS_O, 0)
    for h in order:
        swap_copy(OX, orv, h).start()
    cy[2].wait_recv()
    cy[7].start()
    cy[4].wait_recv()
    cy[8].start()
    combine_all(0, OX, orv, ro, True)

    cy[5].wait_recv()
    cy[6].wait_recv()
    cy[9].start()
    cy[0].wait_recv()
    cy[7].wait_recv()
    cy[8].wait_recv()
    cy[9].wait_recv()
    for c in cx:
        c.wait_send()

    swap_gg = rc(GG, gj.at[1], gr, 1)
    gg_diag = rc(GG + 1, gacc.at[3], gd, 4)
    gg_y = rc(GG + 2, gacc.at[2], gf.at[1], 4)
    gg_x = rc(GG + 3, gacc.at[1], gf.at[0], 2)

    def gather_dy(d, carry):
        build_p(d)
        rows = dot(pb[...], dya[d])
        outs = os_[d].reshape(T, D).astype(F32)
        gg_rows = jnp.sum(rows * outs, axis=1, keepdims=True)
        r_d = rm[d]
        g_d = gm[d]
        r_ids = ra[d]
        gg_d = jnp.zeros((8, T), F32)
        for l in range(NE):
            hit = lane_r == r_d[l:l + 1, :]
            gcol = jnp.sum(jnp.where(hit, g_d[l:l + 1, :], 0.0), axis=1, keepdims=True)
            xa[d, l * CAP:(l + 1) * CAP, :] = (gcol * rows[l * CAP:(l + 1) * CAP, :]).astype(BF16)
            gg_l = jnp.sum(
                jnp.where(hit, gg_rows[l * CAP:(l + 1) * CAP, :], 0.0), axis=0, keepdims=True)
            gg_d = gg_d + jnp.where(r_ids == me * NE + l, gg_l, 0.0)
        gj[lax.rem(d, 2), d // 2] = gg_d
        return carry

    lax.fori_loop(0, 8, gather_dy, 0)
    swap_gg.start()
    for h in order:
        swap_copy(OX, orv, h).wait_send()

    ro[0].wait_recv()
    acc[0, 2, :H] = acc[0, 2, :H] + rd[0, 0]
    ro[5].start()
    ro[1].wait_recv()
    acc[0, 1, H:] = acc[0, 1, H:] + rd[0, 1]
    ro[4].start()
    swap_gg.wait_recv()
    gacc[...] = gj[0] + gr[...]

    def expert_rows(buf, l):
        return buf[:, pl.ds(pl.multiple_of(l * CAP, CAP), CAP), :].reshape(T, D)

    def backward(l, carry):
        dh = dotg(expert_rows(xa, l), wd[l], NT).astype(BF16).astype(F32)
        uf = us[l].astype(F32)
        vf = vs[l].astype(F32)
        s = jax.nn.sigmoid(uf)
        sl = uf * s
        hs[l] = (sl * vf).astype(BF16)
        dv = (dh * sl).astype(BF16)
        du = (dh * vf * (s + sl * (1.0 - s))).astype(BF16)
        us[l] = du
        vs[l] = dv
        pr = (dotg(du, wg[l], NT) + dotg(dv, wu[l], NT)).astype(BF16)
        os_[:, pl.ds(l, 1)] = pr.reshape(8, 1, CAP, D)
        return carry

    gg_diag.start()
    gg_y.start()
    out_xg = pltpu.make_async_copy(xg, xg_ref, lsem.at[5])
    out_c = pltpu.make_async_copy(xa, c_ref, lsem.at[6])
    out_xg.start()
    out_c.start()
    lax.fori_loop(0, NE, backward, 0)

    rp = reduce_copies(RS_P, 1)
    for h in order:
        swap_copy(PX, prv, h).start()
    combine_all(1, PX, prv, rp, False)

    lo, hi = pl.ds(0, H), pl.ds(H, H)
    early = [
        pltpu.make_async_copy(acc.at[1, 0], base_ref, lsem.at[8]),
        pltpu.make_async_copy(acc.at[1, 1, pl.ds(FILL_X, H - FILL_X)],
                              mx_ref.at[pl.ds(0, H - FILL_X)], lsem.at[9]),
        pltpu.make_async_copy(acc.at[1, 2, pl.ds(H, H - FILL_Y)],
                              my_ref.at[pl.ds(H, H - FILL_Y)], lsem.at[10]),
        pltpu.make_async_copy(us, du_ref, lsem.at[14]),
        pltpu.make_async_copy(vs, dv_ref, lsem.at[15]),
        pltpu.make_async_copy(hs, h_ref, lsem.at[16]),
    ]
    for c in early:
        c.start()
    gg_diag.wait_recv()
    gacc[1] = gacc[1] + gd[...]
    gg_x.start()
    gg_x.wait_recv()
    gg_y.wait_recv()
    gd[...] = gacc[0] + gf[0] + gf[1]
    out_gg = pltpu.make_async_copy(gd, gg_ref, lsem.at[7])
    out_gg.start()
    for i in (2, 3, 4, 5):
        ro[i].wait_recv()
    moe_sc[...] = (acc[0, 0] + fr[0] + fr[1]).astype(BF16)
    out_moe = pltpu.make_async_copy(moe_sc, moe_ref, lsem.at[11])
    out_moe.start()
    for c in cr + cg + cy + ro + [swap_gg, gg_diag, gg_y, gg_x]:
        c.wait_send()
    for h in order:
        swap_copy(PX, prv, h).wait_send()
    late_y = pltpu.make_async_copy(acc.at[1, 2, lo], my_ref.at[lo], lsem.at[12])
    late_x = pltpu.make_async_copy(acc.at[1, 1, hi], mx_ref.at[pl.ds(H - FILL_X, H)], lsem.at[13])
    rp[0].wait_recv()
    acc[1, 2, :H] = acc[1, 2, :H] + rd[1, 0]
    late_y.start()
    rp[1].wait_recv()
    acc[1, 1, H:] = acc[1, 1, H:] + rd[1, 1]
    late_x.start()
    rp[2].wait_recv()
    rp[3].wait_recv()
    for c in rp:
        c.wait_send()
    for c in early + [out_xg, out_c, out_moe, out_gg, late_y, late_x]:
        c.wait()


def publish(T, D, xg_ref, c_ref, du_ref, dv_ref, h_ref, moe_in, gg_in,
            dwg_ref, dwu_ref, dwd_ref, moe_ref, gg_ref):
    rows = xg_ref[...].reshape(T, D)
    dwg_ref[0] = dotg(rows, du_ref[0], TN)
    dwu_ref[0] = dotg(rows, dv_ref[0], TN)
    dwd_ref[0] = dotg(h_ref[0], c_ref[...].reshape(T, D), TN)

    @pl.when(pl.program_id(0) == 0)
    def _():
        moe_ref[...] = moe_in[...]
        gg_ref[...] = gg_in[...]


def solution(mesh):
    tok_spec = P(ALL_AXES, None)
    w_spec = P(EP_AXES, None, None)
    gw_spec = P(ALL_AXES, None, None)

    def local_step(tokens, route_idx, gate_vals, w_gate, w_up, w_down, grad_out):
        T, K = route_idx.shape
        D = tokens.shape[1]
        NE, _, FF = w_gate.shape
        CAP = T * K // (8 * NE)
        hbm = pl.BlockSpec(memory_space=pl.ANY)
        sds = jax.ShapeDtypeStruct
        outs = pl.pallas_call(
            functools.partial(kernel, T, D, FF, NE, CAP),
            out_shape=(sds((T, D), BF16), sds((K, T), F32),
                       sds((T, D), F32), sds((T - FILL_X, D), F32), sds((T - FILL_Y, D), F32),
                       sds((FILL_X, D), F32), sds((FILL_Y, D), F32),
                       sds((8, NE, CAP, D), BF16), sds((8, T, D), BF16),
                       sds((NE, T, FF), BF16), sds((NE, T, FF), BF16), sds((NE, T, FF), BF16)),
            in_specs=[hbm] * 7,
            out_specs=(hbm,) * 12,
            scratch_shapes=[
                pltpu.VMEM((8, T, D), BF16),
                pltpu.VMEM((8, T, D), BF16),
                pltpu.VMEM((8, NE, CAP, D), BF16),
                pltpu.VMEM((NE, T, FF), BF16),
                pltpu.VMEM((NE, T, FF), BF16),
                pltpu.VMEM((NE, T, FF), BF16),
                pltpu.VMEM((8, NE, CAP, D), BF16),
                pltpu.VMEM((NE, D, FF), BF16),
                pltpu.VMEM((NE, D, FF), BF16),
                pltpu.VMEM((NE, FF, D), BF16),
                pltpu.VMEM((2, 4, T, D), F32),
                pltpu.VMEM((2, 2, T // 2, D), F32),
                pltpu.VMEM((2, T, D), F32),
                pltpu.VMEM((4, NE, CAP, D), BF16),
                pltpu.VMEM((4, NE, CAP, D), BF16),
                pltpu.VMEM((T, T), BF16),
                pltpu.VMEM((3, T, T), BF16),
                pltpu.VMEM((8, K, T), jnp.int32),
                pltpu.VMEM((8, K, T), F32),
                pltpu.VMEM((16, NE, T), F32),
                pltpu.VMEM((16, NE, T), F32),
                pltpu.VMEM((16, NE, T), F32),
                pltpu.VMEM((T, 16 * NE), BF16),
                pltpu.VMEM((3, T, 16 * NE), BF16),
                pltpu.VMEM((2, 4, K, T), F32),
                pltpu.VMEM((4, K, T), F32),
                pltpu.VMEM((4, K, T), F32),
                pltpu.VMEM((K, T), F32),
                pltpu.VMEM((2, K, T), F32),
                pltpu.VMEM((T, D), BF16),
                pltpu.SemaphoreType.DMA((N_SEM,)),
                pltpu.SemaphoreType.DMA((N_SEM,)),
                pltpu.SemaphoreType.DMA((17,)),
            ],
            compiler_params=pltpu.CompilerParams(
                collective_id=0, has_side_effects=True, vmem_limit_bytes=67043328),
        )(tokens, grad_out, route_idx.T, gate_vals.T, w_gate, w_up, w_down)
        moe, gg, base, mx, my, fx, fy, xg, c, du, dv, h = outs
        rx = lax.ppermute(mx, 'col', [(0, 1), (1, 0)])
        ry = lax.ppermute(my, 'row', [(0, 1), (1, 0)])

        def per_expert(*shape):
            return pl.BlockSpec((1,) + shape, lambda l: (l, 0, 0))

        def whole(a):
            return pl.BlockSpec(a.shape, lambda l: (0, 0))

        dwg, dwu, dwd, moe, gg = pl.pallas_call(
            functools.partial(publish, T, D),
            grid=(NE,),
            out_shape=(sds((NE, D, FF), F32), sds((NE, D, FF), F32), sds((NE, FF, D), F32),
                       sds(moe.shape, BF16), sds(gg.shape, F32)),
            in_specs=[pl.BlockSpec((8, 1, CAP, D), lambda l: (0, l, 0, 0)),
                      pl.BlockSpec((8, CAP, D), lambda l: (0, l, 0)),
                      per_expert(T, FF), per_expert(T, FF), per_expert(T, FF), whole(moe), whole(gg)],
            out_specs=(per_expert(D, FF), per_expert(D, FF), per_expert(FF, D), whole(moe), whole(gg)),
            cost_estimate=pl.CostEstimate(
                flops=6 * NE * T * D * FF, bytes_accessed=36 * 1024 * 1024, transcendentals=0),
            compiler_params=pltpu.CompilerParams(vmem_limit_bytes=60 * 1024 * 1024),
        )(xg, c, du, dv, h, moe, gg)
        gx = (base + jnp.concatenate([fx, rx]) + jnp.concatenate([ry, fy])).astype(BF16)
        return moe, gx, gg.T, dwg, dwu, dwd

    return jax.shard_map(
        local_step, mesh=mesh,
        in_specs=(tok_spec, tok_spec, tok_spec, w_spec, w_spec, w_spec, tok_spec),
        out_specs=(tok_spec, tok_spec, tok_spec, gw_spec, gw_spec, gw_spec),
        check_vma=False)
```

```python
import functools

import jax
import jax.numpy as jnp
from jax import lax
from jax.experimental import pallas as pl
from jax.experimental.pallas import tpu as pltpu
from jax.sharding import PartitionSpec as P


EP_AXES = ('row', 'col', 'core')
ALL_AXES = ('part', 'row', 'col', 'core')
MESH = pl.DeviceIdType.MESH
F32 = jnp.float32
BF16 = jnp.bfloat16
NT = (((1,), (1,)), ((), ()))
TN = (((0,), (0,)), ((), ()))

AG_X, AG_DY, RG, OX, PX, RS_O, RS_P, GG, N_SEM = 0, 10, 20, 34, 38, 42, 48, 52, 56


FILL_X, FILL_Y = 104, 96


def dot(a, b):
    return jnp.dot(a, b, preferred_element_type=F32)


def dotg(a, b, dims):
    return lax.dot_general(a, b, dims, preferred_element_type=F32)


def kernel(T, D, FF, NE, CAP,
           x_ref, dy_ref, route_ref, gate_ref, wg_ref, wu_ref, wd_ref,
           moe_ref, gg_ref, base_ref, mx_ref, my_ref, fx_ref, fy_ref, xg_ref, c_ref, du_ref, dv_ref, h_ref,
           xa, dya, xg, us, vs, hs, os_, wg, wu, wd, acc, rd, fr, orv, prv,
           pb, sb, ra, ga, rm, gm, mb, rt, gt, gj, gr, gacc, gd, gf, moe_sc,
           ssem, rsem, lsem):
    H = T // 2
    row, col, core = lax.axis_index('row'), lax.axis_index('col'), lax.axis_index('core')
    me = row * 4 + col * 2 + core
    partner = row * 4 + col * 2 + (1 - core)

    def dev(rel):
        return {
            'row': 1 - row if rel & 4 else row,
            'col': 1 - col if rel & 2 else col,
            'core': 1 - core if rel & 1 else core,
        }

    def rc(i, src, dst, rel):
        return pltpu.make_async_remote_copy(
            src_ref=src, dst_ref=dst, send_sem=ssem.at[i], recv_sem=rsem.at[i],
            device_id=dev(rel), device_id_type=MESH)

    def gather_copies(b, buf):
        lo, hi = pl.ds(0, H), pl.ds(H, H)
        return [
            rc(b + 0, buf.at[0], buf.at[1], 1),
            rc(b + 1, buf.at[0, hi], buf.at[2, hi], 2),
            rc(b + 2, buf.at[0, lo], buf.at[2, lo], 2),
            rc(b + 3, buf.at[0, lo], buf.at[4, lo], 4),
            rc(b + 4, buf.at[0, hi], buf.at[4, hi], 4),
            rc(b + 5, buf.at[2, hi], buf.at[6, hi], 4),
            rc(b + 6, buf.at[4, lo], buf.at[6, lo], 2),
            rc(b + 7, buf.at[2], buf.at[3], 1),
            rc(b + 8, buf.at[4], buf.at[5], 1),
            rc(b + 9, buf.at[6], buf.at[7], 1),
        ]

    lx = pltpu.make_async_copy(x_ref, xa.at[0], lsem.at[0])
    ldy = pltpu.make_async_copy(dy_ref, dya.at[0], lsem.at[1])
    lwg = pltpu.make_async_copy(wg_ref, wg, lsem.at[2])
    lwu = pltpu.make_async_copy(wu_ref, wu, lsem.at[3])
    lwd = pltpu.make_async_copy(wd_ref, wd, lsem.at[4])
    lr = pltpu.make_async_copy(route_ref, ra.at[0], lsem.at[14])
    lg = pltpu.make_async_copy(gate_ref, ga.at[0], lsem.at[15])
    lx.start()
    lr.start()
    lg.start()
    ldy.start()
    lwg.start()
    lwu.start()
    lwd.start()

    barrier = pltpu.get_barrier_semaphore()
    for rel in (1, 2, 4):
        pl.semaphore_signal(barrier, inc=1, device_id=dev(rel), device_id_type=MESH)
    pl.semaphore_wait(barrier, 3)

    def small_copies(b, src, buf, diag):
        return [
            rc(b + 0, src, buf.at[1], 1),
            rc(b + 1, src, buf.at[2], 2),
            rc(b + 2, src, buf.at[4], 4),
            rc(b + 3, buf.at[6 - diag], buf.at[6], diag),
            rc(b + 4, buf.at[2], buf.at[3], 1),
            rc(b + 5, buf.at[4], buf.at[5], 1),
            rc(b + 6, buf.at[6], buf.at[7], 1),
        ]

    cr = small_copies(RG, ra.at[0], ra, 2)
    cg = small_copies(RG + 7, ga.at[0], ga, 4)
    cx = gather_copies(AG_X, xa)
    cy = gather_copies(AG_DY, dya)
    lr.wait()
    lg.wait()
    for i in (1, 2, 0):
        cr[i].start()
        cg[i].start()
    lx.wait()
    for i in (1, 3, 0):
        cx[i].start()
    cr[2].wait_recv()
    cr[3].start()
    cg[1].wait_recv()
    cg[3].start()
    cx[2].start()
    cx[4].start()
    cr[5].start()
    cg[4].start()
    cr[1].wait_recv()
    cr[4].start()
    cg[2].wait_recv()
    cg[5].start()

    i0 = lax.broadcasted_iota(jnp.int32, (T, T), 0)
    i1 = lax.broadcasted_iota(jnp.int32, (T, T), 1)
    sb[0] = (i0 < i1).astype(F32).astype(BF16)
    sb[1] = (i0 > i1).astype(F32).astype(BF16)
    sb[2] = (i0 == i1).astype(F32).astype(BF16)
    cx[1].wait_recv()
    cx[5].start()
    cx[3].wait_recv()
    cx[6].start()
    cr[3].wait_recv()
    cr[6].start()
    cg[3].wait_recv()
    cg[6].start()
    for i in (0, 4, 5, 6):
        cr[i].wait_recv()
        cg[i].wait_recv()
    mb[...] = jnp.zeros_like(mb)
    gm[...] = jnp.zeros_like(gm)
    sub = lax.broadcasted_iota(jnp.int32, (NE, T), 0)
    for idx in range(12):
        src = idx if idx < 8 else 2 * (idx - 8)
        owner = me if idx < 8 else partner
        ids = sub + owner * NE
        hits = jnp.zeros((NE, T), F32)
        gates = jnp.zeros((NE, T), F32)
        for j in range(8):
            hit = ra[src, j:j + 1, :] == ids
            hits = hits + jnp.where(hit, 1.0, 0.0)
            gates = gates + jnp.where(hit, ga[src, j:j + 1, :], 0.0)
        mb[idx] = hits
        gm[idx] = gates
    m_all = mb[...].reshape(16 * NE, T)
    m_bf = m_all.astype(BF16)
    ranks = dot(m_bf, sb[0])
    rm[...] = jnp.where(m_all > 0.5, ranks, -1.0).reshape(16, NE, T)
    m_t = dotg(sb[2], m_bf, NT)
    r_t = dotg(sb[1], m_bf, NT)
    rt[...] = jnp.where(m_t > 0.5, r_t, -1.0).astype(BF16)
    g_all = gm[...].reshape(16 * NE, T)
    g_hi = g_all.astype(BF16)
    rest = g_all - g_hi.astype(F32)
    g_mid = rest.astype(BF16)
    g_lo = (rest - g_mid.astype(F32)).astype(BF16)
    for k, piece in enumerate((g_hi, g_mid, g_lo)):
        gt[k] = dotg(sb[2], piece, NT).astype(BF16)

    lane_r = lax.broadcasted_iota(jnp.int32, (CAP, T), 0).astype(F32)

    def build_p(d):
        r_d = rm[d]
        for l in range(NE):
            pb[l * CAP:(l + 1) * CAP, :] = jnp.where(lane_r == r_d[l:l + 1, :], 1.0, 0.0).astype(BF16)

    def gather_x(d):
        build_p(d)
        xg[d] = dot(pb[...], xa[d]).astype(BF16).reshape(NE, CAP, D)

    def gather_x_loop(first, step, count):
        def one(i, carry):
            gather_x(first + step * i)
            return carry
        lax.fori_loop(0, count, one, 0)

    cx[0].wait_recv()
    gather_x_loop(0, 1, 2)
    cx[2].wait_recv()
    cx[7].start()
    cx[4].wait_recv()
    cx[8].start()
    ldy.wait()
    for i in (1, 3, 0, 2, 4):
        cy[i].start()
    gather_x_loop(2, 2, 2)
    cx[7].wait_recv()
    cx[8].wait_recv()
    gather_x_loop(3, 2, 2)
    cx[5].wait_recv()
    cx[6].wait_recv()
    cx[9].start()
    gather_x_loop(6, 1, 1)
    cx[9].wait_recv()
    gather_x_loop(7, 1, 1)

    lwg.wait()
    lwu.wait()
    lwd.wait()

    def forward(l, carry):
        rows = xg[:, pl.ds(l, 1)].reshape(T, D)
        u = dot(rows, wg[l]).astype(BF16)
        v = dot(rows, wu[l]).astype(BF16)
        us[l] = u
        vs[l] = v
        uf = u.astype(F32)
        h = (uf * jax.nn.sigmoid(uf) * v.astype(F32)).astype(BF16)
        o = dot(h, wd[l]).astype(BF16)
        os_[:, pl.ds(l, 1)] = o.reshape(8, 1, CAP, D)
        return carry

    lax.fori_loop(0, NE // 2, forward, 0)
    cy[1].wait_recv()
    cy[5].start()
    cy[3].wait_recv()
    cy[6].start()
    lax.fori_loop(NE // 2, NE, forward, 0)

    order = (3, 1, 2, 0)

    def swap_copy(b, buf, h):
        return rc(b + h, os_.at[2 * h + 1], buf.at[h], 1)

    def reduce_copies(b, k):
        lo, hi = pl.ds(0, H), pl.ds(H, H)
        diag = [
            rc(b + 0, acc.at[k, 3, lo], rd.at[k, 0], 2),
            rc(b + 1, acc.at[k, 3, hi], rd.at[k, 1], 4),
        ]
        if k == 1:
            return diag + [
                rc(b + 2, acc.at[k, 1, pl.ds(0, FILL_X)], fx_ref, 2),
                rc(b + 3, acc.at[k, 2, pl.ds(T - FILL_Y, FILL_Y)], fy_ref, 4),
            ]
        return diag + [
            rc(b + 2, acc.at[k, 1, lo], fr.at[0, lo], 2),
            rc(b + 3, acc.at[k, 2, hi], fr.at[1, hi], 4),
            rc(b + 4, acc.at[k, 1, hi], fr.at[0, hi], 2),
            rc(b + 5, acc.at[k, 2, lo], fr.at[1, lo], 4),
        ]

    e0 = lax.broadcasted_iota(jnp.int32, (16 * NE, T), 0)
    e1 = lax.broadcasted_iota(jnp.int32, (16 * NE, T), 1) // CAP
    rank_lane = lax.rem(lax.broadcasted_iota(jnp.int32, (T, T), 1), CAP).astype(F32)

    def spread(idx, rows, weighted):
        pick = jnp.where(e0 == e1 + idx * NE, 1.0, 0.0).astype(BF16)
        hit = dot(rt[...], pick) == rank_lane
        if weighted:
            for k in range(3):
                sb[k] = jnp.where(hit, dot(gt[k], pick), 0.0).astype(BF16)
            return dot(sb[0], rows) + dot(sb[1], rows) + dot(sb[2], rows)
        sb[0] = jnp.where(hit, 1.0, 0.0).astype(BF16)
        return dot(sb[0], rows)

    def combine_all(k, b, recv, copies, weighted):
        def one(i, carry):
            h = 3 - i
            acc[k, h] = spread(2 * h, os_[2 * h].reshape(T, D), weighted)
            swap_copy(b, recv, h).wait_recv()
            acc[k, h] = acc[k, h] + spread(8 + h, recv[h].reshape(T, D), weighted)

            @pl.when(i == 0)
            def _():
                copies[0].start()
                copies[1].start()

            @pl.when(i == 1)
            def _():
                copies[3].start()

            @pl.when(i == 2)
            def _():
                copies[2].start()
            return carry
        lax.fori_loop(0, 4, one, 0)

    ro = reduce_copies(RS_O, 0)
    for h in order:
        swap_copy(OX, orv, h).start()
    cy[2].wait_recv()
    cy[7].start()
    cy[4].wait_recv()
    cy[8].start()
    combine_all(0, OX, orv, ro, True)

    cy[5].wait_recv()
    cy[6].wait_recv()
    cy[9].start()
    cy[0].wait_recv()
    cy[7].wait_recv()
    cy[8].wait_recv()
    cy[9].wait_recv()
    for c in cx:
        c.wait_send()

    swap_gg = rc(GG, gj.at[1], gr, 1)
    gg_diag = rc(GG + 1, gacc.at[3], gd, 4)
    gg_y = rc(GG + 2, gacc.at[2], gf.at[1], 4)
    gg_x = rc(GG + 3, gacc.at[1], gf.at[0], 2)

    def gather_dy(d, carry):
        build_p(d)
        rows = dot(pb[...], dya[d])
        outs = os_[d].reshape(T, D).astype(F32)
        gg_rows = jnp.sum(rows * outs, axis=1, keepdims=True)
        r_d = rm[d]
        g_d = gm[d]
        r_ids = ra[d]
        gg_d = jnp.zeros((8, T), F32)
        for l in range(NE):
            hit = lane_r == r_d[l:l + 1, :]
            gcol = jnp.sum(jnp.where(hit, g_d[l:l + 1, :], 0.0), axis=1, keepdims=True)
            xa[d, l * CAP:(l + 1) * CAP, :] = (gcol * rows[l * CAP:(l + 1) * CAP, :]).astype(BF16)
            gg_l = jnp.sum(
                jnp.where(hit, gg_rows[l * CAP:(l + 1) * CAP, :], 0.0), axis=0, keepdims=True)
            gg_d = gg_d + jnp.where(r_ids == me * NE + l, gg_l, 0.0)
        gj[lax.rem(d, 2), d // 2] = gg_d
        return carry

    lax.fori_loop(0, 8, gather_dy, 0)
    swap_gg.start()
    for h in order:
        swap_copy(OX, orv, h).wait_send()

    ro[0].wait_recv()
    acc[0, 2, :H] = acc[0, 2, :H] + rd[0, 0]
    ro[5].start()
    ro[1].wait_recv()
    acc[0, 1, H:] = acc[0, 1, H:] + rd[0, 1]
    ro[4].start()
    swap_gg.wait_recv()
    gacc[...] = gj[0] + gr[...]

    def expert_rows(buf, l):
        return buf[:, pl.ds(pl.multiple_of(l * CAP, CAP), CAP), :].reshape(T, D)

    def backward(l, carry):
        dh = dotg(expert_rows(xa, l), wd[l], NT).astype(BF16).astype(F32)
        uf = us[l].astype(F32)
        vf = vs[l].astype(F32)
        s = jax.nn.sigmoid(uf)
        sl = uf * s
        hs[l] = (sl * vf).astype(BF16)
        dv = (dh * sl).astype(BF16)
        du = (dh * vf * (s + sl * (1.0 - s))).astype(BF16)
        us[l] = du
        vs[l] = dv
        pr = (dotg(du, wg[l], NT) + dotg(dv, wu[l], NT)).astype(BF16)
        os_[:, pl.ds(l, 1)] = pr.reshape(8, 1, CAP, D)
        return carry

    gg_diag.start()
    gg_y.start()
    out_xg = pltpu.make_async_copy(xg, xg_ref, lsem.at[5])
    out_c = pltpu.make_async_copy(xa, c_ref, lsem.at[6])
    out_xg.start()
    out_c.start()
    lax.fori_loop(0, NE, backward, 0)

    rp = reduce_copies(RS_P, 1)
    for h in order:
        swap_copy(PX, prv, h).start()
    combine_all(1, PX, prv, rp, False)

    lo, hi = pl.ds(0, H), pl.ds(H, H)
    early = [
        pltpu.make_async_copy(acc.at[1, 0], base_ref, lsem.at[8]),
        pltpu.make_async_copy(acc.at[1, 1, pl.ds(FILL_X, H - FILL_X)],
                              mx_ref.at[pl.ds(0, H - FILL_X)], lsem.at[9]),
        pltpu.make_async_copy(acc.at[1, 2, pl.ds(H, H - FILL_Y)],
                              my_ref.at[pl.ds(H, H - FILL_Y)], lsem.at[10]),
        pltpu.make_async_copy(us, du_ref, lsem.at[14]),
        pltpu.make_async_copy(vs, dv_ref, lsem.at[15]),
        pltpu.make_async_copy(hs, h_ref, lsem.at[16]),
    ]
    for c in early:
        c.start()
    gg_diag.wait_recv()
    gacc[1] = gacc[1] + gd[...]
    gg_x.start()
    gg_x.wait_recv()
    gg_y.wait_recv()
    gd[...] = gacc[0] + gf[0] + gf[1]
    out_gg = pltpu.make_async_copy(gd, gg_ref, lsem.at[7])
    out_gg.start()
    for i in (2, 3, 4, 5):
        ro[i].wait_recv()
    moe_sc[...] = (acc[0, 0] + fr[0] + fr[1]).astype(BF16)
    out_moe = pltpu.make_async_copy(moe_sc, moe_ref, lsem.at[11])
    out_moe.start()
    for c in cr + cg + cy + ro + [swap_gg, gg_diag, gg_y, gg_x]:
        c.wait_send()
    for h in order:
        swap_copy(PX, prv, h).wait_send()
    late_y = pltpu.make_async_copy(acc.at[1, 2, lo], my_ref.at[lo], lsem.at[12])
    late_x = pltpu.make_async_copy(acc.at[1, 1, hi], mx_ref.at[pl.ds(H - FILL_X, H)], lsem.at[13])
    rp[0].wait_recv()
    acc[1, 2, :H] = acc[1, 2, :H] + rd[1, 0]
    late_y.start()
    rp[1].wait_recv()
    acc[1, 1, H:] = acc[1, 1, H:] + rd[1, 1]
    late_x.start()
    rp[2].wait_recv()
    rp[3].wait_recv()
    for c in rp:
        c.wait_send()
    for c in early + [out_xg, out_c, out_moe, out_gg, late_y, late_x]:
        c.wait()


def publish(T, D, xg_ref, c_ref, du_ref, dv_ref, h_ref, moe_in, gg_in,
            dwg_ref, dwu_ref, dwd_ref, moe_ref, gg_ref):
    rows = xg_ref[...].reshape(T, D)
    dwg_ref[0] = dotg(rows, du_ref[0], TN)
    dwu_ref[0] = dotg(rows, dv_ref[0], TN)
    dwd_ref[0] = dotg(h_ref[0], c_ref[...].reshape(T, D), TN)

    @pl.when(pl.program_id(0) == 0)
    def _():
        moe_ref[...] = moe_in[...]
        gg_ref[...] = gg_in[...]


def solution(mesh):
    tok_spec = P(ALL_AXES, None)
    w_spec = P(EP_AXES, None, None)
    gw_spec = P(ALL_AXES, None, None)

    def local_step(tokens, route_idx, gate_vals, w_gate, w_up, w_down, grad_out):
        T, K = route_idx.shape
        D = tokens.shape[1]
        NE, _, FF = w_gate.shape
        CAP = T * K // (8 * NE)
        hbm = pl.BlockSpec(memory_space=pl.ANY)
        sds = jax.ShapeDtypeStruct
        outs = pl.pallas_call(
            functools.partial(kernel, T, D, FF, NE, CAP),
            out_shape=(sds((T, D), BF16), sds((K, T), F32),
                       sds((T, D), F32), sds((T - FILL_X, D), F32), sds((T - FILL_Y, D), F32),
                       sds((FILL_X, D), F32), sds((FILL_Y, D), F32),
                       sds((8, NE, CAP, D), BF16), sds((8, T, D), BF16),
                       sds((NE, T, FF), BF16), sds((NE, T, FF), BF16), sds((NE, T, FF), BF16)),
            in_specs=[hbm] * 7,
            out_specs=(hbm,) * 12,
            scratch_shapes=[
                pltpu.VMEM((8, T, D), BF16),
                pltpu.VMEM((8, T, D), BF16),
                pltpu.VMEM((8, NE, CAP, D), BF16),
                pltpu.VMEM((NE, T, FF), BF16),
                pltpu.VMEM((NE, T, FF), BF16),
                pltpu.VMEM((NE, T, FF), BF16),
                pltpu.VMEM((8, NE, CAP, D), BF16),
                pltpu.VMEM((NE, D, FF), BF16),
                pltpu.VMEM((NE, D, FF), BF16),
                pltpu.VMEM((NE, FF, D), BF16),
                pltpu.VMEM((2, 4, T, D), F32),
                pltpu.VMEM((2, 2, T // 2, D), F32),
                pltpu.VMEM((2, T, D), F32),
                pltpu.VMEM((4, NE, CAP, D), BF16),
                pltpu.VMEM((4, NE, CAP, D), BF16),
                pltpu.VMEM((T, T), BF16),
                pltpu.VMEM((3, T, T), BF16),
                pltpu.VMEM((8, K, T), jnp.int32),
                pltpu.VMEM((8, K, T), F32),
                pltpu.VMEM((16, NE, T), F32),
                pltpu.VMEM((16, NE, T), F32),
                pltpu.VMEM((16, NE, T), F32),
                pltpu.VMEM((T, 16 * NE), BF16),
                pltpu.VMEM((3, T, 16 * NE), BF16),
                pltpu.VMEM((2, 4, K, T), F32),
                pltpu.VMEM((4, K, T), F32),
                pltpu.VMEM((4, K, T), F32),
                pltpu.VMEM((K, T), F32),
                pltpu.VMEM((2, K, T), F32),
                pltpu.VMEM((T, D), BF16),
                pltpu.SemaphoreType.DMA((N_SEM,)),
                pltpu.SemaphoreType.DMA((N_SEM,)),
                pltpu.SemaphoreType.DMA((17,)),
            ],
            compiler_params=pltpu.CompilerParams(
                collective_id=0, has_side_effects=True, vmem_limit_bytes=67043328),
        )(tokens, grad_out, route_idx.T, gate_vals.T, w_gate, w_up, w_down)
        moe, gg, base, mx, my, fx, fy, xg, c, du, dv, h = outs
        rx = lax.ppermute(mx, 'col', [(0, 1), (1, 0)])
        ry = lax.ppermute(my, 'row', [(0, 1), (1, 0)])

        def per_expert(*shape):
            return pl.BlockSpec((1,) + shape, lambda l: (l, 0, 0))

        def whole(a):
            return pl.BlockSpec(a.shape, lambda l: (0, 0))

        dwg, dwu, dwd, moe, gg = pl.pallas_call(
            functools.partial(publish, T, D),
            grid=(NE,),
            out_shape=(sds((NE, D, FF), F32), sds((NE, D, FF), F32), sds((NE, FF, D), F32),
                       sds(moe.shape, BF16), sds(gg.shape, F32)),
            in_specs=[pl.BlockSpec((8, 1, CAP, D), lambda l: (0, l, 0, 0)),
                      pl.BlockSpec((8, CAP, D), lambda l: (0, l, 0)),
                      per_expert(T, FF), per_expert(T, FF), per_expert(T, FF), whole(moe), whole(gg)],
            out_specs=(per_expert(D, FF), per_expert(D, FF), per_expert(FF, D), whole(moe), whole(gg)),
            cost_estimate=pl.CostEstimate(
                flops=6 * NE * T * D * FF, bytes_accessed=36 * 1024 * 1024, transcendentals=0),
            compiler_params=pltpu.CompilerParams(vmem_limit_bytes=60 * 1024 * 1024),
        )(xg, c, du, dv, h, moe, gg)
        gx = (base + jnp.concatenate([fx, rx]) + jnp.concatenate([ry, fy])).astype(BF16)
        return moe, gx, gg.T, dwg, dwu, dwd

    return jax.shard_map(
        local_step, mesh=mesh,
        in_specs=(tok_spec, tok_spec, tok_spec, w_spec, w_spec, w_spec, tok_spec),
        out_specs=(tok_spec, tok_spec, tok_spec, gw_spec, gw_spec, gw_spec),
        check_vma=False)
```

```python
import functools

import jax
import jax.numpy as jnp
from jax import lax
from jax.experimental import pallas as pl
from jax.experimental.pallas import tpu as pltpu
from jax.sharding import PartitionSpec as P


EP_AXES = ('row', 'col', 'core')
ALL_AXES = ('part', 'row', 'col', 'core')
MESH = pl.DeviceIdType.MESH
F32 = jnp.float32
BF16 = jnp.bfloat16
NT = (((1,), (1,)), ((), ()))
TN = (((0,), (0,)), ((), ()))

AG_X, AG_DY, RG, OX, PX, RS_O, RS_P, GG, N_SEM = 0, 10, 20, 34, 38, 42, 48, 52, 56


FILL_X, FILL_Y = 104, 96


def dot(a, b):
    return jnp.dot(a, b, preferred_element_type=F32)


def dotg(a, b, dims):
    return lax.dot_general(a, b, dims, preferred_element_type=F32)


def kernel(T, D, FF, NE, CAP,
           x_ref, dy_ref, route_ref, gate_ref, wg_ref, wu_ref, wd_ref,
           moe_ref, gg_ref, base_ref, mx_ref, my_ref, fx_ref, fy_ref, xg_ref, c_ref, du_ref, dv_ref, h_ref,
           xa, dya, xg, us, vs, hs, os_, wg, wu, wd, acc, rd, fr, orv, prv,
           pb, sb, ra, ga, rm, gm, mb, rt, gt, gj, gr, gacc, gd, gf, moe_sc,
           ssem, rsem, lsem):
    H = T // 2
    row, col, core = lax.axis_index('row'), lax.axis_index('col'), lax.axis_index('core')
    me = row * 4 + col * 2 + core
    partner = row * 4 + col * 2 + (1 - core)

    def dev(rel):
        return {
            'row': 1 - row if rel & 4 else row,
            'col': 1 - col if rel & 2 else col,
            'core': 1 - core if rel & 1 else core,
        }

    def rc(i, src, dst, rel):
        return pltpu.make_async_remote_copy(
            src_ref=src, dst_ref=dst, send_sem=ssem.at[i], recv_sem=rsem.at[i],
            device_id=dev(rel), device_id_type=MESH)

    def gather_copies(b, buf):
        lo, hi = pl.ds(0, H), pl.ds(H, H)
        return [
            rc(b + 0, buf.at[0], buf.at[1], 1),
            rc(b + 1, buf.at[0, hi], buf.at[2, hi], 2),
            rc(b + 2, buf.at[0, lo], buf.at[2, lo], 2),
            rc(b + 3, buf.at[0, lo], buf.at[4, lo], 4),
            rc(b + 4, buf.at[0, hi], buf.at[4, hi], 4),
            rc(b + 5, buf.at[2, hi], buf.at[6, hi], 4),
            rc(b + 6, buf.at[4, lo], buf.at[6, lo], 2),
            rc(b + 7, buf.at[2], buf.at[3], 1),
            rc(b + 8, buf.at[4], buf.at[5], 1),
            rc(b + 9, buf.at[6], buf.at[7], 1),
        ]

    lx = pltpu.make_async_copy(x_ref, xa.at[0], lsem.at[0])
    ldy = pltpu.make_async_copy(dy_ref, dya.at[0], lsem.at[1])
    lwg = pltpu.make_async_copy(wg_ref, wg, lsem.at[2])
    lwu = pltpu.make_async_copy(wu_ref, wu, lsem.at[3])
    lwd = pltpu.make_async_copy(wd_ref, wd, lsem.at[4])
    lr = pltpu.make_async_copy(route_ref, ra.at[0], lsem.at[14])
    lg = pltpu.make_async_copy(gate_ref, ga.at[0], lsem.at[15])
    lx.start()
    lr.start()
    lg.start()
    ldy.start()
    lwg.start()
    lwu.start()
    lwd.start()

    barrier = pltpu.get_barrier_semaphore()
    for rel in (1, 2, 4):
        pl.semaphore_signal(barrier, inc=1, device_id=dev(rel), device_id_type=MESH)
    pl.semaphore_wait(barrier, 3)

    def small_copies(b, src, buf, diag):
        return [
            rc(b + 0, src, buf.at[1], 1),
            rc(b + 1, src, buf.at[2], 2),
            rc(b + 2, src, buf.at[4], 4),
            rc(b + 3, buf.at[6 - diag], buf.at[6], diag),
            rc(b + 4, buf.at[2], buf.at[3], 1),
            rc(b + 5, buf.at[4], buf.at[5], 1),
            rc(b + 6, buf.at[6], buf.at[7], 1),
        ]

    cr = small_copies(RG, ra.at[0], ra, 2)
    cg = small_copies(RG + 7, ga.at[0], ga, 4)
    cx = gather_copies(AG_X, xa)
    cy = gather_copies(AG_DY, dya)
    lr.wait()
    lg.wait()
    for i in (1, 2, 0):
        cr[i].start()
        cg[i].start()
    lx.wait()
    for i in (1, 3, 0):
        cx[i].start()
    cr[2].wait_recv()
    cr[3].start()
    cg[1].wait_recv()
    cg[3].start()
    cx[2].start()
    cx[4].start()
    cr[5].start()
    cg[4].start()
    cr[1].wait_recv()
    cr[4].start()
    cg[2].wait_recv()
    cg[5].start()

    i0 = lax.broadcasted_iota(jnp.int32, (T, T), 0)
    i1 = lax.broadcasted_iota(jnp.int32, (T, T), 1)
    sb[0] = (i0 < i1).astype(F32).astype(BF16)
    sb[1] = (i0 > i1).astype(F32).astype(BF16)
    sb[2] = (i0 == i1).astype(F32).astype(BF16)
    cx[1].wait_recv()
    cx[5].start()
    cx[3].wait_recv()
    cx[6].start()
    cr[3].wait_recv()
    cr[6].start()
    cg[3].wait_recv()
    cg[6].start()
    for i in (0, 4, 5, 6):
        cr[i].wait_recv()
        cg[i].wait_recv()
    mb[...] = jnp.zeros_like(mb)
    gm[...] = jnp.zeros_like(gm)
    sub = lax.broadcasted_iota(jnp.int32, (NE, T), 0)
    for idx in range(12):
        src = idx if idx < 8 else 2 * (idx - 8)
        owner = me if idx < 8 else partner
        ids = sub + owner * NE
        hits = jnp.zeros((NE, T), F32)
        gates = jnp.zeros((NE, T), F32)
        for j in range(8):
            hit = ra[src, j:j + 1, :] == ids
            hits = hits + jnp.where(hit, 1.0, 0.0)
            gates = gates + jnp.where(hit, ga[src, j:j + 1, :], 0.0)
        mb[idx] = hits
        gm[idx] = gates
    m_all = mb[...].reshape(16 * NE, T)
    m_bf = m_all.astype(BF16)
    ranks = dot(m_bf, sb[0])
    rm[...] = jnp.where(m_all > 0.5, ranks, -1.0).reshape(16, NE, T)
    m_t = dotg(sb[2], m_bf, NT)
    r_t = dotg(sb[1], m_bf, NT)
    rt[...] = jnp.where(m_t > 0.5, r_t, -1.0).astype(BF16)
    g_all = gm[...].reshape(16 * NE, T)
    g_hi = g_all.astype(BF16)
    rest = g_all - g_hi.astype(F32)
    g_mid = rest.astype(BF16)
    g_lo = (rest - g_mid.astype(F32)).astype(BF16)
    for k, piece in enumerate((g_hi, g_mid, g_lo)):
        gt[k] = dotg(sb[2], piece, NT).astype(BF16)

    lane_r = lax.broadcasted_iota(jnp.int32, (CAP, T), 0).astype(F32)

    def build_p(d):
        r_d = rm[d]
        for l in range(NE):
            pb[l * CAP:(l + 1) * CAP, :] = jnp.where(lane_r == r_d[l:l + 1, :], 1.0, 0.0).astype(BF16)

    def gather_x(d):
        build_p(d)
        xg[d] = dot(pb[...], xa[d]).astype(BF16).reshape(NE, CAP, D)

    def gather_x_loop(first, step, count):
        def one(i, carry):
            gather_x(first + step * i)
            return carry
        lax.fori_loop(0, count, one, 0)

    cx[0].wait_recv()
    gather_x_loop(0, 1, 2)
    cx[2].wait_recv()
    cx[7].start()
    cx[4].wait_recv()
    cx[8].start()
    ldy.wait()
    for i in (1, 3, 0, 2, 4):
        cy[i].start()
    gather_x_loop(2, 2, 2)
    cx[7].wait_recv()
    cx[8].wait_recv()
    gather_x_loop(3, 2, 2)
    cx[5].wait_recv()
    cx[6].wait_recv()
    cx[9].start()
    gather_x_loop(6, 1, 1)
    cx[9].wait_recv()
    gather_x_loop(7, 1, 1)

    lwg.wait()
    lwu.wait()
    lwd.wait()

    def forward(l, carry):
        rows = xg[:, pl.ds(l, 1)].reshape(T, D)
        u = dot(rows, wg[l]).astype(BF16)
        v = dot(rows, wu[l]).astype(BF16)
        us[l] = u
        vs[l] = v
        uf = u.astype(F32)
        h = (uf * jax.nn.sigmoid(uf) * v.astype(F32)).astype(BF16)
        o = dot(h, wd[l]).astype(BF16)
        os_[:, pl.ds(l, 1)] = o.reshape(8, 1, CAP, D)
        return carry

    lax.fori_loop(0, NE // 2, forward, 0)
    cy[1].wait_recv()
    cy[5].start()
    cy[3].wait_recv()
    cy[6].start()
    lax.fori_loop(NE // 2, NE, forward, 0)

    order = (3, 1, 2, 0)

    def swap_copy(b, buf, h):
        return rc(b + h, os_.at[2 * h + 1], buf.at[h], 1)

    def reduce_copies(b, k):
        lo, hi = pl.ds(0, H), pl.ds(H, H)
        diag = [
            rc(b + 0, acc.at[k, 3, lo], rd.at[k, 0], 2),
            rc(b + 1, acc.at[k, 3, hi], rd.at[k, 1], 4),
        ]
        if k == 1:
            return diag + [
                rc(b + 2, acc.at[k, 1, pl.ds(0, FILL_X)], fx_ref, 2),
                rc(b + 3, acc.at[k, 2, pl.ds(T - FILL_Y, FILL_Y)], fy_ref, 4),
            ]
        return diag + [
            rc(b + 2, acc.at[k, 1, lo], fr.at[0, lo], 2),
            rc(b + 3, acc.at[k, 2, hi], fr.at[1, hi], 4),
            rc(b + 4, acc.at[k, 1, hi], fr.at[0, hi], 2),
            rc(b + 5, acc.at[k, 2, lo], fr.at[1, lo], 4),
        ]

    e0 = lax.broadcasted_iota(jnp.int32, (16 * NE, T), 0)
    e1 = lax.broadcasted_iota(jnp.int32, (16 * NE, T), 1) // CAP
    rank_lane = lax.rem(lax.broadcasted_iota(jnp.int32, (T, T), 1), CAP).astype(F32)

    def spread(idx, rows, weighted):
        pick = jnp.where(e0 == e1 + idx * NE, 1.0, 0.0).astype(BF16)
        hit = dot(rt[...], pick) == rank_lane
        if weighted:
            for k in range(3):
                sb[k] = jnp.where(hit, dot(gt[k], pick), 0.0).astype(BF16)
            return dot(sb[0], rows) + dot(sb[1], rows) + dot(sb[2], rows)
        sb[0] = jnp.where(hit, 1.0, 0.0).astype(BF16)
        return dot(sb[0], rows)

    def combine_all(k, b, recv, copies, weighted):
        def one(i, carry):
            h = 3 - i
            acc[k, h] = spread(2 * h, os_[2 * h].reshape(T, D), weighted)
            swap_copy(b, recv, h).wait_recv()
            acc[k, h] = acc[k, h] + spread(8 + h, recv[h].reshape(T, D), weighted)

            @pl.when(i == 0)
            def _():
                copies[0].start()
                copies[1].start()

            @pl.when(i == 1)
            def _():
                copies[3].start()

            @pl.when(i == 2)
            def _():
                copies[2].start()
            return carry
        lax.fori_loop(0, 4, one, 0)

    ro = reduce_copies(RS_O, 0)
    for h in order:
        swap_copy(OX, orv, h).start()
    cy[2].wait_recv()
    cy[7].start()
    cy[4].wait_recv()
    cy[8].start()
    combine_all(0, OX, orv, ro, True)

    cy[5].wait_recv()
    cy[6].wait_recv()
    cy[9].start()
    cy[0].wait_recv()
    cy[7].wait_recv()
    cy[8].wait_recv()
    cy[9].wait_recv()
    for c in cx:
        c.wait_send()

    swap_gg = rc(GG, gj.at[1], gr, 1)
    gg_diag = rc(GG + 1, gacc.at[3], gd, 4)
    gg_y = rc(GG + 2, gacc.at[2], gf.at[1], 4)
    gg_x = rc(GG + 3, gacc.at[1], gf.at[0], 2)

    def gather_dy(d, carry):
        build_p(d)
        rows = dot(pb[...], dya[d])
        outs = os_[d].reshape(T, D).astype(F32)
        gg_rows = jnp.sum(rows * outs, axis=1, keepdims=True)
        r_d = rm[d]
        g_d = gm[d]
        r_ids = ra[d]
        gg_d = jnp.zeros((8, T), F32)
        for l in range(NE):
            hit = lane_r == r_d[l:l + 1, :]
            gcol = jnp.sum(jnp.where(hit, g_d[l:l + 1, :], 0.0), axis=1, keepdims=True)
            xa[d, l * CAP:(l + 1) * CAP, :] = (gcol * rows[l * CAP:(l + 1) * CAP, :]).astype(BF16)
            gg_l = jnp.sum(
                jnp.where(hit, gg_rows[l * CAP:(l + 1) * CAP, :], 0.0), axis=0, keepdims=True)
            gg_d = gg_d + jnp.where(r_ids == me * NE + l, gg_l, 0.0)
        gj[lax.rem(d, 2), d // 2] = gg_d
        return carry

    lax.fori_loop(0, 8, gather_dy, 0)
    swap_gg.start()
    for h in order:
        swap_copy(OX, orv, h).wait_send()

    swap_gg.wait_recv()
    gacc[...] = gj[0] + gr[...]
    gg_diag.start()
    gg_y.start()
    ro[0].wait_recv()
    acc[0, 2, :H] = acc[0, 2, :H] + rd[0, 0]
    ro[5].start()
    ro[1].wait_recv()
    acc[0, 1, H:] = acc[0, 1, H:] + rd[0, 1]
    ro[4].start()

    def expert_rows(buf, l):
        return buf[:, pl.ds(pl.multiple_of(l * CAP, CAP), CAP), :].reshape(T, D)

    def backward(l, carry):
        dh = dotg(expert_rows(xa, l), wd[l], NT).astype(BF16).astype(F32)
        uf = us[l].astype(F32)
        vf = vs[l].astype(F32)
        s = jax.nn.sigmoid(uf)
        sl = uf * s
        hs[l] = (sl * vf).astype(BF16)
        dv = (dh * sl).astype(BF16)
        du = (dh * vf * (s + sl * (1.0 - s))).astype(BF16)
        us[l] = du
        vs[l] = dv
        pr = (dotg(du, wg[l], NT) + dotg(dv, wu[l], NT)).astype(BF16)
        os_[:, pl.ds(l, 1)] = pr.reshape(8, 1, CAP, D)
        return carry

    out_xg = pltpu.make_async_copy(xg, xg_ref, lsem.at[5])
    out_c = pltpu.make_async_copy(xa, c_ref, lsem.at[6])
    out_xg.start()
    out_c.start()
    lax.fori_loop(0, NE, backward, 0)

    rp = reduce_copies(RS_P, 1)
    for h in order:
        swap_copy(PX, prv, h).start()
    gg_diag.wait_recv()
    gacc[1] = gacc[1] + gd[...]
    gg_x.start()
    combine_all(1, PX, prv, rp, False)

    lo, hi = pl.ds(0, H), pl.ds(H, H)
    early = [
        pltpu.make_async_copy(acc.at[1, 0], base_ref, lsem.at[8]),
        pltpu.make_async_copy(acc.at[1, 1, pl.ds(FILL_X, H - FILL_X)],
                              mx_ref.at[pl.ds(0, H - FILL_X)], lsem.at[9]),
        pltpu.make_async_copy(acc.at[1, 2, pl.ds(H, H - FILL_Y)],
                              my_ref.at[pl.ds(H, H - FILL_Y)], lsem.at[10]),
        pltpu.make_async_copy(us, du_ref, lsem.at[14]),
        pltpu.make_async_copy(vs, dv_ref, lsem.at[15]),
        pltpu.make_async_copy(hs, h_ref, lsem.at[16]),
    ]
    for c in early:
        c.start()
    for i in (2, 3, 4, 5):
        ro[i].wait_recv()
    moe_sc[...] = (acc[0, 0] + fr[0] + fr[1]).astype(BF16)
    out_moe = pltpu.make_async_copy(moe_sc, moe_ref, lsem.at[11])
    out_moe.start()
    for c in cr + cg + cy + ro + [swap_gg, gg_diag, gg_y]:
        c.wait_send()
    for h in order:
        swap_copy(PX, prv, h).wait_send()
    late_y = pltpu.make_async_copy(acc.at[1, 2, lo], my_ref.at[lo], lsem.at[12])
    late_x = pltpu.make_async_copy(acc.at[1, 1, hi], mx_ref.at[pl.ds(H - FILL_X, H)], lsem.at[13])
    rp[0].wait_recv()
    acc[1, 2, :H] = acc[1, 2, :H] + rd[1, 0]
    late_y.start()
    rp[1].wait_recv()
    acc[1, 1, H:] = acc[1, 1, H:] + rd[1, 1]
    late_x.start()
    gg_x.wait_recv()
    gg_y.wait_recv()
    gd[...] = gacc[0] + gf[0] + gf[1]
    out_gg = pltpu.make_async_copy(gd, gg_ref, lsem.at[7])
    out_gg.start()
    rp[2].wait_recv()
    rp[3].wait_recv()
    for c in rp + [gg_x]:
        c.wait_send()
    for c in early + [out_xg, out_c, out_moe, out_gg, late_y, late_x]:
        c.wait()


def publish(T, D, xg_ref, c_ref, du_ref, dv_ref, h_ref, moe_in, gg_in,
            dwg_ref, dwu_ref, dwd_ref, moe_ref, gg_ref):
    rows = xg_ref[...].reshape(T, D)
    dwg_ref[0] = dotg(rows, du_ref[0], TN)
    dwu_ref[0] = dotg(rows, dv_ref[0], TN)
    dwd_ref[0] = dotg(h_ref[0], c_ref[...].reshape(T, D), TN)

    @pl.when(pl.program_id(0) == 0)
    def _():
        moe_ref[...] = moe_in[...]
        gg_ref[...] = gg_in[...]


def solution(mesh):
    tok_spec = P(ALL_AXES, None)
    w_spec = P(EP_AXES, None, None)
    gw_spec = P(ALL_AXES, None, None)

    def local_step(tokens, route_idx, gate_vals, w_gate, w_up, w_down, grad_out):
        T, K = route_idx.shape
        D = tokens.shape[1]
        NE, _, FF = w_gate.shape
        CAP = T * K // (8 * NE)
        hbm = pl.BlockSpec(memory_space=pl.ANY)
        sds = jax.ShapeDtypeStruct
        outs = pl.pallas_call(
            functools.partial(kernel, T, D, FF, NE, CAP),
            out_shape=(sds((T, D), BF16), sds((K, T), F32),
                       sds((T, D), F32), sds((T - FILL_X, D), F32), sds((T - FILL_Y, D), F32),
                       sds((FILL_X, D), F32), sds((FILL_Y, D), F32),
                       sds((8, NE, CAP, D), BF16), sds((8, T, D), BF16),
                       sds((NE, T, FF), BF16), sds((NE, T, FF), BF16), sds((NE, T, FF), BF16)),
            in_specs=[hbm] * 7,
            out_specs=(hbm,) * 12,
            scratch_shapes=[
                pltpu.VMEM((8, T, D), BF16),
                pltpu.VMEM((8, T, D), BF16),
                pltpu.VMEM((8, NE, CAP, D), BF16),
                pltpu.VMEM((NE, T, FF), BF16),
                pltpu.VMEM((NE, T, FF), BF16),
                pltpu.VMEM((NE, T, FF), BF16),
                pltpu.VMEM((8, NE, CAP, D), BF16),
                pltpu.VMEM((NE, D, FF), BF16),
                pltpu.VMEM((NE, D, FF), BF16),
                pltpu.VMEM((NE, FF, D), BF16),
                pltpu.VMEM((2, 4, T, D), F32),
                pltpu.VMEM((2, 2, T // 2, D), F32),
                pltpu.VMEM((2, T, D), F32),
                pltpu.VMEM((4, NE, CAP, D), BF16),
                pltpu.VMEM((4, NE, CAP, D), BF16),
                pltpu.VMEM((T, T), BF16),
                pltpu.VMEM((3, T, T), BF16),
                pltpu.VMEM((8, K, T), jnp.int32),
                pltpu.VMEM((8, K, T), F32),
                pltpu.VMEM((16, NE, T), F32),
                pltpu.VMEM((16, NE, T), F32),
                pltpu.VMEM((16, NE, T), F32),
                pltpu.VMEM((T, 16 * NE), BF16),
                pltpu.VMEM((3, T, 16 * NE), BF16),
                pltpu.VMEM((2, 4, K, T), F32),
                pltpu.VMEM((4, K, T), F32),
                pltpu.VMEM((4, K, T), F32),
                pltpu.VMEM((K, T), F32),
                pltpu.VMEM((2, K, T), F32),
                pltpu.VMEM((T, D), BF16),
                pltpu.SemaphoreType.DMA((N_SEM,)),
                pltpu.SemaphoreType.DMA((N_SEM,)),
                pltpu.SemaphoreType.DMA((17,)),
            ],
            compiler_params=pltpu.CompilerParams(
                collective_id=0, has_side_effects=True, vmem_limit_bytes=67043328),
        )(tokens, grad_out, route_idx.T, gate_vals.T, w_gate, w_up, w_down)
        moe, gg, base, mx, my, fx, fy, xg, c, du, dv, h = outs
        rx = lax.ppermute(mx, 'col', [(0, 1), (1, 0)])
        ry = lax.ppermute(my, 'row', [(0, 1), (1, 0)])

        def per_expert(*shape):
            return pl.BlockSpec((1,) + shape, lambda l: (l, 0, 0))

        def whole(a):
            return pl.BlockSpec(a.shape, lambda l: (0, 0))

        dwg, dwu, dwd, moe, gg = pl.pallas_call(
            functools.partial(publish, T, D),
            grid=(NE,),
            out_shape=(sds((NE, D, FF), F32), sds((NE, D, FF), F32), sds((NE, FF, D), F32),
                       sds(moe.shape, BF16), sds(gg.shape, F32)),
            in_specs=[pl.BlockSpec((8, 1, CAP, D), lambda l: (0, l, 0, 0)),
                      pl.BlockSpec((8, CAP, D), lambda l: (0, l, 0)),
                      per_expert(T, FF), per_expert(T, FF), per_expert(T, FF), whole(moe), whole(gg)],
            out_specs=(per_expert(D, FF), per_expert(D, FF), per_expert(FF, D), whole(moe), whole(gg)),
            cost_estimate=pl.CostEstimate(
                flops=6 * NE * T * D * FF, bytes_accessed=36 * 1024 * 1024, transcendentals=0),
            compiler_params=pltpu.CompilerParams(vmem_limit_bytes=60 * 1024 * 1024),
        )(xg, c, du, dv, h, moe, gg)
        gx = (base + jnp.concatenate([fx, rx]) + jnp.concatenate([ry, fy])).astype(BF16)
        return moe, gx, gg.T, dwg, dwu, dwd

    return jax.shard_map(
        local_step, mesh=mesh,
        in_specs=(tok_spec, tok_spec, tok_spec, w_spec, w_spec, w_spec, tok_spec),
        out_specs=(tok_spec, tok_spec, tok_spec, gw_spec, gw_spec, gw_spec),
        check_vma=False)
```

```python
import functools

import jax
import jax.numpy as jnp
from jax import lax
from jax.experimental import pallas as pl
from jax.experimental.pallas import tpu as pltpu
from jax.sharding import PartitionSpec as P


EP_AXES = ('row', 'col', 'core')
ALL_AXES = ('part', 'row', 'col', 'core')
MESH = pl.DeviceIdType.MESH
F32 = jnp.float32
BF16 = jnp.bfloat16
NT = (((1,), (1,)), ((), ()))
TN = (((0,), (0,)), ((), ()))

AG_X, AG_DY, RG, OX, PX, RS_O, RS_P, GG, N_SEM = 0, 10, 20, 34, 38, 42, 48, 52, 56


FILL_X, FILL_Y = 104, 96


def dot(a, b):
    return jnp.dot(a, b, preferred_element_type=F32)


def dotg(a, b, dims):
    return lax.dot_general(a, b, dims, preferred_element_type=F32)


def kernel(T, D, FF, NE, CAP,
           x_ref, dy_ref, route_ref, gate_ref, wg_ref, wu_ref, wd_ref,
           moe_ref, gg_ref, base_ref, mx_ref, my_ref, fx_ref, fy_ref, xg_ref, c_ref, du_ref, dv_ref, h_ref,
           xa, dya, xg, us, vs, hs, os_, wg, wu, wd, acc, rd, fr, orv, prv,
           pb, sb, r0, ra, ga, rm, gm, mb, rt, gt, gj, gr, gacc, gd, gf, moe_sc,
           ssem, rsem, lsem):
    H = T // 2
    row, col, core = lax.axis_index('row'), lax.axis_index('col'), lax.axis_index('core')
    me = row * 4 + col * 2 + core
    partner = row * 4 + col * 2 + (1 - core)

    def dev(rel):
        return {
            'row': 1 - row if rel & 4 else row,
            'col': 1 - col if rel & 2 else col,
            'core': 1 - core if rel & 1 else core,
        }

    def rc(i, src, dst, rel):
        return pltpu.make_async_remote_copy(
            src_ref=src, dst_ref=dst, send_sem=ssem.at[i], recv_sem=rsem.at[i],
            device_id=dev(rel), device_id_type=MESH)

    def gather_copies(b, buf):
        lo, hi = pl.ds(0, H), pl.ds(H, H)
        return [
            rc(b + 0, buf.at[0], buf.at[1], 1),
            rc(b + 1, buf.at[0, hi], buf.at[2, hi], 2),
            rc(b + 2, buf.at[0, lo], buf.at[2, lo], 2),
            rc(b + 3, buf.at[0, lo], buf.at[4, lo], 4),
            rc(b + 4, buf.at[0, hi], buf.at[4, hi], 4),
            rc(b + 5, buf.at[2, hi], buf.at[6, hi], 4),
            rc(b + 6, buf.at[4, lo], buf.at[6, lo], 2),
            rc(b + 7, buf.at[2], buf.at[3], 1),
            rc(b + 8, buf.at[4], buf.at[5], 1),
            rc(b + 9, buf.at[6], buf.at[7], 1),
        ]

    lx = pltpu.make_async_copy(x_ref, xa.at[0], lsem.at[0])
    ldy = pltpu.make_async_copy(dy_ref, dya.at[0], lsem.at[1])
    lwg = pltpu.make_async_copy(wg_ref, wg, lsem.at[2])
    lwu = pltpu.make_async_copy(wu_ref, wu, lsem.at[3])
    lwd = pltpu.make_async_copy(wd_ref, wd, lsem.at[4])
    lr = pltpu.make_async_copy(route_ref, r0, lsem.at[14])
    lg = pltpu.make_async_copy(gate_ref, ga.at[0], lsem.at[15])
    lx.start()
    lr.start()
    lg.start()
    ldy.start()
    lwg.start()
    lwu.start()
    lwd.start()

    barrier = pltpu.get_barrier_semaphore()
    for rel in (1, 2, 4):
        pl.semaphore_signal(barrier, inc=1, device_id=dev(rel), device_id_type=MESH)
    pl.semaphore_wait(barrier, 3)

    def small_copies(b, src, buf, diag):
        return [
            rc(b + 0, src, buf.at[1], 1),
            rc(b + 1, src, buf.at[2], 2),
            rc(b + 2, src, buf.at[4], 4),
            rc(b + 3, buf.at[6 - diag], buf.at[6], diag),
            rc(b + 4, buf.at[2], buf.at[3], 1),
            rc(b + 5, buf.at[4], buf.at[5], 1),
            rc(b + 6, buf.at[6], buf.at[7], 1),
        ]

    cr = small_copies(RG, ra.at[0], ra, 2)
    cg = small_copies(RG + 7, ga.at[0], ga, 4)
    cx = gather_copies(AG_X, xa)
    cy = gather_copies(AG_DY, dya)
    lr.wait()
    ra[0] = r0[...].astype(F32).astype(BF16)
    lg.wait()
    for i in (1, 2, 0):
        cg[i].start()
    lx.wait()
    for i in (1, 2, 0):
        cr[i].start()
    for i in (1, 3, 0):
        cx[i].start()
    cr[2].wait_recv()
    cr[3].start()
    cg[1].wait_recv()
    cg[3].start()
    cx[2].start()
    cx[4].start()
    cr[5].start()
    cg[4].start()
    cr[1].wait_recv()
    cr[4].start()
    cg[2].wait_recv()
    cg[5].start()

    i0 = lax.broadcasted_iota(jnp.int32, (T, T), 0)
    i1 = lax.broadcasted_iota(jnp.int32, (T, T), 1)
    sb[0] = (i0 < i1).astype(F32).astype(BF16)
    sb[1] = (i0 > i1).astype(F32).astype(BF16)
    sb[2] = (i0 == i1).astype(F32).astype(BF16)
    cx[1].wait_recv()
    cx[5].start()
    cx[3].wait_recv()
    cx[6].start()
    cr[3].wait_recv()
    cr[6].start()
    cg[3].wait_recv()
    cg[6].start()
    for i in (0, 4, 5, 6):
        cr[i].wait_recv()
        cg[i].wait_recv()
    mb[...] = jnp.zeros_like(mb)
    gm[...] = jnp.zeros_like(gm)
    sub = lax.broadcasted_iota(jnp.int32, (NE, T), 0)
    for idx in range(12):
        src = idx if idx < 8 else 2 * (idx - 8)
        owner = me if idx < 8 else partner
        ids = (sub + owner * NE).astype(F32)
        routes = ra[src].astype(F32)
        hits = jnp.zeros((NE, T), F32)
        gates = jnp.zeros((NE, T), F32)
        for j in range(8):
            hit = routes[j:j + 1, :] == ids
            hits = hits + jnp.where(hit, 1.0, 0.0)
            gates = gates + jnp.where(hit, ga[src, j:j + 1, :], 0.0)
        mb[idx] = hits
        gm[idx] = gates
    m_all = mb[...].reshape(16 * NE, T)
    m_bf = m_all.astype(BF16)
    ranks = dot(m_bf, sb[0])
    rm[...] = jnp.where(m_all > 0.5, ranks, -1.0).reshape(16, NE, T)
    m_t = dotg(sb[2], m_bf, NT)
    r_t = dotg(sb[1], m_bf, NT)
    rt[...] = jnp.where(m_t > 0.5, r_t, -1.0).astype(BF16)
    g_all = gm[...].reshape(16 * NE, T)
    g_hi = g_all.astype(BF16)
    rest = g_all - g_hi.astype(F32)
    g_mid = rest.astype(BF16)
    g_lo = (rest - g_mid.astype(F32)).astype(BF16)
    for k, piece in enumerate((g_hi, g_mid, g_lo)):
        gt[k] = dotg(sb[2], piece, NT).astype(BF16)

    lane_r = lax.broadcasted_iota(jnp.int32, (CAP, T), 0).astype(F32)

    def build_p(d):
        r_d = rm[d]
        for l in range(NE):
            pb[l * CAP:(l + 1) * CAP, :] = jnp.where(lane_r == r_d[l:l + 1, :], 1.0, 0.0).astype(BF16)

    def gather_x(d):
        build_p(d)
        xg[d] = dot(pb[...], xa[d]).astype(BF16).reshape(NE, CAP, D)

    def gather_x_loop(first, step, count):
        def one(i, carry):
            gather_x(first + step * i)
            return carry
        lax.fori_loop(0, count, one, 0)

    cx[0].wait_recv()
    gather_x_loop(0, 1, 2)
    cx[2].wait_recv()
    cx[7].start()
    cx[4].wait_recv()
    cx[8].start()
    ldy.wait()
    for i in (1, 3, 0, 2, 4):
        cy[i].start()
    gather_x_loop(2, 2, 2)
    cx[7].wait_recv()
    cx[8].wait_recv()
    gather_x_loop(3, 2, 2)
    cx[5].wait_recv()
    cx[6].wait_recv()
    cx[9].start()
    gather_x_loop(6, 1, 1)
    cx[9].wait_recv()
    gather_x_loop(7, 1, 1)

    lwg.wait()
    lwu.wait()
    lwd.wait()

    def forward(l, carry):
        rows = xg[:, pl.ds(l, 1)].reshape(T, D)
        u = dot(rows, wg[l]).astype(BF16)
        v = dot(rows, wu[l]).astype(BF16)
        us[l] = u
        vs[l] = v
        uf = u.astype(F32)
        h = (uf * jax.nn.sigmoid(uf) * v.astype(F32)).astype(BF16)
        o = dot(h, wd[l]).astype(BF16)
        os_[:, pl.ds(l, 1)] = o.reshape(8, 1, CAP, D)
        return carry

    lax.fori_loop(0, NE // 2, forward, 0)
    cy[1].wait_recv()
    cy[5].start()
    cy[3].wait_recv()
    cy[6].start()
    lax.fori_loop(NE // 2, NE, forward, 0)

    order = (3, 1, 2, 0)

    def swap_copy(b, buf, h):
        return rc(b + h, os_.at[2 * h + 1], buf.at[h], 1)

    def reduce_copies(b, k):
        lo, hi = pl.ds(0, H), pl.ds(H, H)
        diag = [
            rc(b + 0, acc.at[k, 3, lo], rd.at[k, 0], 2),
            rc(b + 1, acc.at[k, 3, hi], rd.at[k, 1], 4),
        ]
        if k == 1:
            return diag + [
                rc(b + 2, acc.at[k, 1, pl.ds(0, FILL_X)], fx_ref, 2),
                rc(b + 3, acc.at[k, 2, pl.ds(T - FILL_Y, FILL_Y)], fy_ref, 4),
            ]
        return diag + [
            rc(b + 2, acc.at[k, 1, lo], fr.at[0, lo], 2),
            rc(b + 3, acc.at[k, 2, hi], fr.at[1, hi], 4),
            rc(b + 4, acc.at[k, 1, hi], fr.at[0, hi], 2),
            rc(b + 5, acc.at[k, 2, lo], fr.at[1, lo], 4),
        ]

    e0 = lax.broadcasted_iota(jnp.int32, (16 * NE, T), 0)
    e1 = lax.broadcasted_iota(jnp.int32, (16 * NE, T), 1) // CAP
    rank_lane = lax.rem(lax.broadcasted_iota(jnp.int32, (T, T), 1), CAP).astype(F32)

    def spread(idx, rows, weighted):
        pick = jnp.where(e0 == e1 + idx * NE, 1.0, 0.0).astype(BF16)
        hit = dot(rt[...], pick) == rank_lane
        if weighted:
            for k in range(3):
                sb[k] = jnp.where(hit, dot(gt[k], pick), 0.0).astype(BF16)
            return dot(sb[0], rows) + dot(sb[1], rows) + dot(sb[2], rows)
        sb[0] = jnp.where(hit, 1.0, 0.0).astype(BF16)
        return dot(sb[0], rows)

    def combine_all(k, b, recv, copies, weighted):
        def one(i, carry):
            h = 3 - i
            acc[k, h] = spread(2 * h, os_[2 * h].reshape(T, D), weighted)
            swap_copy(b, recv, h).wait_recv()
            acc[k, h] = acc[k, h] + spread(8 + h, recv[h].reshape(T, D), weighted)

            @pl.when(i == 0)
            def _():
                copies[0].start()
                copies[1].start()

            @pl.when(i == 1)
            def _():
                copies[3].start()

            @pl.when(i == 2)
            def _():
                copies[2].start()
            return carry
        lax.fori_loop(0, 4, one, 0)

    ro = reduce_copies(RS_O, 0)
    for h in order:
        swap_copy(OX, orv, h).start()
    cy[2].wait_recv()
    cy[7].start()
    cy[4].wait_recv()
    cy[8].start()
    combine_all(0, OX, orv, ro, True)

    cy[5].wait_recv()
    cy[6].wait_recv()
    cy[9].start()
    cy[0].wait_recv()
    cy[7].wait_recv()
    cy[8].wait_recv()
    cy[9].wait_recv()
    for c in cx:
        c.wait_send()

    swap_gg = rc(GG, gj.at[1], gr, 1)
    gg_diag = rc(GG + 1, gacc.at[3], gd, 4)
    gg_y = rc(GG + 2, gacc.at[2], gf.at[1], 4)
    gg_x = rc(GG + 3, gacc.at[1], gf.at[0], 2)

    def gather_dy(d, carry):
        build_p(d)
        rows = dot(pb[...], dya[d])
        outs = os_[d].reshape(T, D).astype(F32)
        gg_rows = jnp.sum(rows * outs, axis=1, keepdims=True)
        r_d = rm[d]
        g_d = gm[d]
        r_ids = ra[d].astype(F32)
        gg_d = jnp.zeros((8, T), F32)
        for l in range(NE):
            hit = lane_r == r_d[l:l + 1, :]
            gcol = jnp.sum(jnp.where(hit, g_d[l:l + 1, :], 0.0), axis=1, keepdims=True)
            xa[d, l * CAP:(l + 1) * CAP, :] = (gcol * rows[l * CAP:(l + 1) * CAP, :]).astype(BF16)
            gg_l = jnp.sum(
                jnp.where(hit, gg_rows[l * CAP:(l + 1) * CAP, :], 0.0), axis=0, keepdims=True)
            gg_d = gg_d + jnp.where(r_ids == (me * NE + l).astype(F32), gg_l, 0.0)
        gj[lax.rem(d, 2), d // 2] = gg_d
        return carry

    lax.fori_loop(0, 8, gather_dy, 0)
    swap_gg.start()
    for h in order:
        swap_copy(OX, orv, h).wait_send()

    swap_gg.wait_recv()
    gacc[...] = gj[0] + gr[...]
    gg_diag.start()
    gg_y.start()
    ro[0].wait_recv()
    acc[0, 2, :H] = acc[0, 2, :H] + rd[0, 0]
    ro[5].start()
    ro[1].wait_recv()
    acc[0, 1, H:] = acc[0, 1, H:] + rd[0, 1]
    ro[4].start()

    def expert_rows(buf, l):
        return buf[:, pl.ds(pl.multiple_of(l * CAP, CAP), CAP), :].reshape(T, D)

    def backward(l, carry):
        dh = dotg(expert_rows(xa, l), wd[l], NT).astype(BF16).astype(F32)
        uf = us[l].astype(F32)
        vf = vs[l].astype(F32)
        s = jax.nn.sigmoid(uf)
        sl = uf * s
        hs[l] = (sl * vf).astype(BF16)
        dv = (dh * sl).astype(BF16)
        du = (dh * vf * (s + sl * (1.0 - s))).astype(BF16)
        us[l] = du
        vs[l] = dv
        pr = (dotg(du, wg[l], NT) + dotg(dv, wu[l], NT)).astype(BF16)
        os_[:, pl.ds(l, 1)] = pr.reshape(8, 1, CAP, D)
        return carry

    out_xg = pltpu.make_async_copy(xg, xg_ref, lsem.at[5])
    out_c = pltpu.make_async_copy(xa, c_ref, lsem.at[6])
    out_xg.start()
    out_c.start()
    lax.fori_loop(0, NE, backward, 0)

    rp = reduce_copies(RS_P, 1)
    for h in order:
        swap_copy(PX, prv, h).start()
    gg_diag.wait_recv()
    gacc[1] = gacc[1] + gd[...]
    gg_x.start()
    combine_all(1, PX, prv, rp, False)

    lo, hi = pl.ds(0, H), pl.ds(H, H)
    early = [
        pltpu.make_async_copy(acc.at[1, 0], base_ref, lsem.at[8]),
        pltpu.make_async_copy(acc.at[1, 1, pl.ds(FILL_X, H - FILL_X)],
                              mx_ref.at[pl.ds(0, H - FILL_X)], lsem.at[9]),
        pltpu.make_async_copy(acc.at[1, 2, pl.ds(H, H - FILL_Y)],
                              my_ref.at[pl.ds(H, H - FILL_Y)], lsem.at[10]),
        pltpu.make_async_copy(us, du_ref, lsem.at[14]),
        pltpu.make_async_copy(vs, dv_ref, lsem.at[15]),
        pltpu.make_async_copy(hs, h_ref, lsem.at[16]),
    ]
    for c in early:
        c.start()
    for i in (2, 3, 4, 5):
        ro[i].wait_recv()
    moe_sc[...] = (acc[0, 0] + fr[0] + fr[1]).astype(BF16)
    out_moe = pltpu.make_async_copy(moe_sc, moe_ref, lsem.at[11])
    out_moe.start()
    for c in cr + cg + cy + ro + [swap_gg, gg_diag, gg_y]:
        c.wait_send()
    for h in order:
        swap_copy(PX, prv, h).wait_send()
    late_y = pltpu.make_async_copy(acc.at[1, 2, lo], my_ref.at[lo], lsem.at[12])
    late_x = pltpu.make_async_copy(acc.at[1, 1, hi], mx_ref.at[pl.ds(H - FILL_X, H)], lsem.at[13])
    rp[0].wait_recv()
    acc[1, 2, :H] = acc[1, 2, :H] + rd[1, 0]
    late_y.start()
    rp[1].wait_recv()
    acc[1, 1, H:] = acc[1, 1, H:] + rd[1, 1]
    late_x.start()
    gg_x.wait_recv()
    gg_y.wait_recv()
    gd[...] = gacc[0] + gf[0] + gf[1]
    out_gg = pltpu.make_async_copy(gd, gg_ref, lsem.at[7])
    out_gg.start()
    rp[2].wait_recv()
    rp[3].wait_recv()
    for c in rp + [gg_x]:
        c.wait_send()
    for c in early + [out_xg, out_c, out_moe, out_gg, late_y, late_x]:
        c.wait()


def publish(T, D, xg_ref, c_ref, du_ref, dv_ref, h_ref, moe_in, gg_in,
            dwg_ref, dwu_ref, dwd_ref, moe_ref, gg_ref):
    rows = xg_ref[...].reshape(T, D)
    dwg_ref[0] = dotg(rows, du_ref[0], TN)
    dwu_ref[0] = dotg(rows, dv_ref[0], TN)
    dwd_ref[0] = dotg(h_ref[0], c_ref[...].reshape(T, D), TN)

    @pl.when(pl.program_id(0) == 0)
    def _():
        moe_ref[...] = moe_in[...]
        gg_ref[...] = gg_in[...]


def solution(mesh):
    tok_spec = P(ALL_AXES, None)
    w_spec = P(EP_AXES, None, None)
    gw_spec = P(ALL_AXES, None, None)

    def local_step(tokens, route_idx, gate_vals, w_gate, w_up, w_down, grad_out):
        T, K = route_idx.shape
        D = tokens.shape[1]
        NE, _, FF = w_gate.shape
        CAP = T * K // (8 * NE)
        hbm = pl.BlockSpec(memory_space=pl.ANY)
        sds = jax.ShapeDtypeStruct
        outs = pl.pallas_call(
            functools.partial(kernel, T, D, FF, NE, CAP),
            out_shape=(sds((T, D), BF16), sds((K, T), F32),
                       sds((T, D), F32), sds((T - FILL_X, D), F32), sds((T - FILL_Y, D), F32),
                       sds((FILL_X, D), F32), sds((FILL_Y, D), F32),
                       sds((8, NE, CAP, D), BF16), sds((8, T, D), BF16),
                       sds((NE, T, FF), BF16), sds((NE, T, FF), BF16), sds((NE, T, FF), BF16)),
            in_specs=[hbm] * 7,
            out_specs=(hbm,) * 12,
            scratch_shapes=[
                pltpu.VMEM((8, T, D), BF16),
                pltpu.VMEM((8, T, D), BF16),
                pltpu.VMEM((8, NE, CAP, D), BF16),
                pltpu.VMEM((NE, T, FF), BF16),
                pltpu.VMEM((NE, T, FF), BF16),
                pltpu.VMEM((NE, T, FF), BF16),
                pltpu.VMEM((8, NE, CAP, D), BF16),
                pltpu.VMEM((NE, D, FF), BF16),
                pltpu.VMEM((NE, D, FF), BF16),
                pltpu.VMEM((NE, FF, D), BF16),
                pltpu.VMEM((2, 4, T, D), F32),
                pltpu.VMEM((2, 2, T // 2, D), F32),
                pltpu.VMEM((2, T, D), F32),
                pltpu.VMEM((4, NE, CAP, D), BF16),
                pltpu.VMEM((4, NE, CAP, D), BF16),
                pltpu.VMEM((T, T), BF16),
                pltpu.VMEM((3, T, T), BF16),
                pltpu.VMEM((K, T), jnp.int32),
                pltpu.VMEM((8, K, T), BF16),
                pltpu.VMEM((8, K, T), F32),
                pltpu.VMEM((16, NE, T), F32),
                pltpu.VMEM((16, NE, T), F32),
                pltpu.VMEM((16, NE, T), F32),
                pltpu.VMEM((T, 16 * NE), BF16),
                pltpu.VMEM((3, T, 16 * NE), BF16),
                pltpu.VMEM((2, 4, K, T), F32),
                pltpu.VMEM((4, K, T), F32),
                pltpu.VMEM((4, K, T), F32),
                pltpu.VMEM((K, T), F32),
                pltpu.VMEM((2, K, T), F32),
                pltpu.VMEM((T, D), BF16),
                pltpu.SemaphoreType.DMA((N_SEM,)),
                pltpu.SemaphoreType.DMA((N_SEM,)),
                pltpu.SemaphoreType.DMA((17,)),
            ],
            compiler_params=pltpu.CompilerParams(
                collective_id=0, has_side_effects=True, vmem_limit_bytes=67043328),
        )(tokens, grad_out, route_idx.T, gate_vals.T, w_gate, w_up, w_down)
        moe, gg, base, mx, my, fx, fy, xg, c, du, dv, h = outs
        rx = lax.ppermute(mx, 'col', [(0, 1), (1, 0)])
        ry = lax.ppermute(my, 'row', [(0, 1), (1, 0)])

        def per_expert(*shape):
            return pl.BlockSpec((1,) + shape, lambda l: (l, 0, 0))

        def whole(a):
            return pl.BlockSpec(a.shape, lambda l: (0, 0))

        dwg, dwu, dwd, moe, gg = pl.pallas_call(
            functools.partial(publish, T, D),
            grid=(NE,),
            out_shape=(sds((NE, D, FF), F32), sds((NE, D, FF), F32), sds((NE, FF, D), F32),
                       sds(moe.shape, BF16), sds(gg.shape, F32)),
            in_specs=[pl.BlockSpec((8, 1, CAP, D), lambda l: (0, l, 0, 0)),
                      pl.BlockSpec((8, CAP, D), lambda l: (0, l, 0)),
                      per_expert(T, FF), per_expert(T, FF), per_expert(T, FF), whole(moe), whole(gg)],
            out_specs=(per_expert(D, FF), per_expert(D, FF), per_expert(FF, D), whole(moe), whole(gg)),
            cost_estimate=pl.CostEstimate(
                flops=6 * NE * T * D * FF, bytes_accessed=36 * 1024 * 1024, transcendentals=0),
            compiler_params=pltpu.CompilerParams(vmem_limit_bytes=60 * 1024 * 1024),
        )(xg, c, du, dv, h, moe, gg)
        gx = (base + jnp.concatenate([fx, rx]) + jnp.concatenate([ry, fy])).astype(BF16)
        return moe, gx, gg.T, dwg, dwu, dwd

    return jax.shard_map(
        local_step, mesh=mesh,
        in_specs=(tok_spec, tok_spec, tok_spec, w_spec, w_spec, w_spec, tok_spec),
        out_specs=(tok_spec, tok_spec, tok_spec, gw_spec, gw_spec, gw_spec),
        check_vma=False)
```

```python
import functools

import jax
import jax.numpy as jnp
from jax import lax
from jax.experimental import pallas as pl
from jax.experimental.pallas import tpu as pltpu
from jax.sharding import PartitionSpec as P


EP_AXES = ('row', 'col', 'core')
ALL_AXES = ('part', 'row', 'col', 'core')
MESH = pl.DeviceIdType.MESH
F32 = jnp.float32
BF16 = jnp.bfloat16
NT = (((1,), (1,)), ((), ()))
TN = (((0,), (0,)), ((), ()))

AG_X, AG_DY, RG, OX, PX, RS_O, RS_P, GG, N_SEM = 0, 10, 20, 34, 38, 42, 48, 52, 56


FILL_X, FILL_Y = 104, 88


def dot(a, b):
    return jnp.dot(a, b, preferred_element_type=F32)


def dotg(a, b, dims):
    return lax.dot_general(a, b, dims, preferred_element_type=F32)


def kernel(T, D, FF, NE, CAP,
           x_ref, dy_ref, route_ref, gate_ref, wg_ref, wu_ref, wd_ref,
           moe_ref, gg_ref, base_ref, mx_ref, my_ref, fx_ref, fy_ref, xg_ref, c_ref, du_ref, dv_ref, h_ref,
           xa, dya, xg, us, vs, hs, os_, wg, wu, wd, acc, rd, fr, orv, prv,
           pb, sb, r0, ra, ga, rm, gm, mb, rt, gt, gj, gr, gacc, gd, gf, moe_sc,
           ssem, rsem, lsem):
    H = T // 2
    row, col, core = lax.axis_index('row'), lax.axis_index('col'), lax.axis_index('core')
    me = row * 4 + col * 2 + core
    partner = row * 4 + col * 2 + (1 - core)

    def dev(rel):
        return {
            'row': 1 - row if rel & 4 else row,
            'col': 1 - col if rel & 2 else col,
            'core': 1 - core if rel & 1 else core,
        }

    def rc(i, src, dst, rel):
        return pltpu.make_async_remote_copy(
            src_ref=src, dst_ref=dst, send_sem=ssem.at[i], recv_sem=rsem.at[i],
            device_id=dev(rel), device_id_type=MESH)

    def gather_copies(b, buf):
        lo, hi = pl.ds(0, H), pl.ds(H, H)
        return [
            rc(b + 0, buf.at[0], buf.at[1], 1),
            rc(b + 1, buf.at[0, hi], buf.at[2, hi], 2),
            rc(b + 2, buf.at[0, lo], buf.at[2, lo], 2),
            rc(b + 3, buf.at[0, lo], buf.at[4, lo], 4),
            rc(b + 4, buf.at[0, hi], buf.at[4, hi], 4),
            rc(b + 5, buf.at[2, hi], buf.at[6, hi], 4),
            rc(b + 6, buf.at[4, lo], buf.at[6, lo], 2),
            rc(b + 7, buf.at[2], buf.at[3], 1),
            rc(b + 8, buf.at[4], buf.at[5], 1),
            rc(b + 9, buf.at[6], buf.at[7], 1),
        ]

    lx = pltpu.make_async_copy(x_ref, xa.at[0], lsem.at[0])
    ldy = pltpu.make_async_copy(dy_ref, dya.at[0], lsem.at[1])
    lwg = pltpu.make_async_copy(wg_ref, wg, lsem.at[2])
    lwu = pltpu.make_async_copy(wu_ref, wu, lsem.at[3])
    lwd = pltpu.make_async_copy(wd_ref, wd, lsem.at[4])
    lr = pltpu.make_async_copy(route_ref, r0, lsem.at[14])
    lg = pltpu.make_async_copy(gate_ref, ga.at[0], lsem.at[15])
    lx.start()
    lr.start()
    lg.start()
    ldy.start()
    lwg.start()
    lwu.start()
    lwd.start()

    barrier = pltpu.get_barrier_semaphore()
    for rel in (1, 2, 4):
        pl.semaphore_signal(barrier, inc=1, device_id=dev(rel), device_id_type=MESH)
    pl.semaphore_wait(barrier, 3)

    def small_copies(b, src, buf, diag):
        return [
            rc(b + 0, src, buf.at[1], 1),
            rc(b + 1, src, buf.at[2], 2),
            rc(b + 2, src, buf.at[4], 4),
            rc(b + 3, buf.at[6 - diag], buf.at[6], diag),
            rc(b + 4, buf.at[2], buf.at[3], 1),
            rc(b + 5, buf.at[4], buf.at[5], 1),
            rc(b + 6, buf.at[6], buf.at[7], 1),
        ]

    cr = small_copies(RG, ra.at[0], ra, 2)
    cg = small_copies(RG + 7, ga.at[0], ga, 4)
    cx = gather_copies(AG_X, xa)
    cy = gather_copies(AG_DY, dya)
    lr.wait()
    ra[0] = r0[...].astype(F32).astype(BF16)
    lg.wait()
    for i in (1, 2, 0):
        cg[i].start()
    lx.wait()
    for i in (1, 2, 0):
        cr[i].start()
    for i in (1, 3, 0):
        cx[i].start()
    cr[2].wait_recv()
    cr[3].start()
    cg[1].wait_recv()
    cg[3].start()
    cx[2].start()
    cx[4].start()
    cr[5].start()
    cg[4].start()
    cr[1].wait_recv()
    cr[4].start()
    cg[2].wait_recv()
    cg[5].start()

    i0 = lax.broadcasted_iota(jnp.int32, (T, T), 0)
    i1 = lax.broadcasted_iota(jnp.int32, (T, T), 1)
    sb[0] = (i0 < i1).astype(F32).astype(BF16)
    sb[1] = (i0 > i1).astype(F32).astype(BF16)
    sb[2] = (i0 == i1).astype(F32).astype(BF16)
    cx[1].wait_recv()
    cx[5].start()
    cx[3].wait_recv()
    cx[6].start()
    cr[3].wait_recv()
    cr[6].start()
    cg[3].wait_recv()
    cg[6].start()
    for i in (0, 4, 5, 6):
        cr[i].wait_recv()
        cg[i].wait_recv()
    mb[...] = jnp.zeros_like(mb)
    gm[...] = jnp.zeros_like(gm)
    sub = lax.broadcasted_iota(jnp.int32, (NE, T), 0)
    for idx in range(12):
        src = idx if idx < 8 else 2 * (idx - 8)
        owner = me if idx < 8 else partner
        ids = (sub + owner * NE).astype(F32)
        routes = ra[src].astype(F32)
        hits = jnp.zeros((NE, T), F32)
        gates = jnp.zeros((NE, T), F32)
        for j in range(8):
            hit = routes[j:j + 1, :] == ids
            hits = hits + jnp.where(hit, 1.0, 0.0)
            gates = gates + jnp.where(hit, ga[src, j:j + 1, :], 0.0)
        mb[idx] = hits
        gm[idx] = gates
    m_all = mb[...].reshape(16 * NE, T)
    m_bf = m_all.astype(BF16)
    ranks = dot(m_bf, sb[0])
    rm[...] = jnp.where(m_all > 0.5, ranks, -1.0).reshape(16, NE, T)
    m_t = dotg(sb[2], m_bf, NT)
    r_t = dotg(sb[1], m_bf, NT)
    rt[...] = jnp.where(m_t > 0.5, r_t, -1.0).astype(BF16)
    g_all = gm[...].reshape(16 * NE, T)
    g_hi = g_all.astype(BF16)
    rest = g_all - g_hi.astype(F32)
    g_mid = rest.astype(BF16)
    g_lo = (rest - g_mid.astype(F32)).astype(BF16)
    for k, piece in enumerate((g_hi, g_mid, g_lo)):
        gt[k] = dotg(sb[2], piece, NT).astype(BF16)

    lane_r = lax.broadcasted_iota(jnp.int32, (CAP, T), 0).astype(F32)

    def build_p(d):
        r_d = rm[d]
        for l in range(NE):
            pb[l * CAP:(l + 1) * CAP, :] = jnp.where(lane_r == r_d[l:l + 1, :], 1.0, 0.0).astype(BF16)

    def gather_x(d):
        build_p(d)
        xg[d] = dot(pb[...], xa[d]).astype(BF16).reshape(NE, CAP, D)

    def gather_x_loop(first, step, count):
        def one(i, carry):
            gather_x(first + step * i)
            return carry
        lax.fori_loop(0, count, one, 0)

    cx[0].wait_recv()
    gather_x_loop(0, 1, 2)
    cx[2].wait_recv()
    cx[7].start()
    cx[4].wait_recv()
    cx[8].start()
    ldy.wait()
    for i in (1, 3, 0, 2, 4):
        cy[i].start()
    gather_x_loop(2, 2, 2)
    cx[7].wait_recv()
    cx[8].wait_recv()
    gather_x_loop(3, 2, 2)
    cx[5].wait_recv()
    cx[6].wait_recv()
    cx[9].start()
    gather_x_loop(6, 1, 1)
    cx[9].wait_recv()
    gather_x_loop(7, 1, 1)

    lwg.wait()
    lwu.wait()
    lwd.wait()

    def forward(l, carry):
        rows = xg[:, pl.ds(l, 1)].reshape(T, D)
        u = dot(rows, wg[l]).astype(BF16)
        v = dot(rows, wu[l]).astype(BF16)
        us[l] = u
        vs[l] = v
        uf = u.astype(F32)
        h = (uf * jax.nn.sigmoid(uf) * v.astype(F32)).astype(BF16)
        o = dot(h, wd[l]).astype(BF16)
        os_[:, pl.ds(l, 1)] = o.reshape(8, 1, CAP, D)
        return carry

    lax.fori_loop(0, NE // 2, forward, 0)
    cy[1].wait_recv()
    cy[5].start()
    cy[3].wait_recv()
    cy[6].start()
    lax.fori_loop(NE // 2, NE, forward, 0)

    order = (3, 1, 2, 0)

    def swap_copy(b, buf, h):
        return rc(b + h, os_.at[2 * h + 1], buf.at[h], 1)

    def reduce_copies(b, k):
        lo, hi = pl.ds(0, H), pl.ds(H, H)
        diag = [
            rc(b + 0, acc.at[k, 3, lo], rd.at[k, 0], 2),
            rc(b + 1, acc.at[k, 3, hi], rd.at[k, 1], 4),
        ]
        if k == 1:
            return diag + [
                rc(b + 2, acc.at[k, 1, pl.ds(0, FILL_X)], fx_ref, 2),
                rc(b + 3, acc.at[k, 2, pl.ds(T - FILL_Y, FILL_Y)], fy_ref, 4),
            ]
        return diag + [
            rc(b + 2, acc.at[k, 1, lo], fr.at[0, lo], 2),
            rc(b + 3, acc.at[k, 2, hi], fr.at[1, hi], 4),
            rc(b + 4, acc.at[k, 1, hi], fr.at[0, hi], 2),
            rc(b + 5, acc.at[k, 2, lo], fr.at[1, lo], 4),
        ]

    e0 = lax.broadcasted_iota(jnp.int32, (16 * NE, T), 0)
    e1 = lax.broadcasted_iota(jnp.int32, (16 * NE, T), 1) // CAP
    rank_lane = lax.rem(lax.broadcasted_iota(jnp.int32, (T, T), 1), CAP).astype(F32)

    def spread(idx, rows, weighted):
        pick = jnp.where(e0 == e1 + idx * NE, 1.0, 0.0).astype(BF16)
        hit = dot(rt[...], pick) == rank_lane
        if weighted:
            for k in range(3):
                sb[k] = jnp.where(hit, dot(gt[k], pick), 0.0).astype(BF16)
            return dot(sb[0], rows) + dot(sb[1], rows) + dot(sb[2], rows)
        sb[0] = jnp.where(hit, 1.0, 0.0).astype(BF16)
        return dot(sb[0], rows)

    def combine_all(k, b, recv, copies, weighted):
        def one(i, carry):
            h = 3 - i
            acc[k, h] = spread(2 * h, os_[2 * h].reshape(T, D), weighted)
            swap_copy(b, recv, h).wait_recv()
            acc[k, h] = acc[k, h] + spread(8 + h, recv[h].reshape(T, D), weighted)

            @pl.when(i == 0)
            def _():
                copies[0].start()
                copies[1].start()

            @pl.when(i == 1)
            def _():
                copies[3].start()

            @pl.when(i == 2)
            def _():
                copies[2].start()
            return carry
        lax.fori_loop(0, 4, one, 0)

    ro = reduce_copies(RS_O, 0)
    cy[2].wait_recv()
    for h in order:
        swap_copy(OX, orv, h).start()
    cy[7].start()
    cy[4].wait_recv()
    cy[8].start()
    combine_all(0, OX, orv, ro, True)

    cy[5].wait_recv()
    cy[6].wait_recv()
    cy[9].start()
    cy[0].wait_recv()
    cy[7].wait_recv()
    cy[8].wait_recv()
    cy[9].wait_recv()
    for c in cx:
        c.wait_send()

    swap_gg = rc(GG, gj.at[1], gr, 1)
    gg_diag = rc(GG + 1, gacc.at[3], gd, 4)
    gg_y = rc(GG + 2, gacc.at[2], gf.at[1], 4)
    gg_x = rc(GG + 3, gacc.at[1], gf.at[0], 2)

    def gather_dy(d, carry):
        build_p(d)
        rows = dot(pb[...], dya[d])
        outs = os_[d].reshape(T, D).astype(F32)
        gg_rows = jnp.sum(rows * outs, axis=1, keepdims=True)
        r_d = rm[d]
        g_d = gm[d]
        r_ids = ra[d].astype(F32)
        gg_d = jnp.zeros((8, T), F32)
        for l in range(NE):
            hit = lane_r == r_d[l:l + 1, :]
            gcol = jnp.sum(jnp.where(hit, g_d[l:l + 1, :], 0.0), axis=1, keepdims=True)
            xa[d, l * CAP:(l + 1) * CAP, :] = (gcol * rows[l * CAP:(l + 1) * CAP, :]).astype(BF16)
            gg_l = jnp.sum(
                jnp.where(hit, gg_rows[l * CAP:(l + 1) * CAP, :], 0.0), axis=0, keepdims=True)
            gg_d = gg_d + jnp.where(r_ids == (me * NE + l).astype(F32), gg_l, 0.0)
        gj[lax.rem(d, 2), d // 2] = gg_d
        return carry

    lax.fori_loop(0, 8, gather_dy, 0)
    swap_gg.start()
    for h in order:
        swap_copy(OX, orv, h).wait_send()

    swap_gg.wait_recv()
    gacc[...] = gj[0] + gr[...]
    gg_diag.start()
    gg_y.start()
    ro[0].wait_recv()
    acc[0, 2, :H] = acc[0, 2, :H] + rd[0, 0]
    ro[5].start()
    ro[1].wait_recv()
    acc[0, 1, H:] = acc[0, 1, H:] + rd[0, 1]
    ro[4].start()

    def expert_rows(buf, l):
        return buf[:, pl.ds(pl.multiple_of(l * CAP, CAP), CAP), :].reshape(T, D)

    def backward(l, carry):
        dh = dotg(expert_rows(xa, l), wd[l], NT).astype(BF16).astype(F32)
        uf = us[l].astype(F32)
        vf = vs[l].astype(F32)
        s = jax.nn.sigmoid(uf)
        sl = uf * s
        hs[l] = (sl * vf).astype(BF16)
        dv = (dh * sl).astype(BF16)
        du = (dh * vf * (s + sl * (1.0 - s))).astype(BF16)
        us[l] = du
        vs[l] = dv
        pr = (dotg(du, wg[l], NT) + dotg(dv, wu[l], NT)).astype(BF16)
        os_[:, pl.ds(l, 1)] = pr.reshape(8, 1, CAP, D)
        return carry

    out_xg = pltpu.make_async_copy(xg, xg_ref, lsem.at[5])
    out_c = pltpu.make_async_copy(xa, c_ref, lsem.at[6])
    out_xg.start()
    out_c.start()
    lax.fori_loop(0, NE, backward, 0)

    rp = reduce_copies(RS_P, 1)
    gg_diag.wait_recv()
    gacc[1] = gacc[1] + gd[...]
    for h in order:
        swap_copy(PX, prv, h).start()
    gg_x.start()
    combine_all(1, PX, prv, rp, False)

    lo, hi = pl.ds(0, H), pl.ds(H, H)
    early = [
        pltpu.make_async_copy(acc.at[1, 0], base_ref, lsem.at[8]),
        pltpu.make_async_copy(acc.at[1, 1, pl.ds(FILL_X, H - FILL_X)],
                              mx_ref.at[pl.ds(0, H - FILL_X)], lsem.at[9]),
        pltpu.make_async_copy(acc.at[1, 2, pl.ds(H, H - FILL_Y)],
                              my_ref.at[pl.ds(H, H - FILL_Y)], lsem.at[10]),
        pltpu.make_async_copy(us, du_ref, lsem.at[14]),
        pltpu.make_async_copy(vs, dv_ref, lsem.at[15]),
        pltpu.make_async_copy(hs, h_ref, lsem.at[16]),
    ]
    for c in early:
        c.start()
    for i in (2, 3, 4, 5):
        ro[i].wait_recv()
    moe_sc[...] = (acc[0, 0] + fr[0] + fr[1]).astype(BF16)
    out_moe = pltpu.make_async_copy(moe_sc, moe_ref, lsem.at[11])
    out_moe.start()
    for c in cr + cg + cy + ro + [swap_gg, gg_diag, gg_y]:
        c.wait_send()
    for h in order:
        swap_copy(PX, prv, h).wait_send()
    late_y = pltpu.make_async_copy(acc.at[1, 2, lo], my_ref.at[lo], lsem.at[12])
    late_x = pltpu.make_async_copy(acc.at[1, 1, hi], mx_ref.at[pl.ds(H - FILL_X, H)], lsem.at[13])
    rp[0].wait_recv()
    acc[1, 2, :H] = acc[1, 2, :H] + rd[1, 0]
    late_y.start()
    rp[1].wait_recv()
    acc[1, 1, H:] = acc[1, 1, H:] + rd[1, 1]
    late_x.start()
    gg_x.wait_recv()
    gg_y.wait_recv()
    gd[...] = gacc[0] + gf[0] + gf[1]
    out_gg = pltpu.make_async_copy(gd, gg_ref, lsem.at[7])
    out_gg.start()
    rp[2].wait_recv()
    rp[3].wait_recv()
    for c in rp + [gg_x]:
        c.wait_send()
    for c in early + [out_xg, out_c, out_moe, out_gg, late_y, late_x]:
        c.wait()


def publish(T, D, xg_ref, c_ref, du_ref, dv_ref, h_ref, moe_in, gg_in,
            dwg_ref, dwu_ref, dwd_ref, moe_ref, gg_ref):
    rows = xg_ref[...].reshape(T, D)
    dwg_ref[0] = dotg(rows, du_ref[0], TN)
    dwu_ref[0] = dotg(rows, dv_ref[0], TN)
    dwd_ref[0] = dotg(h_ref[0], c_ref[...].reshape(T, D), TN)

    @pl.when(pl.program_id(0) == 0)
    def _():
        moe_ref[...] = moe_in[...]
        gg_ref[...] = gg_in[...]


def solution(mesh):
    tok_spec = P(ALL_AXES, None)
    w_spec = P(EP_AXES, None, None)
    gw_spec = P(ALL_AXES, None, None)

    def local_step(tokens, route_idx, gate_vals, w_gate, w_up, w_down, grad_out):
        T, K = route_idx.shape
        D = tokens.shape[1]
        NE, _, FF = w_gate.shape
        CAP = T * K // (8 * NE)
        hbm = pl.BlockSpec(memory_space=pl.ANY)
        sds = jax.ShapeDtypeStruct
        outs = pl.pallas_call(
            functools.partial(kernel, T, D, FF, NE, CAP),
            out_shape=(sds((T, D), BF16), sds((K, T), F32),
                       sds((T, D), F32), sds((T - FILL_X, D), F32), sds((T - FILL_Y, D), F32),
                       sds((FILL_X, D), F32), sds((FILL_Y, D), F32),
                       sds((8, NE, CAP, D), BF16), sds((8, T, D), BF16),
                       sds((NE, T, FF), BF16), sds((NE, T, FF), BF16), sds((NE, T, FF), BF16)),
            in_specs=[hbm] * 7,
            out_specs=(hbm,) * 12,
            scratch_shapes=[
                pltpu.VMEM((8, T, D), BF16),
                pltpu.VMEM((8, T, D), BF16),
                pltpu.VMEM((8, NE, CAP, D), BF16),
                pltpu.VMEM((NE, T, FF), BF16),
                pltpu.VMEM((NE, T, FF), BF16),
                pltpu.VMEM((NE, T, FF), BF16),
                pltpu.VMEM((8, NE, CAP, D), BF16),
                pltpu.VMEM((NE, D, FF), BF16),
                pltpu.VMEM((NE, D, FF), BF16),
                pltpu.VMEM((NE, FF, D), BF16),
                pltpu.VMEM((2, 4, T, D), F32),
                pltpu.VMEM((2, 2, T // 2, D), F32),
                pltpu.VMEM((2, T, D), F32),
                pltpu.VMEM((4, NE, CAP, D), BF16),
                pltpu.VMEM((4, NE, CAP, D), BF16),
                pltpu.VMEM((T, T), BF16),
                pltpu.VMEM((3, T, T), BF16),
                pltpu.VMEM((K, T), jnp.int32),
                pltpu.VMEM((8, K, T), BF16),
                pltpu.VMEM((8, K, T), F32),
                pltpu.VMEM((16, NE, T), F32),
                pltpu.VMEM((16, NE, T), F32),
                pltpu.VMEM((16, NE, T), F32),
                pltpu.VMEM((T, 16 * NE), BF16),
                pltpu.VMEM((3, T, 16 * NE), BF16),
                pltpu.VMEM((2, 4, K, T), F32),
                pltpu.VMEM((4, K, T), F32),
                pltpu.VMEM((4, K, T), F32),
                pltpu.VMEM((K, T), F32),
                pltpu.VMEM((2, K, T), F32),
                pltpu.VMEM((T, D), BF16),
                pltpu.SemaphoreType.DMA((N_SEM,)),
                pltpu.SemaphoreType.DMA((N_SEM,)),
                pltpu.SemaphoreType.DMA((17,)),
            ],
            compiler_params=pltpu.CompilerParams(
                collective_id=0, has_side_effects=True, vmem_limit_bytes=67043328),
        )(tokens, grad_out, route_idx.T, gate_vals.T, w_gate, w_up, w_down)
        moe, gg, base, mx, my, fx, fy, xg, c, du, dv, h = outs
        rx = lax.ppermute(mx, 'col', [(0, 1), (1, 0)])
        ry = lax.ppermute(my, 'row', [(0, 1), (1, 0)])

        def per_expert(*shape):
            return pl.BlockSpec((1,) + shape, lambda l: (l, 0, 0))

        def whole(a):
            return pl.BlockSpec(a.shape, lambda l: (0, 0))

        dwg, dwu, dwd, moe, gg = pl.pallas_call(
            functools.partial(publish, T, D),
            grid=(NE,),
            out_shape=(sds((NE, D, FF), F32), sds((NE, D, FF), F32), sds((NE, FF, D), F32),
                       sds(moe.shape, BF16), sds(gg.shape, F32)),
            in_specs=[pl.BlockSpec((8, 1, CAP, D), lambda l: (0, l, 0, 0)),
                      pl.BlockSpec((8, CAP, D), lambda l: (0, l, 0)),
                      per_expert(T, FF), per_expert(T, FF), per_expert(T, FF), whole(moe), whole(gg)],
            out_specs=(per_expert(D, FF), per_expert(D, FF), per_expert(FF, D), whole(moe), whole(gg)),
            cost_estimate=pl.CostEstimate(
                flops=6 * NE * T * D * FF, bytes_accessed=36 * 1024 * 1024, transcendentals=0),
            compiler_params=pltpu.CompilerParams(vmem_limit_bytes=60 * 1024 * 1024),
        )(xg, c, du, dv, h, moe, gg)
        gx = (base + jnp.concatenate([fx, rx]) + jnp.concatenate([ry, fy])).astype(BF16)
        return moe, gx, gg.T, dwg, dwu, dwd

    return jax.shard_map(
        local_step, mesh=mesh,
        in_specs=(tok_spec, tok_spec, tok_spec, w_spec, w_spec, w_spec, tok_spec),
        out_specs=(tok_spec, tok_spec, tok_spec, gw_spec, gw_spec, gw_spec),
        check_vma=False)
```

```python
import functools

import jax
import jax.numpy as jnp
from jax import lax
from jax.experimental import pallas as pl
from jax.experimental.pallas import tpu as pltpu
from jax.sharding import PartitionSpec as P


EP_AXES = ('row', 'col', 'core')
ALL_AXES = ('part', 'row', 'col', 'core')
MESH = pl.DeviceIdType.MESH
F32 = jnp.float32
BF16 = jnp.bfloat16
NT = (((1,), (1,)), ((), ()))
TN = (((0,), (0,)), ((), ()))

AG_X, AG_DY, RG, OX, PX, RS_O, RS_P, GG, N_SEM = 0, 10, 20, 34, 38, 42, 48, 52, 56


FILL_X, FILL_Y = 104, 96


def dot(a, b):
    return jnp.dot(a, b, preferred_element_type=F32)


def dotg(a, b, dims):
    return lax.dot_general(a, b, dims, preferred_element_type=F32)


def kernel(T, D, FF, NE, CAP,
           x_ref, dy_ref, route_ref, gate_ref, wg_ref, wu_ref, wd_ref,
           moe_ref, gg_ref, base_ref, mx_ref, my_ref, fx_ref, fy_ref, xg_ref, c_ref, du_ref, dv_ref, h_ref,
           xa, dya, xg, us, vs, hs, os_, wg, wu, wd, acc, rd, fr, orv, prv,
           pb, sb, r0, ra, ga, rm, gm, mb, rt, gt, gj, gr, gacc, gd, gf, moe_sc,
           ssem, rsem, lsem):
    H = T // 2
    row, col, core = lax.axis_index('row'), lax.axis_index('col'), lax.axis_index('core')
    me = row * 4 + col * 2 + core
    partner = row * 4 + col * 2 + (1 - core)

    def dev(rel):
        return {
            'row': 1 - row if rel & 4 else row,
            'col': 1 - col if rel & 2 else col,
            'core': 1 - core if rel & 1 else core,
        }

    def rc(i, src, dst, rel):
        return pltpu.make_async_remote_copy(
            src_ref=src, dst_ref=dst, send_sem=ssem.at[i], recv_sem=rsem.at[i],
            device_id=dev(rel), device_id_type=MESH)

    def gather_copies(b, buf):
        lo, hi = pl.ds(0, H), pl.ds(H, H)
        return [
            rc(b + 0, buf.at[0], buf.at[1], 1),
            rc(b + 1, buf.at[0, hi], buf.at[2, hi], 2),
            rc(b + 2, buf.at[0, lo], buf.at[2, lo], 2),
            rc(b + 3, buf.at[0, lo], buf.at[4, lo], 4),
            rc(b + 4, buf.at[0, hi], buf.at[4, hi], 4),
            rc(b + 5, buf.at[2, hi], buf.at[6, hi], 4),
            rc(b + 6, buf.at[4, lo], buf.at[6, lo], 2),
            rc(b + 7, buf.at[2], buf.at[3], 1),
            rc(b + 8, buf.at[4], buf.at[5], 1),
            rc(b + 9, buf.at[6], buf.at[7], 1),
        ]

    lx = pltpu.make_async_copy(x_ref, xa.at[0], lsem.at[0])
    ldy = pltpu.make_async_copy(dy_ref, dya.at[0], lsem.at[1])
    lwg = pltpu.make_async_copy(wg_ref, wg, lsem.at[2])
    lwu = pltpu.make_async_copy(wu_ref, wu, lsem.at[3])
    lwd = pltpu.make_async_copy(wd_ref, wd, lsem.at[4])
    lr = pltpu.make_async_copy(route_ref, r0, lsem.at[14])
    lg = pltpu.make_async_copy(gate_ref, ga.at[0], lsem.at[15])
    lx.start()
    lr.start()
    lg.start()
    ldy.start()
    lwg.start()
    lwu.start()
    lwd.start()

    barrier = pltpu.get_barrier_semaphore()
    for rel in (1, 2, 4):
        pl.semaphore_signal(barrier, inc=1, device_id=dev(rel), device_id_type=MESH)
    pl.semaphore_wait(barrier, 3)

    def small_copies(b, src, buf, diag):
        return [
            rc(b + 0, src, buf.at[1], 1),
            rc(b + 1, src, buf.at[2], 2),
            rc(b + 2, src, buf.at[4], 4),
            rc(b + 3, buf.at[6 - diag], buf.at[6], diag),
            rc(b + 4, buf.at[2], buf.at[3], 1),
            rc(b + 5, buf.at[4], buf.at[5], 1),
            rc(b + 6, buf.at[6], buf.at[7], 1),
        ]

    cr = small_copies(RG, ra.at[0], ra, 2)
    cg = small_copies(RG + 7, ga.at[0], ga, 4)
    cx = gather_copies(AG_X, xa)
    cy = gather_copies(AG_DY, dya)
    lr.wait()
    ra[0] = r0[...].astype(F32).astype(BF16)
    lg.wait()
    for i in (1, 2, 0):
        cg[i].start()
    lx.wait()
    for i in (1, 2, 0):
        cr[i].start()
    for i in (1, 3, 0):
        cx[i].start()
    cr[2].wait_recv()
    cr[3].start()
    cg[1].wait_recv()
    cg[3].start()
    cx[2].start()
    cx[4].start()
    cr[5].start()
    cg[4].start()
    cr[1].wait_recv()
    cr[4].start()
    cg[2].wait_recv()
    cg[5].start()

    i0 = lax.broadcasted_iota(jnp.int32, (T, T), 0)
    i1 = lax.broadcasted_iota(jnp.int32, (T, T), 1)
    sb[0] = (i0 < i1).astype(F32).astype(BF16)
    sb[1] = (i0 > i1).astype(F32).astype(BF16)
    sb[2] = (i0 == i1).astype(F32).astype(BF16)
    cx[1].wait_recv()
    cx[5].start()
    cx[3].wait_recv()
    cx[6].start()
    cr[3].wait_recv()
    cr[6].start()
    cg[3].wait_recv()
    cg[6].start()
    for i in (0, 4, 5, 6):
        cr[i].wait_recv()
        cg[i].wait_recv()
    mb[...] = jnp.zeros_like(mb)
    gm[...] = jnp.zeros_like(gm)
    sub = lax.broadcasted_iota(jnp.int32, (NE, T), 0)
    for idx in range(12):
        src = idx if idx < 8 else 2 * (idx - 8)
        owner = me if idx < 8 else partner
        ids = (sub + owner * NE).astype(F32)
        routes = ra[src].astype(F32)
        hits = jnp.zeros((NE, T), F32)
        gates = jnp.zeros((NE, T), F32)
        for j in range(8):
            hit = routes[j:j + 1, :] == ids
            hits = hits + jnp.where(hit, 1.0, 0.0)
            gates = gates + jnp.where(hit, ga[src, j:j + 1, :], 0.0)
        mb[idx] = hits
        gm[idx] = gates
    m_all = mb[...].reshape(16 * NE, T)
    m_bf = m_all.astype(BF16)
    ranks = dot(m_bf, sb[0])
    rm[...] = jnp.where(m_all > 0.5, ranks, -1.0).reshape(16, NE, T)
    m_t = dotg(sb[2], m_bf, NT)
    r_t = dotg(sb[1], m_bf, NT)
    rt[...] = jnp.where(m_t > 0.5, r_t, -1.0).astype(BF16)
    g_all = gm[...].reshape(16 * NE, T)
    g_hi = g_all.astype(BF16)
    rest = g_all - g_hi.astype(F32)
    g_mid = rest.astype(BF16)
    g_lo = (rest - g_mid.astype(F32)).astype(BF16)
    for k, piece in enumerate((g_hi, g_mid, g_lo)):
        gt[k] = dotg(sb[2], piece, NT).astype(BF16)

    lane_r = lax.broadcasted_iota(jnp.int32, (CAP, T), 0).astype(F32)

    def build_p(d):
        r_d = rm[d]
        for l in range(NE):
            pb[l * CAP:(l + 1) * CAP, :] = jnp.where(lane_r == r_d[l:l + 1, :], 1.0, 0.0).astype(BF16)

    def gather_x(d):
        build_p(d)
        xg[d] = dot(pb[...], xa[d]).astype(BF16).reshape(NE, CAP, D)

    def gather_x_loop(first, step, count):
        def one(i, carry):
            gather_x(first + step * i)
            return carry
        lax.fori_loop(0, count, one, 0)

    cx[0].wait_recv()
    gather_x_loop(0, 1, 2)
    cx[2].wait_recv()
    cx[7].start()
    cx[4].wait_recv()
    cx[8].start()
    ldy.wait()
    for i in (1, 3, 0, 2, 4):
        cy[i].start()
    gather_x_loop(2, 2, 2)
    cx[7].wait_recv()
    cx[8].wait_recv()
    gather_x_loop(3, 2, 2)
    cx[5].wait_recv()
    cx[6].wait_recv()
    cx[9].start()
    gather_x_loop(6, 1, 1)
    cx[9].wait_recv()
    gather_x_loop(7, 1, 1)

    lwg.wait()
    lwu.wait()
    lwd.wait()

    def forward(l, carry):
        rows = xg[:, pl.ds(l, 1)].reshape(T, D)
        u = dot(rows, wg[l]).astype(BF16)
        v = dot(rows, wu[l]).astype(BF16)
        us[l] = u
        vs[l] = v
        uf = u.astype(F32)
        h = (uf * jax.nn.sigmoid(uf) * v.astype(F32)).astype(BF16)
        o = dot(h, wd[l]).astype(BF16)
        os_[:, pl.ds(l, 1)] = o.reshape(8, 1, CAP, D)
        return carry

    lax.fori_loop(0, NE // 2, forward, 0)
    cy[1].wait_recv()
    cy[5].start()
    cy[3].wait_recv()
    cy[6].start()
    lax.fori_loop(NE // 2, NE, forward, 0)

    order = (3, 1, 2, 0)

    def swap_copy(b, buf, h):
        return rc(b + h, os_.at[2 * h + 1], buf.at[h], 1)

    def reduce_copies(b, k):
        lo, hi = pl.ds(0, H), pl.ds(H, H)
        diag = [
            rc(b + 0, acc.at[k, 3, lo], rd.at[k, 0], 2),
            rc(b + 1, acc.at[k, 3, hi], rd.at[k, 1], 4),
        ]
        if k == 1:
            return diag + [
                rc(b + 2, acc.at[k, 1, pl.ds(0, FILL_X)], fx_ref, 2),
                rc(b + 3, acc.at[k, 2, pl.ds(T - FILL_Y, FILL_Y)], fy_ref, 4),
            ]
        return diag + [
            rc(b + 2, acc.at[k, 1, lo], fr.at[0, lo], 2),
            rc(b + 3, acc.at[k, 2, hi], fr.at[1, hi], 4),
            rc(b + 4, acc.at[k, 1, hi], fr.at[0, hi], 2),
            rc(b + 5, acc.at[k, 2, lo], fr.at[1, lo], 4),
        ]

    e0 = lax.broadcasted_iota(jnp.int32, (16 * NE, T), 0)
    e1 = lax.broadcasted_iota(jnp.int32, (16 * NE, T), 1) // CAP
    rank_lane = lax.rem(lax.broadcasted_iota(jnp.int32, (T, T), 1), CAP).astype(F32)

    def spread(idx, rows, weighted):
        pick = jnp.where(e0 == e1 + idx * NE, 1.0, 0.0).astype(BF16)
        hit = dot(rt[...], pick) == rank_lane
        if weighted:
            for k in range(3):
                sb[k] = jnp.where(hit, dot(gt[k], pick), 0.0).astype(BF16)
            return dot(sb[0], rows) + dot(sb[1], rows) + dot(sb[2], rows)
        sb[0] = jnp.where(hit, 1.0, 0.0).astype(BF16)
        return dot(sb[0], rows)

    def combine_all(k, b, recv, copies, weighted, after_first=None):
        def one(i, carry):
            h = 3 - i
            acc[k, h] = spread(2 * h, os_[2 * h].reshape(T, D), weighted)
            swap_copy(b, recv, h).wait_recv()
            acc[k, h] = acc[k, h] + spread(8 + h, recv[h].reshape(T, D), weighted)

            @pl.when(i == 0)
            def _():
                copies[0].start()
                copies[1].start()
                if after_first is not None:
                    after_first()

            @pl.when(i == 1)
            def _():
                copies[3].start()

            @pl.when(i == 2)
            def _():
                copies[2].start()
            return carry
        lax.fori_loop(0, 4, one, 0)

    ro = reduce_copies(RS_O, 0)
    for h in order:
        swap_copy(OX, orv, h).start()
    def pass_dy():
        cy[2].wait_recv()
        cy[7].start()
        cy[4].wait_recv()
        cy[8].start()

    combine_all(0, OX, orv, ro, True, pass_dy)

    cy[5].wait_recv()
    cy[6].wait_recv()
    cy[9].start()
    cy[0].wait_recv()
    cy[7].wait_recv()
    cy[8].wait_recv()
    cy[9].wait_recv()
    for c in cx:
        c.wait_send()

    swap_gg = rc(GG, gj.at[1], gr, 1)
    gg_diag = rc(GG + 1, gacc.at[3], gd, 4)
    gg_y = rc(GG + 2, gacc.at[2], gf.at[1], 4)
    gg_x = rc(GG + 3, gacc.at[1], gf.at[0], 2)

    def gather_dy(d, carry):
        build_p(d)
        rows = dot(pb[...], dya[d])
        outs = os_[d].reshape(T, D).astype(F32)
        gg_rows = jnp.sum(rows * outs, axis=1, keepdims=True)
        r_d = rm[d]
        g_d = gm[d]
        r_ids = ra[d].astype(F32)
        gg_d = jnp.zeros((8, T), F32)
        for l in range(NE):
            hit = lane_r == r_d[l:l + 1, :]
            gcol = jnp.sum(jnp.where(hit, g_d[l:l + 1, :], 0.0), axis=1, keepdims=True)
            xa[d, l * CAP:(l + 1) * CAP, :] = (gcol * rows[l * CAP:(l + 1) * CAP, :]).astype(BF16)
            gg_l = jnp.sum(
                jnp.where(hit, gg_rows[l * CAP:(l + 1) * CAP, :], 0.0), axis=0, keepdims=True)
            gg_d = gg_d + jnp.where(r_ids == (me * NE + l).astype(F32), gg_l, 0.0)
        gj[lax.rem(d, 2), d // 2] = gg_d
        return carry

    lax.fori_loop(0, 8, gather_dy, 0)
    swap_gg.start()
    for h in order:
        swap_copy(OX, orv, h).wait_send()

    swap_gg.wait_recv()
    gacc[...] = gj[0] + gr[...]
    gg_diag.start()
    gg_y.start()
    ro[0].wait_recv()
    acc[0, 2, :H] = acc[0, 2, :H] + rd[0, 0]
    ro[5].start()
    ro[1].wait_recv()
    acc[0, 1, H:] = acc[0, 1, H:] + rd[0, 1]
    ro[4].start()

    def expert_rows(buf, l):
        return buf[:, pl.ds(pl.multiple_of(l * CAP, CAP), CAP), :].reshape(T, D)

    def backward(l, carry):
        dh = dotg(expert_rows(xa, l), wd[l], NT).astype(BF16).astype(F32)
        uf = us[l].astype(F32)
        vf = vs[l].astype(F32)
        s = jax.nn.sigmoid(uf)
        sl = uf * s
        hs[l] = (sl * vf).astype(BF16)
        dv = (dh * sl).astype(BF16)
        du = (dh * vf * (s + sl * (1.0 - s))).astype(BF16)
        us[l] = du
        vs[l] = dv
        pr = (dotg(du, wg[l], NT) + dotg(dv, wu[l], NT)).astype(BF16)
        os_[:, pl.ds(l, 1)] = pr.reshape(8, 1, CAP, D)
        return carry

    out_xg = pltpu.make_async_copy(xg, xg_ref, lsem.at[5])
    out_c = pltpu.make_async_copy(xa, c_ref, lsem.at[6])
    out_xg.start()
    out_c.start()
    lax.fori_loop(0, NE, backward, 0)

    rp = reduce_copies(RS_P, 1)
    for h in order:
        swap_copy(PX, prv, h).start()
    gg_diag.wait_recv()
    gacc[1] = gacc[1] + gd[...]
    gg_x.start()
    combine_all(1, PX, prv, rp, False)

    lo, hi = pl.ds(0, H), pl.ds(H, H)
    early = [
        pltpu.make_async_copy(acc.at[1, 0], base_ref, lsem.at[8]),
        pltpu.make_async_copy(acc.at[1, 1, pl.ds(FILL_X, H - FILL_X)],
                              mx_ref.at[pl.ds(0, H - FILL_X)], lsem.at[9]),
        pltpu.make_async_copy(acc.at[1, 2, pl.ds(H, H - FILL_Y)],
                              my_ref.at[pl.ds(H, H - FILL_Y)], lsem.at[10]),
        pltpu.make_async_copy(us, du_ref, lsem.at[14]),
        pltpu.make_async_copy(vs, dv_ref, lsem.at[15]),
        pltpu.make_async_copy(hs, h_ref, lsem.at[16]),
    ]
    for c in early:
        c.start()
    for i in (2, 3, 4, 5):
        ro[i].wait_recv()
    moe_sc[...] = (acc[0, 0] + fr[0] + fr[1]).astype(BF16)
    out_moe = pltpu.make_async_copy(moe_sc, moe_ref, lsem.at[11])
    out_moe.start()
    for c in cr + cg + cy + ro + [swap_gg, gg_diag, gg_y]:
        c.wait_send()
    for h in order:
        swap_copy(PX, prv, h).wait_send()
    late_y = pltpu.make_async_copy(acc.at[1, 2, lo], my_ref.at[lo], lsem.at[12])
    late_x = pltpu.make_async_copy(acc.at[1, 1, hi], mx_ref.at[pl.ds(H - FILL_X, H)], lsem.at[13])
    rp[0].wait_recv()
    acc[1, 2, :H] = acc[1, 2, :H] + rd[1, 0]
    late_y.start()
    rp[1].wait_recv()
    acc[1, 1, H:] = acc[1, 1, H:] + rd[1, 1]
    late_x.start()
    gg_x.wait_recv()
    gg_y.wait_recv()
    gd[...] = gacc[0] + gf[0] + gf[1]
    out_gg = pltpu.make_async_copy(gd, gg_ref, lsem.at[7])
    out_gg.start()
    rp[2].wait_recv()
    rp[3].wait_recv()
    for c in rp + [gg_x]:
        c.wait_send()
    for c in early + [out_xg, out_c, out_moe, out_gg, late_y, late_x]:
        c.wait()


def publish(T, D, xg_ref, c_ref, du_ref, dv_ref, h_ref, moe_in, gg_in,
            dwg_ref, dwu_ref, dwd_ref, moe_ref, gg_ref):
    rows = xg_ref[...].reshape(T, D)
    dwg_ref[0] = dotg(rows, du_ref[0], TN)
    dwu_ref[0] = dotg(rows, dv_ref[0], TN)
    dwd_ref[0] = dotg(h_ref[0], c_ref[...].reshape(T, D), TN)

    @pl.when(pl.program_id(0) == 0)
    def _():
        moe_ref[...] = moe_in[...]
        gg_ref[...] = gg_in[...]


def solution(mesh):
    tok_spec = P(ALL_AXES, None)
    w_spec = P(EP_AXES, None, None)
    gw_spec = P(ALL_AXES, None, None)

    def local_step(tokens, route_idx, gate_vals, w_gate, w_up, w_down, grad_out):
        T, K = route_idx.shape
        D = tokens.shape[1]
        NE, _, FF = w_gate.shape
        CAP = T * K // (8 * NE)
        hbm = pl.BlockSpec(memory_space=pl.ANY)
        sds = jax.ShapeDtypeStruct
        outs = pl.pallas_call(
            functools.partial(kernel, T, D, FF, NE, CAP),
            out_shape=(sds((T, D), BF16), sds((K, T), F32),
                       sds((T, D), F32), sds((T - FILL_X, D), F32), sds((T - FILL_Y, D), F32),
                       sds((FILL_X, D), F32), sds((FILL_Y, D), F32),
                       sds((8, NE, CAP, D), BF16), sds((8, T, D), BF16),
                       sds((NE, T, FF), BF16), sds((NE, T, FF), BF16), sds((NE, T, FF), BF16)),
            in_specs=[hbm] * 7,
            out_specs=(hbm,) * 12,
            scratch_shapes=[
                pltpu.VMEM((8, T, D), BF16),
                pltpu.VMEM((8, T, D), BF16),
                pltpu.VMEM((8, NE, CAP, D), BF16),
                pltpu.VMEM((NE, T, FF), BF16),
                pltpu.VMEM((NE, T, FF), BF16),
                pltpu.VMEM((NE, T, FF), BF16),
                pltpu.VMEM((8, NE, CAP, D), BF16),
                pltpu.VMEM((NE, D, FF), BF16),
                pltpu.VMEM((NE, D, FF), BF16),
                pltpu.VMEM((NE, FF, D), BF16),
                pltpu.VMEM((2, 4, T, D), F32),
                pltpu.VMEM((2, 2, T // 2, D), F32),
                pltpu.VMEM((2, T, D), F32),
                pltpu.VMEM((4, NE, CAP, D), BF16),
                pltpu.VMEM((4, NE, CAP, D), BF16),
                pltpu.VMEM((T, T), BF16),
                pltpu.VMEM((3, T, T), BF16),
                pltpu.VMEM((K, T), jnp.int32),
                pltpu.VMEM((8, K, T), BF16),
                pltpu.VMEM((8, K, T), F32),
                pltpu.VMEM((16, NE, T), F32),
                pltpu.VMEM((16, NE, T), F32),
                pltpu.VMEM((16, NE, T), F32),
                pltpu.VMEM((T, 16 * NE), BF16),
                pltpu.VMEM((3, T, 16 * NE), BF16),
                pltpu.VMEM((2, 4, K, T), F32),
                pltpu.VMEM((4, K, T), F32),
                pltpu.VMEM((4, K, T), F32),
                pltpu.VMEM((K, T), F32),
                pltpu.VMEM((2, K, T), F32),
                pltpu.VMEM((T, D), BF16),
                pltpu.SemaphoreType.DMA((N_SEM,)),
                pltpu.SemaphoreType.DMA((N_SEM,)),
                pltpu.SemaphoreType.DMA((17,)),
            ],
            compiler_params=pltpu.CompilerParams(
                collective_id=0, has_side_effects=True, vmem_limit_bytes=67043328),
        )(tokens, grad_out, route_idx.T, gate_vals.T, w_gate, w_up, w_down)
        moe, gg, base, mx, my, fx, fy, xg, c, du, dv, h = outs
        rx = lax.ppermute(mx, 'col', [(0, 1), (1, 0)])
        ry = lax.ppermute(my, 'row', [(0, 1), (1, 0)])

        def per_expert(*shape):
            return pl.BlockSpec((1,) + shape, lambda l: (l, 0, 0))

        def whole(a):
            return pl.BlockSpec(a.shape, lambda l: (0, 0))

        dwg, dwu, dwd, moe, gg = pl.pallas_call(
            functools.partial(publish, T, D),
            grid=(NE,),
            out_shape=(sds((NE, D, FF), F32), sds((NE, D, FF), F32), sds((NE, FF, D), F32),
                       sds(moe.shape, BF16), sds(gg.shape, F32)),
            in_specs=[pl.BlockSpec((8, 1, CAP, D), lambda l: (0, l, 0, 0)),
                      pl.BlockSpec((8, CAP, D), lambda l: (0, l, 0)),
                      per_expert(T, FF), per_expert(T, FF), per_expert(T, FF), whole(moe), whole(gg)],
            out_specs=(per_expert(D, FF), per_expert(D, FF), per_expert(FF, D), whole(moe), whole(gg)),
            cost_estimate=pl.CostEstimate(
                flops=6 * NE * T * D * FF, bytes_accessed=36 * 1024 * 1024, transcendentals=0),
            compiler_params=pltpu.CompilerParams(vmem_limit_bytes=60 * 1024 * 1024),
        )(xg, c, du, dv, h, moe, gg)
        gx = (base + jnp.concatenate([fx, rx]) + jnp.concatenate([ry, fy])).astype(BF16)
        return moe, gx, gg.T, dwg, dwu, dwd

    return jax.shard_map(
        local_step, mesh=mesh,
        in_specs=(tok_spec, tok_spec, tok_spec, w_spec, w_spec, w_spec, tok_spec),
        out_specs=(tok_spec, tok_spec, tok_spec, gw_spec, gw_spec, gw_spec),
        check_vma=False)
```

```python
import functools

import jax
import jax.numpy as jnp
from jax import lax
from jax.experimental import pallas as pl
from jax.experimental.pallas import tpu as pltpu
from jax.sharding import PartitionSpec as P


EP_AXES = ('row', 'col', 'core')
ALL_AXES = ('part', 'row', 'col', 'core')
MESH = pl.DeviceIdType.MESH
F32 = jnp.float32
BF16 = jnp.bfloat16
NT = (((1,), (1,)), ((), ()))
TN = (((0,), (0,)), ((), ()))

AG_X, AG_DY, RG, OX, PX, RS_O, RS_P, GG, N_SEM = 0, 10, 20, 34, 38, 42, 48, 52, 56


FILL_X, FILL_Y = 112, 96


def dot(a, b):
    return jnp.dot(a, b, preferred_element_type=F32)


def dotg(a, b, dims):
    return lax.dot_general(a, b, dims, preferred_element_type=F32)


def kernel(T, D, FF, NE, CAP,
           x_ref, dy_ref, route_ref, gate_ref, wg_ref, wu_ref, wd_ref,
           moe_ref, gg_ref, base_ref, mx_ref, my_ref, fx_ref, fy_ref, xg_ref, c_ref, du_ref, dv_ref, h_ref,
           xa, dya, xg, us, vs, hs, os_, wg, wu, wd, acc, rd, fr, orv, prv,
           pb, sb, r0, ra, ga, rm, gm, mb, rt, gt, gj, gr, gacc, gd, gf, moe_sc,
           ssem, rsem, lsem):
    H = T // 2
    row, col, core = lax.axis_index('row'), lax.axis_index('col'), lax.axis_index('core')
    me = row * 4 + col * 2 + core
    partner = row * 4 + col * 2 + (1 - core)

    def dev(rel):
        return {
            'row': 1 - row if rel & 4 else row,
            'col': 1 - col if rel & 2 else col,
            'core': 1 - core if rel & 1 else core,
        }

    def rc(i, src, dst, rel):
        return pltpu.make_async_remote_copy(
            src_ref=src, dst_ref=dst, send_sem=ssem.at[i], recv_sem=rsem.at[i],
            device_id=dev(rel), device_id_type=MESH)

    def gather_copies(b, buf):
        lo, hi = pl.ds(0, H), pl.ds(H, H)
        return [
            rc(b + 0, buf.at[0], buf.at[1], 1),
            rc(b + 1, buf.at[0, hi], buf.at[2, hi], 2),
            rc(b + 2, buf.at[0, lo], buf.at[2, lo], 2),
            rc(b + 3, buf.at[0, lo], buf.at[4, lo], 4),
            rc(b + 4, buf.at[0, hi], buf.at[4, hi], 4),
            rc(b + 5, buf.at[2, hi], buf.at[6, hi], 4),
            rc(b + 6, buf.at[4, lo], buf.at[6, lo], 2),
            rc(b + 7, buf.at[2], buf.at[3], 1),
            rc(b + 8, buf.at[4], buf.at[5], 1),
            rc(b + 9, buf.at[6], buf.at[7], 1),
        ]

    lx = pltpu.make_async_copy(x_ref, xa.at[0], lsem.at[0])
    ldy = pltpu.make_async_copy(dy_ref, dya.at[0], lsem.at[1])
    lwg = pltpu.make_async_copy(wg_ref, wg, lsem.at[2])
    lwu = pltpu.make_async_copy(wu_ref, wu, lsem.at[3])
    lwd = pltpu.make_async_copy(wd_ref, wd, lsem.at[4])
    lr = pltpu.make_async_copy(route_ref, r0, lsem.at[14])
    lg = pltpu.make_async_copy(gate_ref, ga.at[0], lsem.at[15])
    lx.start()
    lr.start()
    lg.start()
    ldy.start()
    lwg.start()
    lwu.start()
    lwd.start()

    barrier = pltpu.get_barrier_semaphore()
    for rel in (1, 2, 4):
        pl.semaphore_signal(barrier, inc=1, device_id=dev(rel), device_id_type=MESH)
    pl.semaphore_wait(barrier, 3)

    def small_copies(b, src, buf, diag):
        return [
            rc(b + 0, src, buf.at[1], 1),
            rc(b + 1, src, buf.at[2], 2),
            rc(b + 2, src, buf.at[4], 4),
            rc(b + 3, buf.at[6 - diag], buf.at[6], diag),
            rc(b + 4, buf.at[2], buf.at[3], 1),
            rc(b + 5, buf.at[4], buf.at[5], 1),
            rc(b + 6, buf.at[6], buf.at[7], 1),
        ]

    cr = small_copies(RG, ra.at[0], ra, 2)
    cg = small_copies(RG + 7, ga.at[0], ga, 4)
    cx = gather_copies(AG_X, xa)
    cy = gather_copies(AG_DY, dya)
    lr.wait()
    ra[0] = r0[...].astype(F32).astype(BF16)
    lg.wait()
    for i in (1, 2, 0):
        cg[i].start()
    lx.wait()
    for i in (1, 2, 0):
        cr[i].start()
    for i in (1, 3, 0):
        cx[i].start()
    cr[2].wait_recv()
    cr[3].start()
    cg[1].wait_recv()
    cg[3].start()
    cx[2].start()
    cx[4].start()
    cr[5].start()
    cg[4].start()
    cr[1].wait_recv()
    cr[4].start()
    cg[2].wait_recv()
    cg[5].start()

    i0 = lax.broadcasted_iota(jnp.int32, (T, T), 0)
    i1 = lax.broadcasted_iota(jnp.int32, (T, T), 1)
    sb[0] = (i0 < i1).astype(F32).astype(BF16)
    sb[1] = (i0 > i1).astype(F32).astype(BF16)
    sb[2] = (i0 == i1).astype(F32).astype(BF16)
    cx[1].wait_recv()
    cx[5].start()
    cx[3].wait_recv()
    cx[6].start()
    cr[3].wait_recv()
    cr[6].start()
    cg[3].wait_recv()
    cg[6].start()
    for i in (0, 4, 5, 6):
        cr[i].wait_recv()
        cg[i].wait_recv()
    mb[...] = jnp.zeros_like(mb)
    gm[...] = jnp.zeros_like(gm)
    sub = lax.broadcasted_iota(jnp.int32, (NE, T), 0)
    for idx in range(12):
        src = idx if idx < 8 else 2 * (idx - 8)
        owner = me if idx < 8 else partner
        ids = (sub + owner * NE).astype(F32)
        routes = ra[src].astype(F32)
        hits = jnp.zeros((NE, T), F32)
        gates = jnp.zeros((NE, T), F32)
        for j in range(8):
            hit = routes[j:j + 1, :] == ids
            hits = hits + jnp.where(hit, 1.0, 0.0)
            gates = gates + jnp.where(hit, ga[src, j:j + 1, :], 0.0)
        mb[idx] = hits
        gm[idx] = gates
    m_all = mb[...].reshape(16 * NE, T)
    m_bf = m_all.astype(BF16)
    ranks = dot(m_bf, sb[0])
    rm[...] = jnp.where(m_all > 0.5, ranks, -1.0).reshape(16, NE, T)
    m_t = dotg(sb[2], m_bf, NT)
    r_t = dotg(sb[1], m_bf, NT)
    rt[...] = jnp.where(m_t > 0.5, r_t, -1.0).astype(BF16)
    g_all = gm[...].reshape(16 * NE, T)
    g_hi = g_all.astype(BF16)
    rest = g_all - g_hi.astype(F32)
    g_mid = rest.astype(BF16)
    g_lo = (rest - g_mid.astype(F32)).astype(BF16)
    for k, piece in enumerate((g_hi, g_mid, g_lo)):
        gt[k] = dotg(sb[2], piece, NT).astype(BF16)

    lane_r = lax.broadcasted_iota(jnp.int32, (CAP, T), 0).astype(F32)

    def build_p(d):
        r_d = rm[d]
        for l in range(NE):
            pb[l * CAP:(l + 1) * CAP, :] = jnp.where(lane_r == r_d[l:l + 1, :], 1.0, 0.0).astype(BF16)

    def gather_x(d):
        build_p(d)
        xg[d] = dot(pb[...], xa[d]).astype(BF16).reshape(NE, CAP, D)

    def gather_x_loop(first, step, count):
        def one(i, carry):
            gather_x(first + step * i)
            return carry
        lax.fori_loop(0, count, one, 0)

    cx[0].wait_recv()
    gather_x_loop(0, 1, 2)
    cx[2].wait_recv()
    cx[7].start()
    cx[4].wait_recv()
    cx[8].start()
    ldy.wait()
    for i in (1, 3, 0, 2, 4):
        cy[i].start()
    gather_x_loop(2, 2, 2)
    cx[7].wait_recv()
    cx[8].wait_recv()
    gather_x_loop(3, 2, 2)
    cx[5].wait_recv()
    cx[6].wait_recv()
    cx[9].start()
    gather_x_loop(6, 1, 1)
    cx[9].wait_recv()
    gather_x_loop(7, 1, 1)

    lwg.wait()
    lwu.wait()
    lwd.wait()

    def forward(l, carry):
        rows = xg[:, pl.ds(l, 1)].reshape(T, D)
        u = dot(rows, wg[l]).astype(BF16)
        v = dot(rows, wu[l]).astype(BF16)
        us[l] = u
        vs[l] = v
        uf = u.astype(F32)
        h = (uf * jax.nn.sigmoid(uf) * v.astype(F32)).astype(BF16)
        o = dot(h, wd[l]).astype(BF16)
        os_[:, pl.ds(l, 1)] = o.reshape(8, 1, CAP, D)
        return carry

    lax.fori_loop(0, NE // 2, forward, 0)
    cy[1].wait_recv()
    cy[5].start()
    cy[3].wait_recv()
    cy[6].start()
    lax.fori_loop(NE // 2, NE, forward, 0)

    order = (3, 1, 2, 0)

    def swap_copy(b, buf, h):
        return rc(b + h, os_.at[2 * h + 1], buf.at[h], 1)

    def reduce_copies(b, k):
        lo, hi = pl.ds(0, H), pl.ds(H, H)
        diag = [
            rc(b + 0, acc.at[k, 3, lo], rd.at[k, 0], 2),
            rc(b + 1, acc.at[k, 3, hi], rd.at[k, 1], 4),
        ]
        if k == 1:
            return diag + [
                rc(b + 2, acc.at[k, 1, pl.ds(0, FILL_X)], fx_ref, 2),
                rc(b + 3, acc.at[k, 2, pl.ds(T - FILL_Y, FILL_Y)], fy_ref, 4),
            ]
        return diag + [
            rc(b + 2, acc.at[k, 1, lo], fr.at[0, lo], 2),
            rc(b + 3, acc.at[k, 2, hi], fr.at[1, hi], 4),
            rc(b + 4, acc.at[k, 1, hi], fr.at[0, hi], 2),
            rc(b + 5, acc.at[k, 2, lo], fr.at[1, lo], 4),
        ]

    e0 = lax.broadcasted_iota(jnp.int32, (16 * NE, T), 0)
    e1 = lax.broadcasted_iota(jnp.int32, (16 * NE, T), 1) // CAP
    rank_lane = lax.rem(lax.broadcasted_iota(jnp.int32, (T, T), 1), CAP).astype(F32)

    def spread(idx, rows, weighted):
        pick = jnp.where(e0 == e1 + idx * NE, 1.0, 0.0).astype(BF16)
        hit = dot(rt[...], pick) == rank_lane
        if weighted:
            for k in range(3):
                sb[k] = jnp.where(hit, dot(gt[k], pick), 0.0).astype(BF16)
            return dot(sb[0], rows) + dot(sb[1], rows) + dot(sb[2], rows)
        sb[0] = jnp.where(hit, 1.0, 0.0).astype(BF16)
        return dot(sb[0], rows)

    def combine_all(k, b, recv, copies, weighted):
        def one(i, carry):
            h = 3 - i
            acc[k, h] = spread(2 * h, os_[2 * h].reshape(T, D), weighted)
            swap_copy(b, recv, h).wait_recv()
            acc[k, h] = acc[k, h] + spread(8 + h, recv[h].reshape(T, D), weighted)

            @pl.when(i == 0)
            def _():
                copies[0].start()
                copies[1].start()

            @pl.when(i == 1)
            def _():
                copies[3].start()

            @pl.when(i == 2)
            def _():
                copies[2].start()
            return carry
        lax.fori_loop(0, 4, one, 0)

    ro = reduce_copies(RS_O, 0)
    for h in order:
        swap_copy(OX, orv, h).start()
    cy[2].wait_recv()
    cy[7].start()
    cy[4].wait_recv()
    cy[8].start()
    combine_all(0, OX, orv, ro, True)

    cy[5].wait_recv()
    cy[6].wait_recv()
    cy[9].start()
    cy[0].wait_recv()
    cy[7].wait_recv()
    cy[8].wait_recv()
    cy[9].wait_recv()
    for c in cx:
        c.wait_send()

    swap_gg = rc(GG, gj.at[1], gr, 1)
    gg_diag = rc(GG + 1, gacc.at[3], gd, 4)
    gg_y = rc(GG + 2, gacc.at[2], gf.at[1], 4)
    gg_x = rc(GG + 3, gacc.at[1], gf.at[0], 2)

    def gather_dy(d, carry):
        build_p(d)
        rows = dot(pb[...], dya[d])
        outs = os_[d].reshape(T, D).astype(F32)
        gg_rows = jnp.sum(rows * outs, axis=1, keepdims=True)
        r_d = rm[d]
        g_d = gm[d]
        r_ids = ra[d].astype(F32)
        gg_d = jnp.zeros((8, T), F32)
        for l in range(NE):
            hit = lane_r == r_d[l:l + 1, :]
            gcol = jnp.sum(jnp.where(hit, g_d[l:l + 1, :], 0.0), axis=1, keepdims=True)
            xa[d, l * CAP:(l + 1) * CAP, :] = (gcol * rows[l * CAP:(l + 1) * CAP, :]).astype(BF16)
            gg_l = jnp.sum(
                jnp.where(hit, gg_rows[l * CAP:(l + 1) * CAP, :], 0.0), axis=0, keepdims=True)
            gg_d = gg_d + jnp.where(r_ids == (me * NE + l).astype(F32), gg_l, 0.0)
        gj[lax.rem(d, 2), d // 2] = gg_d
        return carry

    lax.fori_loop(0, 8, gather_dy, 0)
    swap_gg.start()
    for h in order:
        swap_copy(OX, orv, h).wait_send()

    swap_gg.wait_recv()
    gacc[...] = gj[0] + gr[...]
    gg_diag.start()
    gg_y.start()
    ro[0].wait_recv()
    acc[0, 2, :H] = acc[0, 2, :H] + rd[0, 0]
    ro[5].start()
    ro[1].wait_recv()
    acc[0, 1, H:] = acc[0, 1, H:] + rd[0, 1]
    ro[4].start()

    def expert_rows(buf, l):
        return buf[:, pl.ds(pl.multiple_of(l * CAP, CAP), CAP), :].reshape(T, D)

    def backward(l, carry):
        dh = dotg(expert_rows(xa, l), wd[l], NT).astype(BF16).astype(F32)
        uf = us[l].astype(F32)
        vf = vs[l].astype(F32)
        s = jax.nn.sigmoid(uf)
        sl = uf * s
        hs[l] = (sl * vf).astype(BF16)
        dv = (dh * sl).astype(BF16)
        du = (dh * vf * (s + sl * (1.0 - s))).astype(BF16)
        us[l] = du
        vs[l] = dv
        pr = (dotg(du, wg[l], NT) + dotg(dv, wu[l], NT)).astype(BF16)
        os_[:, pl.ds(l, 1)] = pr.reshape(8, 1, CAP, D)
        return carry

    out_xg = pltpu.make_async_copy(xg, xg_ref, lsem.at[5])
    out_c = pltpu.make_async_copy(xa, c_ref, lsem.at[6])
    out_xg.start()
    out_c.start()
    lax.fori_loop(0, NE, backward, 0)

    rp = reduce_copies(RS_P, 1)
    for h in order:
        swap_copy(PX, prv, h).start()
    gg_diag.wait_recv()
    gacc[1] = gacc[1] + gd[...]
    gg_x.start()
    combine_all(1, PX, prv, rp, False)

    lo, hi = pl.ds(0, H), pl.ds(H, H)
    early = [
        pltpu.make_async_copy(acc.at[1, 0], base_ref, lsem.at[8]),
        pltpu.make_async_copy(acc.at[1, 1, pl.ds(FILL_X, H - FILL_X)],
                              mx_ref.at[pl.ds(0, H - FILL_X)], lsem.at[9]),
        pltpu.make_async_copy(acc.at[1, 2, pl.ds(H, H - FILL_Y)],
                              my_ref.at[pl.ds(H, H - FILL_Y)], lsem.at[10]),
        pltpu.make_async_copy(us, du_ref, lsem.at[14]),
        pltpu.make_async_copy(vs, dv_ref, lsem.at[15]),
        pltpu.make_async_copy(hs, h_ref, lsem.at[16]),
    ]
    for c in early:
        c.start()
    for i in (2, 3, 4, 5):
        ro[i].wait_recv()
    moe_sc[...] = (acc[0, 0] + fr[0] + fr[1]).astype(BF16)
    out_moe = pltpu.make_async_copy(moe_sc, moe_ref, lsem.at[11])
    out_moe.start()
    for c in cr + cg + cy + ro + [swap_gg, gg_diag, gg_y]:
        c.wait_send()
    for h in order:
        swap_copy(PX, prv, h).wait_send()
    late_y = pltpu.make_async_copy(acc.at[1, 2, lo], my_ref.at[lo], lsem.at[12])
    late_x = pltpu.make_async_copy(acc.at[1, 1, hi], mx_ref.at[pl.ds(H - FILL_X, H)], lsem.at[13])
    rp[0].wait_recv()
    acc[1, 2, :H] = acc[1, 2, :H] + rd[1, 0]
    late_y.start()
    rp[1].wait_recv()
    acc[1, 1, H:] = acc[1, 1, H:] + rd[1, 1]
    late_x.start()
    gg_x.wait_recv()
    gg_y.wait_recv()
    gd[...] = gacc[0] + gf[0] + gf[1]
    out_gg = pltpu.make_async_copy(gd, gg_ref, lsem.at[7])
    out_gg.start()
    rp[2].wait_recv()
    rp[3].wait_recv()
    for c in rp + [gg_x]:
        c.wait_send()
    for c in early + [out_xg, out_c, out_moe, out_gg, late_y, late_x]:
        c.wait()


def publish(T, D, xg_ref, c_ref, du_ref, dv_ref, h_ref, moe_in, gg_in,
            dwg_ref, dwu_ref, dwd_ref, moe_ref, gg_ref):
    rows = xg_ref[...].reshape(T, D)
    dwg_ref[0] = dotg(rows, du_ref[0], TN)
    dwu_ref[0] = dotg(rows, dv_ref[0], TN)
    dwd_ref[0] = dotg(h_ref[0], c_ref[...].reshape(T, D), TN)

    @pl.when(pl.program_id(0) == 0)
    def _():
        moe_ref[...] = moe_in[...]
        gg_ref[...] = gg_in[...]


def solution(mesh):
    tok_spec = P(ALL_AXES, None)
    w_spec = P(EP_AXES, None, None)
    gw_spec = P(ALL_AXES, None, None)

    def local_step(tokens, route_idx, gate_vals, w_gate, w_up, w_down, grad_out):
        T, K = route_idx.shape
        D = tokens.shape[1]
        NE, _, FF = w_gate.shape
        CAP = T * K // (8 * NE)
        hbm = pl.BlockSpec(memory_space=pl.ANY)
        sds = jax.ShapeDtypeStruct
        outs = pl.pallas_call(
            functools.partial(kernel, T, D, FF, NE, CAP),
            out_shape=(sds((T, D), BF16), sds((K, T), F32),
                       sds((T, D), F32), sds((T - FILL_X, D), F32), sds((T - FILL_Y, D), F32),
                       sds((FILL_X, D), F32), sds((FILL_Y, D), F32),
                       sds((8, NE, CAP, D), BF16), sds((8, T, D), BF16),
                       sds((NE, T, FF), BF16), sds((NE, T, FF), BF16), sds((NE, T, FF), BF16)),
            in_specs=[hbm] * 7,
            out_specs=(hbm,) * 12,
            scratch_shapes=[
                pltpu.VMEM((8, T, D), BF16),
                pltpu.VMEM((8, T, D), BF16),
                pltpu.VMEM((8, NE, CAP, D), BF16),
                pltpu.VMEM((NE, T, FF), BF16),
                pltpu.VMEM((NE, T, FF), BF16),
                pltpu.VMEM((NE, T, FF), BF16),
                pltpu.VMEM((8, NE, CAP, D), BF16),
                pltpu.VMEM((NE, D, FF), BF16),
                pltpu.VMEM((NE, D, FF), BF16),
                pltpu.VMEM((NE, FF, D), BF16),
                pltpu.VMEM((2, 4, T, D), F32),
                pltpu.VMEM((2, 2, T // 2, D), F32),
                pltpu.VMEM((2, T, D), F32),
                pltpu.VMEM((4, NE, CAP, D), BF16),
                pltpu.VMEM((4, NE, CAP, D), BF16),
                pltpu.VMEM((T, T), BF16),
                pltpu.VMEM((3, T, T), BF16),
                pltpu.VMEM((K, T), jnp.int32),
                pltpu.VMEM((8, K, T), BF16),
                pltpu.VMEM((8, K, T), F32),
                pltpu.VMEM((16, NE, T), F32),
                pltpu.VMEM((16, NE, T), F32),
                pltpu.VMEM((16, NE, T), F32),
                pltpu.VMEM((T, 16 * NE), BF16),
                pltpu.VMEM((3, T, 16 * NE), BF16),
                pltpu.VMEM((2, 4, K, T), F32),
                pltpu.VMEM((4, K, T), F32),
                pltpu.VMEM((4, K, T), F32),
                pltpu.VMEM((K, T), F32),
                pltpu.VMEM((2, K, T), F32),
                pltpu.VMEM((T, D), BF16),
                pltpu.SemaphoreType.DMA((N_SEM,)),
                pltpu.SemaphoreType.DMA((N_SEM,)),
                pltpu.SemaphoreType.DMA((17,)),
            ],
            compiler_params=pltpu.CompilerParams(
                collective_id=0, has_side_effects=True, vmem_limit_bytes=67043328),
        )(tokens, grad_out, route_idx.T, gate_vals.T, w_gate, w_up, w_down)
        moe, gg, base, mx, my, fx, fy, xg, c, du, dv, h = outs
        rx = lax.ppermute(mx, 'col', [(0, 1), (1, 0)])
        ry = lax.ppermute(my, 'row', [(0, 1), (1, 0)])

        def per_expert(*shape):
            return pl.BlockSpec((1,) + shape, lambda l: (l, 0, 0))

        def whole(a):
            return pl.BlockSpec(a.shape, lambda l: (0, 0))

        dwg, dwu, dwd, moe, gg = pl.pallas_call(
            functools.partial(publish, T, D),
            grid=(NE,),
            out_shape=(sds((NE, D, FF), F32), sds((NE, D, FF), F32), sds((NE, FF, D), F32),
                       sds(moe.shape, BF16), sds(gg.shape, F32)),
            in_specs=[pl.BlockSpec((8, 1, CAP, D), lambda l: (0, l, 0, 0)),
                      pl.BlockSpec((8, CAP, D), lambda l: (0, l, 0)),
                      per_expert(T, FF), per_expert(T, FF), per_expert(T, FF), whole(moe), whole(gg)],
            out_specs=(per_expert(D, FF), per_expert(D, FF), per_expert(FF, D), whole(moe), whole(gg)),
            cost_estimate=pl.CostEstimate(
                flops=6 * NE * T * D * FF, bytes_accessed=36 * 1024 * 1024, transcendentals=0),
            compiler_params=pltpu.CompilerParams(vmem_limit_bytes=60 * 1024 * 1024),
        )(xg, c, du, dv, h, moe, gg)
        gx = (base + jnp.concatenate([fx, rx]) + jnp.concatenate([ry, fy])).astype(BF16)
        return moe, gx, gg.T, dwg, dwu, dwd

    return jax.shard_map(
        local_step, mesh=mesh,
        in_specs=(tok_spec, tok_spec, tok_spec, w_spec, w_spec, w_spec, tok_spec),
        out_specs=(tok_spec, tok_spec, tok_spec, gw_spec, gw_spec, gw_spec),
        check_vma=False)
```
